32 devices in a mesh: batch: 1 (over z), rows: 4 (over y), ksplit: 8 (over x, core).
Axes of the slice: x: 4, y: 4, z: 1, core: 2. Of those that a mesh axis runs over, the one named last changes fastest.
The devices are a block of a 4x4x8 slice.
Arguments:
- a_vals: bfloat16 [4, 8, 16, 128, 128], P(('batch', 'rows'), 'ksplit')
- b_vals: bfloat16 [8, 64, 128, 128], P(('batch', 'ksplit'))
- pairs: int32 [4, 8, 512, 1, 2], P(('batch', 'rows'), 'ksplit')
- plist_idx: int32 [4, 8, 512, 2], P(('batch', 'rows'), 'ksplit')
- c_idx: int32 [4, 8, 64, 2], P(('batch', 'rows'), 'ksplit')
Outputs:
- output: float32 [4, 8, 64, 128, 128], P(('batch', 'rows'), 'ksplit')
All inputs are finite; a program needn't handle non-finite values.
Results may differ from the reference program's by a relative error of at most 0.001.
Values are sent between devices in bfloat16 or wider.
A program may use at most 768 MiB of HBM per device.

```python
import jax
import jax.numpy as jnp
from jax import lax

BLOCK_SIZE = 128
ROW_GROUPS = 4
K_DEVICES = 8
BLOCK_ROWS = 512
BLOCK_COLS = 128
ROWS_TOUCH = 16
COLS_PER_DEV = 4
SENDERS = 8
K_PER_ROW = 1

ROW_LOCAL = BLOCK_ROWS // ROW_GROUPS
K_ACTIVE = 2 * K_PER_ROW
COL_TOUCH = SENDERS * COLS_PER_DEV
OWNER_SHARE = ROWS_TOUCH * COLS_PER_DEV // K_DEVICES
CAP_A = ROWS_TOUCH * K_PER_ROW
CAP_B = K_ACTIVE * COL_TOUCH
CAP_C = K_DEVICES * OWNER_SHARE
CAP_DEST = SENDERS * OWNER_SHARE
CAP_PART = K_DEVICES * CAP_DEST


def permute_rows(key, count, length):
    return jax.vmap(lambda sub_key: jax.random.permutation(sub_key, length))(jax.random.split(key, count))


def draw_indices(key):
    key_list = jax.random.split(key, 8)
    row_pick = permute_rows(key_list[0], ROW_GROUPS, ROW_LOCAL)[:, :ROWS_TOUCH]
    row_glob = row_pick + ROW_LOCAL * jnp.arange(ROW_GROUPS)[:, None]
    col_union = jax.random.permutation(key_list[1], BLOCK_COLS)[:K_DEVICES * COLS_PER_DEV]
    owner_shift = jax.random.randint(key_list[2], (ROW_GROUPS,), 0, K_DEVICES)
    band_start = jax.random.randint(key_list[3], (ROW_GROUPS, K_DEVICES, ROWS_TOUCH), 0, K_ACTIVE)
    a_order = permute_rows(key_list[4], ROW_GROUPS * K_DEVICES, CAP_A).reshape(ROW_GROUPS, K_DEVICES, CAP_A)
    b_order = permute_rows(key_list[5], K_DEVICES, CAP_B)
    c_order = permute_rows(key_list[6], ROW_GROUPS * K_DEVICES, CAP_C).reshape(ROW_GROUPS, K_DEVICES, CAP_C)
    p_order = permute_rows(key_list[7], ROW_GROUPS * K_DEVICES * K_DEVICES, CAP_DEST).reshape(ROW_GROUPS, K_DEVICES, K_DEVICES, CAP_DEST)
    dev_ids = jnp.arange(K_DEVICES)
    group_ids = jnp.arange(ROW_GROUPS)
    group4 = group_ids[:, None, None, None]
    owner4 = dev_ids[None, :, None, None]
    class4 = dev_ids[None, None, :, None]
    share4 = jnp.arange(OWNER_SHARE)[None, None, None, :]
    owned_pos = (owner4 - owner_shift[:, None, None, None]) % K_DEVICES + K_DEVICES * share4
    c_row = jnp.broadcast_to(row_glob[group4, owned_pos // COLS_PER_DEV], (ROW_GROUPS, K_DEVICES, K_DEVICES, OWNER_SHARE))
    c_col = col_union[K_DEVICES * (owned_pos % COLS_PER_DEV) + class4]
    c_all = jnp.stack([c_row, c_col], axis=-1).reshape(ROW_GROUPS, K_DEVICES, CAP_C, 2)
    c_idx = c_all[group_ids[:, None, None], dev_ids[None, :, None], c_order]
    full_shape = (ROW_GROUPS, K_DEVICES, K_DEVICES, SENDERS, OWNER_SHARE)
    group5 = group_ids[:, None, None, None, None]
    source5 = dev_ids[None, :, None, None, None]
    dest5 = dev_ids[None, None, :, None, None]
    sender5 = jnp.arange(SENDERS)[None, None, None, :, None]
    share5 = jnp.arange(OWNER_SHARE)[None, None, None, None, :]
    sent_pos = (dest5 - owner_shift[:, None, None, None, None]) % K_DEVICES + K_DEVICES * share5
    row_slot = jnp.broadcast_to(sent_pos // COLS_PER_DEV, full_shape)
    col_set = sent_pos % COLS_PER_DEV
    col_pos = K_DEVICES * col_set + (source5 - sender5) % K_DEVICES
    local_col = jnp.broadcast_to(sender5 * COLS_PER_DEV + col_set, full_shape)
    p_row = row_glob[group5, row_slot]
    p_col = col_union[col_pos]
    plist_all = jnp.stack([p_row, p_col], axis=-1).reshape(ROW_GROUPS, K_DEVICES, K_DEVICES, CAP_DEST, 2)
    step_ids = jnp.arange(K_PER_ROW)
    group6 = group5[..., None]
    source6 = source5[..., None]
    row6 = row_slot[..., None]
    a_slot = a_order[group6, source6, row6 * K_PER_ROW + step_ids]
    k_slot = (band_start[group6, source6, row6] + step_ids) % K_ACTIVE
    b_slot = b_order[source6, k_slot * COL_TOUCH + local_col[..., None]]
    pair_all = jnp.stack([a_slot, b_slot], axis=-1).reshape(ROW_GROUPS, K_DEVICES, K_DEVICES, CAP_DEST, K_PER_ROW, 2)
    reorder = (group_ids[:, None, None, None], dev_ids[None, :, None, None], dev_ids[None, None, :, None], p_order)
    plist_idx = plist_all[reorder].reshape(ROW_GROUPS, K_DEVICES, CAP_PART, 2)
    pairs = pair_all[reorder].reshape(ROW_GROUPS, K_DEVICES, CAP_PART, K_PER_ROW, 2)
    return pairs.astype(jnp.int32), plist_idx.astype(jnp.int32), c_idx.astype(jnp.int32)


def setup_inputs(seed: int = 0, part: int = 0) -> dict:
    base_key = jax.random.fold_in(jax.random.key(seed), part)
    index_key, a_key, b_key = jax.random.split(base_key, 3)
    pairs, plist_idx, c_idx = draw_indices(index_key)
    a_scale = (BLOCK_SIZE * K_PER_ROW * SENDERS) ** -0.5
    a_vals = (jax.random.normal(a_key, (ROW_GROUPS, K_DEVICES, CAP_A, BLOCK_SIZE, BLOCK_SIZE), jnp.float32) * a_scale).astype(jnp.bfloat16)
    b_vals = jax.random.normal(b_key, (K_DEVICES, CAP_B, BLOCK_SIZE, BLOCK_SIZE), jnp.float32).astype(jnp.bfloat16)
    return {'a_vals': a_vals, 'b_vals': b_vals, 'pairs': pairs, 'plist_idx': plist_idx, 'c_idx': c_idx}


def device_partials(a_dev, b_dev, pair_dev):
    a_sel = jnp.take(a_dev, pair_dev[:, :, 0], axis=0).astype(jnp.float32)
    b_sel = jnp.take(b_dev, pair_dev[:, :, 1], axis=0).astype(jnp.float32)
    return jnp.einsum('stab,stbc->sac', a_sel, b_sel).astype(jnp.bfloat16)


def reference(a_vals, b_vals, pairs, plist_idx, c_idx):
    flat_size = BLOCK_SIZE * BLOCK_SIZE

    def produce(device):
        group = device // K_DEVICES
        source = device % K_DEVICES
        return device_partials(a_vals[group, source], b_vals[source], pairs[group, source])

    partials = lax.map(produce, jnp.arange(ROW_GROUPS * K_DEVICES))
    partials = partials.reshape(ROW_GROUPS, K_DEVICES, K_DEVICES, CAP_DEST, flat_size)
    sent_idx = plist_idx.reshape(ROW_GROUPS, K_DEVICES, K_DEVICES, CAP_DEST, 2)

    def collect(device):
        group = device // K_DEVICES
        owner = device % K_DEVICES
        recv_vals = partials[group, :, owner].reshape(CAP_PART, flat_size).astype(jnp.float32)
        recv_idx = sent_idx[group, :, owner].reshape(CAP_PART, 2)
        hit_mask = jnp.all(c_idx[group, owner][:, None, :] == recv_idx[None, :, :], axis=-1).astype(jnp.float32)
        return jnp.dot(hit_mask, recv_vals, preferred_element_type=jnp.float32)

    c_vals = lax.map(collect, jnp.arange(ROW_GROUPS * K_DEVICES))
    return c_vals.reshape(ROW_GROUPS, K_DEVICES, CAP_C, BLOCK_SIZE, BLOCK_SIZE)
```

```python
import functools

import jax
import jax.numpy as jnp
from jax import lax
from jax.experimental import pallas as pl
from jax.experimental.pallas import tpu as pltpu
from jax.sharding import PartitionSpec as P

MESH = pl.DeviceIdType.MESH
HALF_SET = 32
CHUNK = 4
UNROLL = 8
FRONT = 8


class Move:
    def __init__(self, link, kind, src, dst, part, first, count, dep):
        self.link, self.kind, self.src, self.dst = link, kind, src, dst
        self.part, self.first, self.count, self.dep = part, first, count, dep
        self.after = []
        self.shift = 0
        self.arrive = None


def cut(first, count, size):
    return [(first + at, min(size, count - at)) for at in range(0, count, size)]


def plan(n_a, n_b, half_set):
    half = half_set // 2
    quarter = (n_b - half_set) // 4
    h1, h2 = cut(0, half // 2, CHUNK), cut(half // 2, half - half // 2, CHUNK)
    q1, q2 = cut(0, quarter // 2, CHUNK), cut(quarter // 2, quarter - quarter // 2, CHUNK)
    a1, a2 = (0, n_a // 2), (n_a // 2, n_a - n_a // 2)
    moves = []

    def add(link, kind, src, dst, part, piece, dep, shift=0):
        move = Move(link, kind, src, dst, part, piece[0], piece[1], dep)
        move.shift = shift
        move.index = len(moves)
        moves.append(move)
        if dep is not None:
            dep.after.append(move)
        if link != "d":
            add_pair(move)
        return move

    def add_pair(move):
        row = {"+y": -1, "-y": 1}.get(move.link, 0) + move.shift
        add("d", move.kind, move.dst, move.dst, move.part, (move.first, move.count), move, row)

    def spread(move, up, down, piece):
        for link in ("+y",) * up + ("-y",) * down:
            step = 1 if link == "+y" else -1
            nxt = add(link, "b", move.dst, move.dst, move.part, piece, move)
            if move.part == "q":
                if (link == "+y" and piece in q1) or (link == "-y" and piece in q2):
                    add(link, "b", move.dst, move.dst, "q", piece, nxt, -step)

    def over_x(link, back, pieces, part, group):
        out = []
        for piece in pieces:
            move = add(link, "b", 0, back, part, piece, None)
            out.append((move, piece, group))
        return out

    add("d", "b", 0, 0, "all", (0, n_b), None)
    add("d", "a", 0, 0, "all", (0, n_a), None)
    right = over_x("+x", 3, h1, "h", 1) + over_x("+x", 3, h2, "h", 2) + over_x("+x", 3, q1, "q", 1) + over_x("+x", 3, q2, "q", 2)
    left = over_x("-x", 1, h2, "h", 2) + over_x("-x", 1, h1, "h", 1) + over_x("-x", 1, q2, "q", 2) + over_x("-x", 1, q1, "q", 1)
    for received, link, keep in ((right, "+x", 1), (left, "-x", 2)):
        for move, piece, group in received:
            spread(move, move.part == "q" or group == 1, move.part == "q" or group == 2, piece)
            if group == keep:
                nxt = add(link, "b", move.dst, 2, move.part, piece, move)
                spread(nxt, nxt.part == "q" or group == 1, nxt.part == "q" or group == 2, piece)
    late = []
    for (received, link, back, half_a) in ((right, "+x", 3, a1), (left, "-x", 1, a2)):
        for piece in (a1, a2) if link == "+x" else (a2, a1):
            move = add(link, "a", 0, back, "all", piece, received[-1][0])
            if piece == half_a:
                add(link, "a", move.dst, 2, "all", piece, move)
    return moves


def expected(moves):
    free = {"+x": 0.0, "-x": 0.0, "+y": 0.0, "-y": 0.0, "d": 0.0}
    lag = {"+x": 2.6, "-x": 2.6, "+y": 2.6, "-y": 2.6, "d": 1.4}
    ready = [(0.0, i, m) for i, m in enumerate(moves) if m.dep is None]
    order = []
    count = len(moves)
    while ready:
        ready.sort(key=lambda item: (item[0], item[1]))
        at, _, move = ready.pop(0)
        begin = max(at, free[move.link])
        free[move.link] = begin + move.count * (0.1 if move.link == "d" else 1.0)
        move.arrive = free[move.link] + lag[move.link]
        order.append(move)
        for nxt in move.after:
            ready.append((move.arrive, nxt.index, nxt))
    assert len(order) == count
    return sorted(moves, key=lambda m: (m.arrive, m.index))


def kernel(sizes, a_hbm, b_hbm, pairs_hbm, plist_hbm, own_hbm, out_hbm, *scratch):
    n_x, n_y, n_a, n_b, n_own = sizes
    a_slot, b_slot = scratch[0:8], scratch[8:16]
    (acc, pairs_own, plist_own, own, pairs_in, plist_in, table_v, table,
     send_sem, recv_sem, list_send, list_recv, load_sem, out_sem) = scratch[16:]
    y = lax.axis_index("rows")
    p = lax.axis_index("ksplit")
    x, core = p // 2, p % 2
    moves = plan(n_a, n_b, HALF_SET)
    arrivals = expected(moves)

    def at(dx, other):
        return 2 * ((x + dx) % n_x) + (core + other) % 2

    target = {
        "+x": {"ksplit": at(1, 0)},
        "-x": {"ksplit": at(n_x - 1, 0)},
        "+y": {"rows": (y + 1) % n_y},
        "-y": {"rows": (y + n_y - 1) % n_y},
        "d": {"ksplit": at(0, 1)},
    }

    loads = [
        pltpu.make_async_copy(b_hbm, b_slot[0], load_sem.at[0]),
        pltpu.make_async_copy(a_hbm, a_slot[0], load_sem.at[1]),
        pltpu.make_async_copy(pairs_hbm, pairs_own, load_sem.at[2]),
        pltpu.make_async_copy(plist_hbm, plist_own, load_sem.at[3]),
        pltpu.make_async_copy(own_hbm, own, load_sem.at[4]),
    ]
    for load in loads:
        load.start()

    peers = [(dx, other) for dx in range(n_x) for other in range(2) if (dx, other) != (0, 0)]
    barrier = pltpu.get_barrier_semaphore()
    for dx, other in peers:
        pl.semaphore_signal(barrier, inc=1, device_id={"ksplit": at(dx, other)}, device_id_type=MESH)
    for link in ("+y", "-y"):
        pl.semaphore_signal(barrier, inc=1, device_id=target[link], device_id_type=MESH)
    pl.semaphore_wait(barrier, len(peers) + 2)

    def copy(move, row):
        holder = (row + move.shift + 2 * n_y) % n_y
        half = HALF_SET // 2
        quarter = (n_b - HALF_SET) // 4
        base = {"all": 0, "h": (holder % 2) * half, "q": HALF_SET + holder * quarter}[move.part]
        where = pl.ds(base + move.first, move.count)
        slots = a_slot if move.kind == "a" else b_slot
        src = slots[2 * move.src]
        dst = slots[2 * move.dst + (1 if move.link == "d" else 0)]
        return pltpu.make_async_remote_copy(
            src_ref=src.at[where],
            dst_ref=dst.at[where],
            send_sem=send_sem.at[move.index],
            recv_sem=recv_sem.at[move.index],
            device_id=target[move.link],
            device_id_type=MESH,
        )

    def start(move):
        copy(move, y).start()

    def receive(move):
        row = {"+y": y + n_y - 1, "-y": y + 1}.get(move.link, y)
        copy(move, row).wait_recv()

    def lists(number, dx, other):
        mine, theirs = 2 * dx + other, 2 * ((n_x - dx) % n_x) + other
        where = pl.ds(pl.multiple_of(((x + dx) % n_x) * 128, 128), 128)
        pair = []
        for which, (src, dst) in enumerate(((pairs_own, pairs_in), (plist_own, plist_in))):
            pair.append(pltpu.make_async_remote_copy(
                src_ref=src.at[:, where],
                dst_ref=dst.at[theirs],
                send_sem=list_send.at[2 * number + which],
                recv_sem=list_recv.at[2 * number + which],
                device_id={"ksplit": at(dx, other)},
                device_id_type=MESH,
            ))
        return pair

    def lists_in(number, dx, other):
        mine = 2 * dx + other
        pair = []
        back = peers.index(((n_x - dx) % n_x, other))
        for which, (src, dst) in enumerate(((pairs_own, pairs_in), (plist_own, plist_in))):
            pair.append(pltpu.make_async_remote_copy(
                src_ref=src.at[:, pl.ds(0, 128)],
                dst_ref=dst.at[mine],
                send_sem=list_send.at[2 * back + which],
                recv_sem=list_recv.at[2 * back + which],
                device_id={"ksplit": at(dx, other)},
                device_id_type=MESH,
            ))
        return pair

    loads[0].wait()
    for move in moves:
        if move.dep is None and move.kind == "b" and move.link != "d":
            start(move)
    for load in loads[1:]:
        load.wait()
    for number, (dx, other) in enumerate(peers):
        for one in lists(number, dx, other):
            one.start()
    for move in moves:
        if move.dep is None and (move.kind == "a" or move.link == "d"):
            start(move)

    def make_table():
        mine = pl.ds(pl.multiple_of(x * 128, 128), 128)
        pairs_in[0] = pairs_own[:, mine]
        plist_in[0] = plist_own[:, mine]
        for number, (dx, other) in enumerate(peers):
            for one in lists_in(number, dx, other):
                one.wait_recv()
        key = plist_in[:, 0, :] * 65536 + plist_in[:, 1, :]
        code = pairs_in[:, 0, :] * 65536 + pairs_in[:, 1, :]
        wanted = own[0:1, :] * 65536 + own[1:2, :]
        wanted = jnp.concatenate([wanted] * (128 // n_own), axis=1)
        wanted = jnp.broadcast_to(wanted, key.shape)

        def turn(_, state):
            key, code, found = state
            found = jnp.where(key == wanted, code, found)
            return pltpu.roll(key, 1, 1), pltpu.roll(code, 1, 1), found

        _, _, found = lax.fori_loop(0, 128, turn, (key, code, jnp.zeros_like(code)), unroll=8)
        table_v[0] = found // 65536
        table_v[1] = found % 65536

    def use_table():
        to_smem = pltpu.make_async_copy(table_v, table, load_sem.at[5])
        to_smem.start()
        to_smem.wait()

    def product(slot, c):
        left = a_slot[slot][table[0, slot, c]]
        right = b_slot[slot][table[1, slot, c]]
        part = jnp.dot(left, right, preferred_element_type=jnp.float32)
        return part.astype(jnp.bfloat16).astype(jnp.float32)

    def compute(slots, first=False, last=False):
        def step(i, _):
            for u in range(UNROLL):
                c = i * UNROLL + u
                total = product(slots[0], c)
                for slot in slots[1:]:
                    total = total + product(slot, c)
                acc[c] = total if first else acc[c] + total
            if last:
                out_copy(i).start()
            return 0

        lax.fori_loop(0, n_own // UNROLL, step, 0)

    def out_copy(i):
        where = pl.ds(i * UNROLL, UNROLL)
        return pltpu.make_async_copy(acc.at[where], out_hbm.at[where], out_sem.at[i])

    seen = set()

    def take(move):
        if move.index not in seen:
            seen.add(move.index)
            receive(move)
            for nxt in move.after:
                start(nxt)

    def need(dx, other):
        return [m for m in arrivals if m.dst == dx and (m.link == "d") == bool(other)]

    wire = [m for m in arrivals if m.link != "d"]
    early = [m for m in wire if m.arrive < 10.0]
    for move in early:
        take(move)
    make_table()
    for move in wire:
        if move.arrive < 14.0:
            take(move)
    use_table()
    for move in need(0, 1):
        take(move)
    compute((0, 1), first=True)
    done = {0}
    for position, move in enumerate(wire):
        take(move)
        rest = [m for m in wire[position + 1:]]
        for dx in (3, 1):
            if dx not in done and not [m for m in rest if m.dst == dx]:
                done.add(dx)
                for m in need(dx, 1):
                    take(m)
                compute((2 * dx, 2 * dx + 1))
    compute((4,))
    for m in need(2, 1):
        take(m)
    compute((5,), last=True)
    assert len(seen) == len(moves)

    for number, (dx, other) in enumerate(peers):
        for one in lists(number, dx, other):
            one.wait_send()
    for move in moves:
        copy(move, y).wait_send()
    for i in range(n_own // UNROLL):
        out_copy(i).wait()


def solution(mesh):
    n_y = mesh.shape["rows"]
    n_x = mesh.shape["ksplit"] // 2
    row_spec = P(("batch", "rows"), "ksplit")
    col_spec = P(("batch", "ksplit"))

    def device_step(a_loc, b_loc, pair_loc, plist_loc, cidx_loc):
        a, b = a_loc[0, 0], b_loc[0]
        n_a, size, _ = a.shape
        n_b = b.shape[0]
        n_own = cidx_loc.shape[2]
        n_part = plist_loc.shape[2]
        assert n_x == 4 and n_y == 4 and n_part == n_x * 128 and 128 % n_own == 0
        moves = plan(n_a, n_b, HALF_SET)
        any_space = pl.BlockSpec(memory_space=pl.ANY)
        out = pl.pallas_call(
            functools.partial(kernel, (n_x, n_y, n_a, n_b, n_own)),
            out_shape=jax.ShapeDtypeStruct((n_own, size, size), jnp.float32),
            in_specs=[any_space] * 5,
            out_specs=any_space,
            scratch_shapes=[pltpu.VMEM((n_a, size, size), jnp.bfloat16)] * 8
            + [pltpu.VMEM((n_b, size, size), jnp.bfloat16)] * 8
            + [
                pltpu.VMEM((n_own, size, size), jnp.float32),
                pltpu.VMEM((2, n_part), jnp.int32),
                pltpu.VMEM((2, n_part), jnp.int32),
                pltpu.VMEM((2, n_own), jnp.int32),
                pltpu.VMEM((8, 2, 128), jnp.int32),
                pltpu.VMEM((8, 2, 128), jnp.int32),
                pltpu.VMEM((2, 8, 128), jnp.int32),
                pltpu.SMEM((2, 8, 128), jnp.int32),
                pltpu.SemaphoreType.DMA((len(moves),)),
                pltpu.SemaphoreType.DMA((len(moves),)),
                pltpu.SemaphoreType.DMA((14,)),
                pltpu.SemaphoreType.DMA((14,)),
                pltpu.SemaphoreType.DMA((6,)),
                pltpu.SemaphoreType.DMA((n_own // UNROLL,)),
            ],
            compiler_params=pltpu.CompilerParams(
                collective_id=0, has_side_effects=True, vmem_limit_bytes=48 * 1024 * 1024
            ),
        )(a, b, pair_loc[0, 0, :, 0, :].T, plist_loc[0, 0].T, cidx_loc[0, 0].T)
        return out[None, None]

    return jax.shard_map(
        device_step, mesh=mesh, in_specs=(row_spec, col_spec, row_spec, row_spec, row_spec), out_specs=row_spec, check_vma=False
    )
```

```python
import functools

import jax
import jax.numpy as jnp
from jax import lax
from jax.experimental import pallas as pl
from jax.experimental.pallas import tpu as pltpu
from jax.sharding import PartitionSpec as P

MESH = pl.DeviceIdType.MESH
HALF_SET = 32
CHUNK = 4
A_CHUNK = 4
WINDOW = 2
TABLE_AT = 9.0
LAG = 3.0
UNROLL = 8


class Move:
    def __init__(self, link, kind, src, dst, part, first, count, dep, shift, rank):
        self.link, self.kind, self.src, self.dst = link, kind, src, dst
        self.part, self.first, self.count, self.dep = part, first, count, dep
        self.shift = shift
        self.rank = rank
        self.after = []


def cut(first, count, size):
    return [(first + at, min(size, count - at)) for at in range(0, count, size)]


def plan(n_a, n_b):
    half = HALF_SET // 2
    quarter = (n_b - HALF_SET) // 4
    h1, h2 = cut(0, half // 2, CHUNK), cut(half // 2, half - half // 2, CHUNK)
    q1, q2 = cut(0, quarter // 2, CHUNK), cut(quarter // 2, quarter - quarter // 2, CHUNK)
    a1, a2 = cut(0, n_a // 2, A_CHUNK), cut(n_a // 2, n_a - n_a // 2, A_CHUNK)
    moves = []

    def add(link, kind, src, dst, part, piece, dep, rank, shift=0):
        move = Move(link, kind, src, dst, part, piece[0], piece[1], dep, shift, rank)
        move.index = len(moves)
        moves.append(move)
        if dep is not None:
            dep.after.append(move)
        if link != "d":
            row = {"+y": -1, "-y": 1}.get(link, 0) + shift
            add("d", kind, dst, dst, part, piece, move, 0, row)
        return move

    def spread(move, piece, far):
        if move.part == "h":
            add("+y" if piece in h1 else "-y", "b", move.dst, move.dst, "h", piece, move, far + 1)
            return
        up = add("+y", "b", move.dst, move.dst, "q", piece, move, far)
        down = add("-y", "b", move.dst, move.dst, "q", piece, move, far)
        if piece in q1:
            add("+y", "b", move.dst, move.dst, "q", piece, up, far + 2, -1)
        else:
            add("-y", "b", move.dst, move.dst, "q", piece, down, far + 2, 1)

    for kind, count in (("b", n_b), ("a", n_a)):
        add("d", kind, 0, 0, "all", (0, count), None, 9)
    for link, slot in (("+x", 3), ("-x", 1)):
        first = link == "+x"
        for part, one, two in (("q", q1, q2), ("h", h1, h2)):
            keep = one if first else two
            for piece in (one + two) if first else (two + one):
                move = add(link, "b", 0, slot, part, piece, None, 0)
                spread(move, piece, 0)
                if piece in keep:
                    spread(add(link, "b", slot, 2, part, piece, move, 1), piece, 3)
        keep = a1 if first else a2
        for piece in (a1 + a2) if first else (a2 + a1):
            move = add(link, "a", 0, slot, "all", piece, None, 2)
            if piece in keep:
                add(link, "a", slot, 2, "all", piece, move, 3)
    return moves


LINKS = ("+x", "-x", "+y", "-y")


def order(moves):
    waiting = {link: [m for m in moves if m.link == link and m.dep is None] for link in LINKS}
    flying = {link: 0 for link in LINKS}
    free = {link: 0.0 for link in LINKS}
    events, steps, now = [], [], 0.0

    def send():
        for link in LINKS:
            waiting[link].sort(key=lambda m: (m.rank, m.index))
        busy = True
        while busy:
            busy = False
            for link in LINKS:
                if waiting[link] and flying[link] < WINDOW:
                    move = waiting[link].pop(0)
                    flying[link] += 1
                    free[link] = max(now, free[link]) + move.count
                    events.append((free[link] + LAG, move.index, move))
                    steps.append((now, "send", move))
                    busy = True

    send()
    while events:
        events.sort(key=lambda e: e[:2])
        now, _, move = events.pop(0)
        flying[move.link] -= 1
        steps.append((now, "take", move))
        for nxt in move.after:
            if nxt.link == "d":
                steps.append((now, "send", nxt))
            else:
                waiting[nxt.link].append(nxt)
        send()
    assert not any(waiting.values())
    return steps


def kernel(sizes, a_hbm, b_hbm, pairs_hbm, plist_hbm, own_hbm, out_hbm, *scratch):
    n_x, n_y, n_a, n_b, n_own = sizes
    a_slot, b_slot = scratch[0:8], scratch[8:16]
    (acc, pairs_own, plist_own, own, pairs_in, plist_in, table_v, table,
     send_sem, recv_sem, list_send, list_recv, load_sem, out_sem) = scratch[16:]
    y = lax.axis_index("rows")
    p = lax.axis_index("ksplit")
    x, core = p // 2, p % 2
    moves = plan(n_a, n_b)
    steps = order(moves)

    def at(dx, other):
        return 2 * ((x + dx) % n_x) + (core + other) % 2

    target = {
        "+x": {"ksplit": at(1, 0)},
        "-x": {"ksplit": at(n_x - 1, 0)},
        "+y": {"rows": (y + 1) % n_y},
        "-y": {"rows": (y + n_y - 1) % n_y},
        "d": {"ksplit": at(0, 1)},
    }

    loads = [
        pltpu.make_async_copy(b_hbm, b_slot[0], load_sem.at[0]),
        pltpu.make_async_copy(a_hbm, a_slot[0], load_sem.at[1]),
        pltpu.make_async_copy(pairs_hbm, pairs_own, load_sem.at[2]),
        pltpu.make_async_copy(plist_hbm, plist_own, load_sem.at[3]),
        pltpu.make_async_copy(own_hbm, own, load_sem.at[4]),
    ]
    for load in loads:
        load.start()

    peers = [(dx, other) for dx in range(n_x) for other in range(2) if (dx, other) != (0, 0)]
    barrier = pltpu.get_barrier_semaphore()
    for dx, other in peers:
        pl.semaphore_signal(barrier, inc=1, device_id={"ksplit": at(dx, other)}, device_id_type=MESH)
    for link in ("+y", "-y"):
        pl.semaphore_signal(barrier, inc=1, device_id=target[link], device_id_type=MESH)
    pl.semaphore_wait(barrier, len(peers) + 2)

    def copy(move, row):
        holder = (row + move.shift + 2 * n_y) % n_y
        half = HALF_SET // 2
        quarter = (n_b - HALF_SET) // 4
        base = {"all": 0, "h": (holder % 2) * half, "q": HALF_SET + holder * quarter}[move.part]
        where = pl.ds(base + move.first, move.count)
        slots = a_slot if move.kind == "a" else b_slot
        src = slots[2 * move.src]
        dst = slots[2 * move.dst + (1 if move.link == "d" else 0)]
        return pltpu.make_async_remote_copy(
            src_ref=src.at[where],
            dst_ref=dst.at[where],
            send_sem=send_sem.at[move.index],
            recv_sem=recv_sem.at[move.index],
            device_id=target[move.link],
            device_id_type=MESH,
        )

    def start(move):
        copy(move, y).start()

    def receive(move):
        row = {"+y": y + n_y - 1, "-y": y + 1}.get(move.link, y)
        copy(move, row).wait_recv()

    def lists(number, dx, other):
        mine, theirs = 2 * dx + other, 2 * ((n_x - dx) % n_x) + other
        where = pl.ds(pl.multiple_of(((x + dx) % n_x) * 128, 128), 128)
        pair = []
        for which, (src, dst) in enumerate(((pairs_own, pairs_in), (plist_own, plist_in))):
            pair.append(pltpu.make_async_remote_copy(
                src_ref=src.at[:, where],
                dst_ref=dst.at[theirs],
                send_sem=list_send.at[2 * number + which],
                recv_sem=list_recv.at[2 * number + which],
                device_id={"ksplit": at(dx, other)},
                device_id_type=MESH,
            ))
        return pair

    def lists_in(number, dx, other):
        mine = 2 * dx + other
        pair = []
        back = peers.index(((n_x - dx) % n_x, other))
        for which, (src, dst) in enumerate(((pairs_own, pairs_in), (plist_own, plist_in))):
            pair.append(pltpu.make_async_remote_copy(
                src_ref=src.at[:, pl.ds(0, 128)],
                dst_ref=dst.at[mine],
                send_sem=list_send.at[2 * back + which],
                recv_sem=list_recv.at[2 * back + which],
                device_id={"ksplit": at(dx, other)},
                device_id_type=MESH,
            ))
        return pair

    def run(step):
        _, what, move = step
        if what == "send":
            start(move)
        else:
            receive(move)

    for load in loads:
        load.wait()
    while steps[0][1] == "send":
        run(steps.pop(0))
    for number, (dx, other) in enumerate(peers):
        for one in lists(number, dx, other):
            one.start()
    for move in moves:
        if move.dep is None and move.link == "d":
            start(move)

    def make_table():
        mine = pl.ds(pl.multiple_of(x * 128, 128), 128)
        pairs_in[0] = pairs_own[:, mine]
        plist_in[0] = plist_own[:, mine]
        for number, (dx, other) in enumerate(peers):
            for one in lists_in(number, dx, other):
                one.wait_recv()
        key = plist_in[:, 0, :] * 65536 + plist_in[:, 1, :]
        code = pairs_in[:, 0, :] * 65536 + pairs_in[:, 1, :]
        wanted = own[0:1, :] * 65536 + own[1:2, :]
        wanted = jnp.concatenate([wanted] * (128 // n_own), axis=1)
        wanted = jnp.broadcast_to(wanted, key.shape)

        def turn(_, state):
            key, code, found = state
            found = jnp.where(key == wanted, code, found)
            return pltpu.roll(key, 1, 1), pltpu.roll(code, 1, 1), found

        _, _, found = lax.fori_loop(0, 128, turn, (key, code, jnp.zeros_like(code)), unroll=8)
        table_v[0] = found // 65536
        table_v[1] = found % 65536

    def use_table():
        to_smem = pltpu.make_async_copy(table_v, table, load_sem.at[5])
        to_smem.start()
        to_smem.wait()

    def product(slot, c):
        left = a_slot[slot][table[0, slot, c]]
        right = b_slot[slot][table[1, slot, c]]
        part = jnp.dot(left, right, preferred_element_type=jnp.float32)
        return part.astype(jnp.bfloat16).astype(jnp.float32)

    def compute(slots, part=(0, 1), first=False, last=False):
        def step(i, _):
            for u in range(UNROLL):
                c = i * UNROLL + u
                total = product(slots[0], c)
                for slot in slots[1:]:
                    total = total + product(slot, c)
                acc[c] = total if first else acc[c] + total
            if last:
                out_copy(i).start()
            return 0

        count = n_own // UNROLL // part[1]
        lax.fori_loop(part[0] * count, (part[0] + 1) * count, step, 0)

    def out_copy(i):
        where = pl.ds(i * UNROLL, UNROLL)
        return pltpu.make_async_copy(acc.at[where], out_hbm.at[where], out_sem.at[i])

    def from_partner(dx):
        for move in moves:
            if move.link == "d" and move.dst == dx:
                receive(move)

    jobs = []
    queued = set()
    stage = 0

    def ready(dx):
        return not [s for s in steps if s[1] == "take" and s[2].dst == dx]

    while steps:
        now = steps[0][0]
        if stage == 0 and now > TABLE_AT:
            make_table()
            stage = 1
        elif stage == 1 and now > TABLE_AT + 3.0:
            use_table()
            from_partner(0)
            jobs += [functools.partial(compute, (0, 1), (i, 2), first=True) for i in range(2)]
            stage = 2
        run(steps.pop(0))
        while steps and steps[0][1] == "send":
            run(steps.pop(0))
        for dx in (1, 3):
            if dx not in queued and ready(dx):
                queued.add(dx)
                jobs.append(functools.partial(from_partner, dx))
                jobs += [functools.partial(compute, (2 * dx, 2 * dx + 1), (i, 2)) for i in range(2)]
        if jobs:
            jobs.pop(0)()
    for job in jobs:
        job()
    compute((4,))
    from_partner(2)
    compute((5,), last=True)

    for number, (dx, other) in enumerate(peers):
        for one in lists(number, dx, other):
            one.wait_send()
    for move in moves:
        copy(move, y).wait_send()
    for i in range(n_own // UNROLL):
        out_copy(i).wait()


def solution(mesh):
    n_y = mesh.shape["rows"]
    n_x = mesh.shape["ksplit"] // 2
    row_spec = P(("batch", "rows"), "ksplit")
    col_spec = P(("batch", "ksplit"))

    def device_step(a_loc, b_loc, pair_loc, plist_loc, cidx_loc):
        a, b = a_loc[0, 0], b_loc[0]
        n_a, size, _ = a.shape
        n_b = b.shape[0]
        n_own = cidx_loc.shape[2]
        n_part = plist_loc.shape[2]
        assert n_x == 4 and n_y == 4 and n_part == n_x * 128 and 128 % n_own == 0
        moves = plan(n_a, n_b)
        in_hbm = pl.BlockSpec(memory_space=pltpu.HBM)
        out = pl.pallas_call(
            functools.partial(kernel, (n_x, n_y, n_a, n_b, n_own)),
            out_shape=jax.ShapeDtypeStruct((n_own, size, size), jnp.float32),
            in_specs=[in_hbm] * 5,
            out_specs=in_hbm,
            scratch_shapes=[pltpu.VMEM((n_a, size, size), jnp.bfloat16)] * 8
            + [pltpu.VMEM((n_b, size, size), jnp.bfloat16)] * 8
            + [
                pltpu.VMEM((n_own, size, size), jnp.float32),
                pltpu.VMEM((2, n_part), jnp.int32),
                pltpu.VMEM((2, n_part), jnp.int32),
                pltpu.VMEM((2, n_own), jnp.int32),
                pltpu.VMEM((8, 2, 128), jnp.int32),
                pltpu.VMEM((8, 2, 128), jnp.int32),
                pltpu.VMEM((2, 8, 128), jnp.int32),
                pltpu.SMEM((2, 8, 128), jnp.int32),
                pltpu.SemaphoreType.DMA((len(moves),)),
                pltpu.SemaphoreType.DMA((len(moves),)),
                pltpu.SemaphoreType.DMA((14,)),
                pltpu.SemaphoreType.DMA((14,)),
                pltpu.SemaphoreType.DMA((6,)),
                pltpu.SemaphoreType.DMA((n_own // UNROLL,)),
            ],
            compiler_params=pltpu.CompilerParams(
                collective_id=0, has_side_effects=True, vmem_limit_bytes=48 * 1024 * 1024
            ),
        )(a, b, pair_loc[0, 0, :, 0, :].T, plist_loc[0, 0].T, cidx_loc[0, 0].T)
        return out[None, None]

    return jax.shard_map(
        device_step, mesh=mesh, in_specs=(row_spec, col_spec, row_spec, row_spec, row_spec), out_specs=row_spec, check_vma=False
    )
```

```python
import functools

import jax
import jax.numpy as jnp
from jax import lax
from jax.experimental import pallas as pl
from jax.experimental.pallas import tpu as pltpu
from jax.sharding import PartitionSpec as P

MESH = pl.DeviceIdType.MESH
HALF_SET = 32
CHUNK = 4
A_CHUNK = 4
WINDOW = 3
TABLE_AT = 9.0
VMEM = 67_000_000
LAG = 3.0
UNROLL = 8


class Move:
    def __init__(self, link, kind, src, dst, part, first, count, dep, shift, rank):
        self.link, self.kind, self.src, self.dst = link, kind, src, dst
        self.part, self.first, self.count, self.dep = part, first, count, dep
        self.shift = shift
        self.rank = rank
        self.after = []


def cut(first, count, size):
    return [(first + at, min(size, count - at)) for at in range(0, count, size)]


def plan(n_a, n_b):
    half = HALF_SET // 2
    quarter = (n_b - HALF_SET) // 4
    h1, h2 = cut(0, half // 2, CHUNK), cut(half // 2, half - half // 2, CHUNK)
    q1, q2 = cut(0, quarter // 2, CHUNK), cut(quarter // 2, quarter - quarter // 2, CHUNK)
    a1, a2 = cut(0, n_a // 2, A_CHUNK), cut(n_a // 2, n_a - n_a // 2, A_CHUNK)
    moves = []

    def add(link, kind, src, dst, part, piece, dep, rank, shift=0):
        move = Move(link, kind, src, dst, part, piece[0], piece[1], dep, shift, rank)
        move.index = len(moves)
        moves.append(move)
        if dep is not None:
            dep.after.append(move)
        if link != "d":
            row = {"+y": -1, "-y": 1}.get(link, 0) + shift
            add("d", kind, dst, dst, part, piece, move, 0, row)
        return move

    def spread(move, piece, far):
        if move.part == "h":
            add("+y" if piece in h1 else "-y", "b", move.dst, move.dst, "h", piece, move, far + 1)
            return
        up = add("+y", "b", move.dst, move.dst, "q", piece, move, far)
        down = add("-y", "b", move.dst, move.dst, "q", piece, move, far)
        if piece in q1:
            add("+y", "b", move.dst, move.dst, "q", piece, up, far + 2, -1)
        else:
            add("-y", "b", move.dst, move.dst, "q", piece, down, far + 2, 1)

    for kind, count in (("b", n_b), ("a", n_a)):
        add("d", kind, 0, 0, "all", (0, count), None, 9)
    for link, slot in (("+x", 3), ("-x", 1)):
        first = link == "+x"
        for part, one, two in (("q", q1, q2), ("h", h1, h2)):
            keep = one if first else two
            for piece in (one + two) if first else (two + one):
                move = add(link, "b", 0, slot, part, piece, None, 0)
                spread(move, piece, 0)
                if piece in keep:
                    spread(add(link, "b", slot, 2, part, piece, move, 1), piece, 3)
        keep = a1 if first else a2
        for piece in (a1 + a2) if first else (a2 + a1):
            move = add(link, "a", 0, slot, "all", piece, None, 2)
            if piece in keep:
                add(link, "a", slot, 2, "all", piece, move, 3)
    return moves


LINKS = ("+x", "-x", "+y", "-y")


def order(moves):
    waiting = {link: [m for m in moves if m.link == link and m.dep is None] for link in LINKS}
    flying = {link: 0 for link in LINKS}
    free = {link: 0.0 for link in LINKS}
    events, steps, now = [], [], 0.0

    def send():
        for link in LINKS:
            waiting[link].sort(key=lambda m: (m.rank, m.index))
        busy = True
        while busy:
            busy = False
            for link in LINKS:
                if waiting[link] and flying[link] < WINDOW:
                    move = waiting[link].pop(0)
                    flying[link] += 1
                    free[link] = max(now, free[link]) + move.count
                    events.append((free[link] + LAG, move.index, move))
                    steps.append((now, "send", move))
                    busy = True

    send()
    while events:
        events.sort(key=lambda e: e[:2])
        now, _, move = events.pop(0)
        flying[move.link] -= 1
        steps.append((now, "take", move))
        for nxt in move.after:
            if nxt.link == "d":
                steps.append((now, "send", nxt))
            else:
                waiting[nxt.link].append(nxt)
        send()
    assert not any(waiting.values())
    return steps


def kernel(sizes, a_hbm, b_hbm, pairs_hbm, plist_hbm, own_hbm, out_hbm, *scratch):
    n_x, n_y, n_a, n_b, n_own = sizes
    a_slot, b_slot = scratch[0:8], scratch[8:16]
    (acc, pairs_own, plist_own, own, pairs_in, plist_in, table_v, table,
     send_sem, recv_sem, list_send, list_recv, load_sem, out_sem) = scratch[16:]
    y = lax.axis_index("rows")
    p = lax.axis_index("ksplit")
    x, core = p // 2, p % 2
    moves = plan(n_a, n_b)
    steps = order(moves)

    def at(dx, other):
        return 2 * ((x + dx) % n_x) + (core + other) % 2

    target = {
        "+x": {"ksplit": at(1, 0)},
        "-x": {"ksplit": at(n_x - 1, 0)},
        "+y": {"rows": (y + 1) % n_y},
        "-y": {"rows": (y + n_y - 1) % n_y},
        "d": {"ksplit": at(0, 1)},
    }

    loads = [
        pltpu.make_async_copy(b_hbm, b_slot[0], load_sem.at[0]),
        pltpu.make_async_copy(a_hbm, a_slot[0], load_sem.at[1]),
        pltpu.make_async_copy(pairs_hbm, pairs_own, load_sem.at[2]),
        pltpu.make_async_copy(plist_hbm, plist_own, load_sem.at[3]),
        pltpu.make_async_copy(own_hbm, own, load_sem.at[4]),
    ]
    for load in loads:
        load.start()

    peers = [(dx, other) for dx in range(n_x) for other in range(2) if (dx, other) != (0, 0)]
    barrier = pltpu.get_barrier_semaphore()
    for dx, other in peers:
        pl.semaphore_signal(barrier, inc=1, device_id={"ksplit": at(dx, other)}, device_id_type=MESH)
    for link in ("+y", "-y"):
        pl.semaphore_signal(barrier, inc=1, device_id=target[link], device_id_type=MESH)
    pl.semaphore_wait(barrier, len(peers) + 2)

    def copy(move, row):
        holder = (row + move.shift + 2 * n_y) % n_y
        half = HALF_SET // 2
        quarter = (n_b - HALF_SET) // 4
        base = {"all": 0, "h": (holder % 2) * half, "q": HALF_SET + holder * quarter}[move.part]
        where = pl.ds(base + move.first, move.count)
        slots = a_slot if move.kind == "a" else b_slot
        src = slots[2 * move.src]
        dst = slots[2 * move.dst + (1 if move.link == "d" else 0)]
        return pltpu.make_async_remote_copy(
            src_ref=src.at[where],
            dst_ref=dst.at[where],
            send_sem=send_sem.at[move.index],
            recv_sem=recv_sem.at[move.index],
            device_id=target[move.link],
            device_id_type=MESH,
        )

    def start(move):
        copy(move, y).start()

    def receive(move):
        row = {"+y": y + n_y - 1, "-y": y + 1}.get(move.link, y)
        copy(move, row).wait_recv()

    def lists(number, dx, other):
        mine, theirs = 2 * dx + other, 2 * ((n_x - dx) % n_x) + other
        where = pl.ds(pl.multiple_of(((x + dx) % n_x) * 128, 128), 128)
        pair = []
        for which, (src, dst) in enumerate(((pairs_own, pairs_in), (plist_own, plist_in))):
            pair.append(pltpu.make_async_remote_copy(
                src_ref=src.at[:, where],
                dst_ref=dst.at[theirs],
                send_sem=list_send.at[2 * number + which],
                recv_sem=list_recv.at[2 * number + which],
                device_id={"ksplit": at(dx, other)},
                device_id_type=MESH,
            ))
        return pair

    def lists_in(number, dx, other):
        mine = 2 * dx + other
        pair = []
        back = peers.index(((n_x - dx) % n_x, other))
        for which, (src, dst) in enumerate(((pairs_own, pairs_in), (plist_own, plist_in))):
            pair.append(pltpu.make_async_remote_copy(
                src_ref=src.at[:, pl.ds(0, 128)],
                dst_ref=dst.at[mine],
                send_sem=list_send.at[2 * back + which],
                recv_sem=list_recv.at[2 * back + which],
                device_id={"ksplit": at(dx, other)},
                device_id_type=MESH,
            ))
        return pair

    def run(step):
        _, what, move = step
        if what == "send":
            start(move)
        else:
            receive(move)

    for load in loads:
        load.wait()
    while steps[0][1] == "send":
        run(steps.pop(0))
    for number, (dx, other) in enumerate(peers):
        for one in lists(number, dx, other):
            one.start()
    for move in moves:
        if move.dep is None and move.link == "d":
            start(move)

    def make_table():
        mine = pl.ds(pl.multiple_of(x * 128, 128), 128)
        pairs_in[0] = pairs_own[:, mine]
        plist_in[0] = plist_own[:, mine]
        for number, (dx, other) in enumerate(peers):
            for one in lists_in(number, dx, other):
                one.wait_recv()
        key = plist_in[:, 0, :] * 65536 + plist_in[:, 1, :]
        code = pairs_in[:, 0, :] * 65536 + pairs_in[:, 1, :]
        wanted = own[0:1, :] * 65536 + own[1:2, :]
        wanted = jnp.concatenate([wanted] * (128 // n_own), axis=1)
        wanted = jnp.broadcast_to(wanted, key.shape)

        def turn(_, state):
            key, code, found = state
            found = jnp.where(key == wanted, code, found)
            return pltpu.roll(key, 1, 1), pltpu.roll(code, 1, 1), found

        _, _, found = lax.fori_loop(0, 128, turn, (key, code, jnp.zeros_like(code)), unroll=8)
        table_v[0] = found // 65536
        table_v[1] = found % 65536

    def use_table():
        to_smem = pltpu.make_async_copy(table_v, table, load_sem.at[5])
        to_smem.start()
        to_smem.wait()

    def product(slot, c):
        left = a_slot[slot][table[0, slot, c]]
        right = b_slot[slot][table[1, slot, c]]
        part = jnp.dot(left, right, preferred_element_type=jnp.float32)
        return part.astype(jnp.bfloat16).astype(jnp.float32)

    def compute(slots, part=(0, 1), first=False, last=False):
        def step(i, _):
            for u in range(UNROLL):
                c = i * UNROLL + u
                total = product(slots[0], c)
                for slot in slots[1:]:
                    total = total + product(slot, c)
                acc[c] = total if first else acc[c] + total
            if last:
                out_copy(i).start()
            return 0

        count = n_own // UNROLL // part[1]
        lax.fori_loop(part[0] * count, (part[0] + 1) * count, step, 0)

    def out_copy(i):
        where = pl.ds(i * UNROLL, UNROLL)
        return pltpu.make_async_copy(acc.at[where], out_hbm.at[where], out_sem.at[i])

    def from_partner(dx):
        for move in moves:
            if move.link == "d" and move.dst == dx:
                receive(move)

    jobs = []
    queued = set()
    stage = 0

    def ready(dx):
        return not [s for s in steps if s[1] == "take" and s[2].dst == dx]

    while steps:
        now = steps[0][0]
        if stage == 0 and now > TABLE_AT:
            make_table()
            stage = 1
        elif stage == 1 and now > TABLE_AT + 3.0:
            use_table()
            from_partner(0)
            jobs += [functools.partial(compute, (0, 1), (i, 2), first=True) for i in range(2)]
            stage = 2
        run(steps.pop(0))
        while steps and steps[0][1] == "send":
            run(steps.pop(0))
        for dx in (1, 3):
            if dx not in queued and ready(dx):
                queued.add(dx)
                jobs.append(functools.partial(from_partner, dx))
                jobs += [functools.partial(compute, (2 * dx, 2 * dx + 1), (i, 2)) for i in range(2)]
        if jobs:
            jobs.pop(0)()
    for job in jobs:
        job()
    compute((4,))
    from_partner(2)
    compute((5,), last=True)

    for number, (dx, other) in enumerate(peers):
        for one in lists(number, dx, other):
            one.wait_send()
    for move in moves:
        copy(move, y).wait_send()
    for i in range(n_own // UNROLL):
        out_copy(i).wait()


def solution(mesh):
    n_y = mesh.shape["rows"]
    n_x = mesh.shape["ksplit"] // 2
    row_spec = P(("batch", "rows"), "ksplit")
    col_spec = P(("batch", "ksplit"))

    def device_step(a_loc, b_loc, pair_loc, plist_loc, cidx_loc):
        a, b = a_loc[0, 0], b_loc[0]
        n_a, size, _ = a.shape
        n_b = b.shape[0]
        n_own = cidx_loc.shape[2]
        n_part = plist_loc.shape[2]
        assert n_x == 4 and n_y == 4 and n_part == n_x * 128 and 128 % n_own == 0
        moves = plan(n_a, n_b)
        in_hbm = pl.BlockSpec(memory_space=pltpu.HBM)
        out = pl.pallas_call(
            functools.partial(kernel, (n_x, n_y, n_a, n_b, n_own)),
            out_shape=jax.ShapeDtypeStruct((n_own, size, size), jnp.float32),
            in_specs=[in_hbm] * 5,
            out_specs=in_hbm,
            scratch_shapes=[pltpu.VMEM((n_a, size, size), jnp.bfloat16)] * 8
            + [pltpu.VMEM((n_b, size, size), jnp.bfloat16)] * 8
            + [
                pltpu.VMEM((n_own, size, size), jnp.float32),
                pltpu.VMEM((2, n_part), jnp.int32),
                pltpu.VMEM((2, n_part), jnp.int32),
                pltpu.VMEM((2, n_own), jnp.int32),
                pltpu.VMEM((8, 2, 128), jnp.int32),
                pltpu.VMEM((8, 2, 128), jnp.int32),
                pltpu.VMEM((2, 8, 128), jnp.int32),
                pltpu.SMEM((2, 8, 128), jnp.int32),
                pltpu.SemaphoreType.DMA((len(moves),)),
                pltpu.SemaphoreType.DMA((len(moves),)),
                pltpu.SemaphoreType.DMA((14,)),
                pltpu.SemaphoreType.DMA((14,)),
                pltpu.SemaphoreType.DMA((6,)),
                pltpu.SemaphoreType.DMA((n_own // UNROLL,)),
            ],
            compiler_params=pltpu.CompilerParams(
                collective_id=0, has_side_effects=True, vmem_limit_bytes=VMEM
            ),
        )(a, b, pair_loc[0, 0, :, 0, :].T, plist_loc[0, 0].T, cidx_loc[0, 0].T)
        return out[None, None]

    return jax.shard_map(
        device_step, mesh=mesh, in_specs=(row_spec, col_spec, row_spec, row_spec, row_spec), out_specs=row_spec, check_vma=False
    )
```

```python
import functools

import jax
import jax.numpy as jnp
from jax import lax
from jax.experimental import pallas as pl
from jax.experimental.pallas import tpu as pltpu
from jax.sharding import PartitionSpec as P

MESH = pl.DeviceIdType.MESH
HALF_SET = 32
CHUNK = 4
A_CHUNK = 4
WINDOW = 1
GAP = 0.2
TABLE_AT = 9.0
VMEM = 67_000_000
LAG = 3.0
UNROLL = 8


class Move:
    def __init__(self, link, kind, src, dst, part, first, count, dep, shift, rank):
        self.link, self.kind, self.src, self.dst = link, kind, src, dst
        self.part, self.first, self.count, self.dep = part, first, count, dep
        self.shift = shift
        self.rank = rank
        self.after = []


def cut(first, count, size):
    return [(first + at, min(size, count - at)) for at in range(0, count, size)]


def plan(n_a, n_b):
    half = HALF_SET // 2
    quarter = (n_b - HALF_SET) // 4
    h1, h2 = cut(0, half // 2, CHUNK), cut(half // 2, half - half // 2, CHUNK)
    q1, q2 = cut(0, quarter // 2, CHUNK), cut(quarter // 2, quarter - quarter // 2, CHUNK)
    a1, a2 = cut(0, n_a // 2, A_CHUNK), cut(n_a // 2, n_a - n_a // 2, A_CHUNK)
    moves = []

    def add(link, kind, src, dst, part, piece, dep, rank, shift=0):
        move = Move(link, kind, src, dst, part, piece[0], piece[1], dep, shift, rank)
        move.index = len(moves)
        moves.append(move)
        if dep is not None:
            dep.after.append(move)
        if link != "d":
            row = {"+y": -1, "-y": 1}.get(link, 0) + shift
            add("d", kind, dst, dst, part, piece, move, 0, row)
        return move

    def spread(move, piece, far):
        if move.part == "h":
            add("+y" if piece in h1 else "-y", "b", move.dst, move.dst, "h", piece, move, far + 1)
            return
        up = add("+y", "b", move.dst, move.dst, "q", piece, move, far)
        down = add("-y", "b", move.dst, move.dst, "q", piece, move, far)
        if piece in q1:
            add("+y", "b", move.dst, move.dst, "q", piece, up, far + 2, -1)
        else:
            add("-y", "b", move.dst, move.dst, "q", piece, down, far + 2, 1)

    for kind, count in (("b", n_b), ("a", n_a)):
        add("d", kind, 0, 0, "all", (0, count), None, 9)
    for link, slot in (("+x", 3), ("-x", 1)):
        first = link == "+x"
        for part, one, two in (("q", q1, q2), ("h", h1, h2)):
            keep = one if first else two
            for piece in (one + two) if first else (two + one):
                move = add(link, "b", 0, slot, part, piece, None, 0)
                spread(move, piece, 0)
                if piece in keep:
                    spread(add(link, "b", slot, 2, part, piece, move, 1), piece, 3)
        keep = a1 if first else a2
        for piece in (a1 + a2) if first else (a2 + a1):
            move = add(link, "a", 0, slot, "all", piece, None, 2)
            if piece in keep:
                add(link, "a", slot, 2, "all", piece, move, 3)
    return moves


LINKS = ("+x", "-x", "+y", "-y")


def order(moves):
    waiting = {link: [m for m in moves if m.link == link and m.dep is None] for link in LINKS}
    flying = {link: [] for link in LINKS}
    free = {link: 0.0 for link in LINKS}
    events, steps, now = [], [], 0.0

    def send():
        for link in LINKS:
            waiting[link].sort(key=lambda m: (m.rank, m.index))
        busy = True
        while busy:
            busy = False
            for link in LINKS:
                if waiting[link] and len([m for m in flying[link] if m.leaves > now]) < WINDOW:
                    move = waiting[link].pop(0)
                    if len(flying[link]) == WINDOW:
                        steps.append((now, "sent", flying[link].pop(0)))
                    flying[link].append(move)
                    free[link] = max(now, free[link]) + move.count
                    move.leaves = free[link] + GAP
                    events.append((move.leaves, 0, move.index, move))
                    events.append((free[link] + LAG, 1, move.index, move))
                    steps.append((now, "send", move))
                    busy = True

    send()
    while events:
        events.sort(key=lambda e: e[:3])
        now, come, _, move = events.pop(0)
        if come:
            steps.append((now, "take", move))
            for nxt in move.after:
                if nxt.link == "d":
                    steps.append((now, "send", nxt))
                else:
                    waiting[nxt.link].append(nxt)
        send()
    assert not any(waiting.values())
    return steps


def kernel(sizes, a_hbm, b_hbm, pairs_hbm, plist_hbm, own_hbm, out_hbm, *scratch):
    n_x, n_y, n_a, n_b, n_own = sizes
    a_slot, b_slot = scratch[0:8], scratch[8:16]
    (acc, pairs_own, plist_own, own, pairs_in, plist_in, table_v, table,
     send_sem, recv_sem, list_send, list_recv, load_sem, out_sem) = scratch[16:]
    y = lax.axis_index("rows")
    p = lax.axis_index("ksplit")
    x, core = p // 2, p % 2
    moves = plan(n_a, n_b)
    steps = order(moves)

    def at(dx, other):
        return 2 * ((x + dx) % n_x) + (core + other) % 2

    target = {
        "+x": {"ksplit": at(1, 0)},
        "-x": {"ksplit": at(n_x - 1, 0)},
        "+y": {"rows": (y + 1) % n_y},
        "-y": {"rows": (y + n_y - 1) % n_y},
        "d": {"ksplit": at(0, 1)},
    }

    loads = [
        pltpu.make_async_copy(b_hbm, b_slot[0], load_sem.at[0]),
        pltpu.make_async_copy(a_hbm, a_slot[0], load_sem.at[1]),
        pltpu.make_async_copy(pairs_hbm, pairs_own, load_sem.at[2]),
        pltpu.make_async_copy(plist_hbm, plist_own, load_sem.at[3]),
        pltpu.make_async_copy(own_hbm, own, load_sem.at[4]),
    ]
    for load in loads:
        load.start()

    peers = [(dx, other) for dx in range(n_x) for other in range(2) if (dx, other) != (0, 0)]
    barrier = pltpu.get_barrier_semaphore()
    for dx, other in peers:
        pl.semaphore_signal(barrier, inc=1, device_id={"ksplit": at(dx, other)}, device_id_type=MESH)
    for link in ("+y", "-y"):
        pl.semaphore_signal(barrier, inc=1, device_id=target[link], device_id_type=MESH)
    pl.semaphore_wait(barrier, len(peers) + 2)

    def copy(move, row):
        holder = (row + move.shift + 2 * n_y) % n_y
        half = HALF_SET // 2
        quarter = (n_b - HALF_SET) // 4
        base = {"all": 0, "h": (holder % 2) * half, "q": HALF_SET + holder * quarter}[move.part]
        where = pl.ds(base + move.first, move.count)
        slots = a_slot if move.kind == "a" else b_slot
        src = slots[2 * move.src]
        dst = slots[2 * move.dst + (1 if move.link == "d" else 0)]
        return pltpu.make_async_remote_copy(
            src_ref=src.at[where],
            dst_ref=dst.at[where],
            send_sem=send_sem.at[move.index],
            recv_sem=recv_sem.at[move.index],
            device_id=target[move.link],
            device_id_type=MESH,
        )

    def start(move):
        copy(move, y).start()

    def receive(move):
        row = {"+y": y + n_y - 1, "-y": y + 1}.get(move.link, y)
        copy(move, row).wait_recv()

    def lists(number, dx, other):
        mine, theirs = 2 * dx + other, 2 * ((n_x - dx) % n_x) + other
        where = pl.ds(pl.multiple_of(((x + dx) % n_x) * 128, 128), 128)
        pair = []
        for which, (src, dst) in enumerate(((pairs_own, pairs_in), (plist_own, plist_in))):
            pair.append(pltpu.make_async_remote_copy(
                src_ref=src.at[:, where],
                dst_ref=dst.at[theirs],
                send_sem=list_send.at[2 * number + which],
                recv_sem=list_recv.at[2 * number + which],
                device_id={"ksplit": at(dx, other)},
                device_id_type=MESH,
            ))
        return pair

    def lists_in(number, dx, other):
        mine = 2 * dx + other
        pair = []
        back = peers.index(((n_x - dx) % n_x, other))
        for which, (src, dst) in enumerate(((pairs_own, pairs_in), (plist_own, plist_in))):
            pair.append(pltpu.make_async_remote_copy(
                src_ref=src.at[:, pl.ds(0, 128)],
                dst_ref=dst.at[mine],
                send_sem=list_send.at[2 * back + which],
                recv_sem=list_recv.at[2 * back + which],
                device_id={"ksplit": at(dx, other)},
                device_id_type=MESH,
            ))
        return pair

    sent = set()

    def run(step):
        _, what, move = step
        if what == "send":
            start(move)
        elif what == "sent":
            copy(move, y).wait_send()
            sent.add(move.index)
        else:
            receive(move)

    for load in loads:
        load.wait()
    while steps[0][1] == "send":
        run(steps.pop(0))
    for number, (dx, other) in enumerate(peers):
        for one in lists(number, dx, other):
            one.start()
    for move in moves:
        if move.dep is None and move.link == "d":
            start(move)

    def make_table():
        mine = pl.ds(pl.multiple_of(x * 128, 128), 128)
        pairs_in[0] = pairs_own[:, mine]
        plist_in[0] = plist_own[:, mine]
        for number, (dx, other) in enumerate(peers):
            for one in lists_in(number, dx, other):
                one.wait_recv()
        key = plist_in[:, 0, :] * 65536 + plist_in[:, 1, :]
        code = pairs_in[:, 0, :] * 65536 + pairs_in[:, 1, :]
        wanted = own[0:1, :] * 65536 + own[1:2, :]
        wanted = jnp.concatenate([wanted] * (128 // n_own), axis=1)
        wanted = jnp.broadcast_to(wanted, key.shape)

        def turn(_, state):
            key, code, found = state
            found = jnp.where(key == wanted, code, found)
            return pltpu.roll(key, 1, 1), pltpu.roll(code, 1, 1), found

        _, _, found = lax.fori_loop(0, 128, turn, (key, code, jnp.zeros_like(code)), unroll=8)
        table_v[0] = found // 65536
        table_v[1] = found % 65536

    def use_table():
        to_smem = pltpu.make_async_copy(table_v, table, load_sem.at[5])
        to_smem.start()
        to_smem.wait()

    def product(slot, c):
        left = a_slot[slot][table[0, slot, c]]
        right = b_slot[slot][table[1, slot, c]]
        part = jnp.dot(left, right, preferred_element_type=jnp.float32)
        return part.astype(jnp.bfloat16).astype(jnp.float32)

    def compute(slots, part=(0, 1), first=False, last=False):
        def step(i, _):
            for u in range(UNROLL):
                c = i * UNROLL + u
                total = product(slots[0], c)
                for slot in slots[1:]:
                    total = total + product(slot, c)
                acc[c] = total if first else acc[c] + total
            if last:
                out_copy(i).start()
            return 0

        count = n_own // UNROLL // part[1]
        lax.fori_loop(part[0] * count, (part[0] + 1) * count, step, 0)

    def out_copy(i):
        where = pl.ds(i * UNROLL, UNROLL)
        return pltpu.make_async_copy(acc.at[where], out_hbm.at[where], out_sem.at[i])

    def from_partner(dx):
        for move in moves:
            if move.link == "d" and move.dst == dx:
                receive(move)

    jobs = []
    queued = set()
    stage = 0

    def ready(dx):
        return not [s for s in steps if s[1] == "take" and s[2].dst == dx]

    while steps:
        now = steps[0][0]
        if stage == 0 and now > TABLE_AT:
            make_table()
            stage = 1
        elif stage == 1 and now > TABLE_AT + 3.0:
            use_table()
            from_partner(0)
            jobs += [functools.partial(compute, (0, 1), (i, 2), first=True) for i in range(2)]
            stage = 2
        run(steps.pop(0))
        while steps and steps[0][1] != "take":
            run(steps.pop(0))
        for dx in (1, 3):
            if dx not in queued and ready(dx):
                queued.add(dx)
                jobs.append(functools.partial(from_partner, dx))
                jobs += [functools.partial(compute, (2 * dx, 2 * dx + 1), (i, 2)) for i in range(2)]
        if jobs:
            jobs.pop(0)()
    for job in jobs:
        job()
    compute((4,))
    from_partner(2)
    compute((5,), last=True)

    for number, (dx, other) in enumerate(peers):
        for one in lists(number, dx, other):
            one.wait_send()
    for move in moves:
        if move.index not in sent:
            copy(move, y).wait_send()
    for i in range(n_own // UNROLL):
        out_copy(i).wait()


def solution(mesh):
    n_y = mesh.shape["rows"]
    n_x = mesh.shape["ksplit"] // 2
    row_spec = P(("batch", "rows"), "ksplit")
    col_spec = P(("batch", "ksplit"))

    def device_step(a_loc, b_loc, pair_loc, plist_loc, cidx_loc):
        a, b = a_loc[0, 0], b_loc[0]
        n_a, size, _ = a.shape
        n_b = b.shape[0]
        n_own = cidx_loc.shape[2]
        n_part = plist_loc.shape[2]
        assert n_x == 4 and n_y == 4 and n_part == n_x * 128 and 128 % n_own == 0
        moves = plan(n_a, n_b)
        in_hbm = pl.BlockSpec(memory_space=pltpu.HBM)
        out = pl.pallas_call(
            functools.partial(kernel, (n_x, n_y, n_a, n_b, n_own)),
            out_shape=jax.ShapeDtypeStruct((n_own, size, size), jnp.float32),
            in_specs=[in_hbm] * 5,
            out_specs=in_hbm,
            scratch_shapes=[pltpu.VMEM((n_a, size, size), jnp.bfloat16)] * 8
            + [pltpu.VMEM((n_b, size, size), jnp.bfloat16)] * 8
            + [
                pltpu.VMEM((n_own, size, size), jnp.float32),
                pltpu.VMEM((2, n_part), jnp.int32),
                pltpu.VMEM((2, n_part), jnp.int32),
                pltpu.VMEM((2, n_own), jnp.int32),
                pltpu.VMEM((8, 2, 128), jnp.int32),
                pltpu.VMEM((8, 2, 128), jnp.int32),
                pltpu.VMEM((2, 8, 128), jnp.int32),
                pltpu.SMEM((2, 8, 128), jnp.int32),
                pltpu.SemaphoreType.DMA((len(moves),)),
                pltpu.SemaphoreType.DMA((len(moves),)),
                pltpu.SemaphoreType.DMA((14,)),
                pltpu.SemaphoreType.DMA((14,)),
                pltpu.SemaphoreType.DMA((6,)),
                pltpu.SemaphoreType.DMA((n_own // UNROLL,)),
            ],
            compiler_params=pltpu.CompilerParams(
                collective_id=0, has_side_effects=True, vmem_limit_bytes=VMEM
            ),
        )(a, b, pair_loc[0, 0, :, 0, :].T, plist_loc[0, 0].T, cidx_loc[0, 0].T)
        return out[None, None]

    return jax.shard_map(
        device_step, mesh=mesh, in_specs=(row_spec, col_spec, row_spec, row_spec, row_spec), out_specs=row_spec, check_vma=False
    )
```

```python
import functools

import jax
import jax.numpy as jnp
from jax import lax
from jax.experimental import pallas as pl
from jax.experimental.pallas import tpu as pltpu
from jax.sharding import PartitionSpec as P

MESH = pl.DeviceIdType.MESH
HALF_SET = 64
CHUNK = 4
A_CHUNK = 4
WINDOW = 3
TABLE_AT = 9.0
VMEM = 67_000_000
LAG = 3.0
UNROLL = 8


class Move:
    def __init__(self, link, kind, src, dst, part, first, count, dep, shift, rank):
        self.link, self.kind, self.src, self.dst = link, kind, src, dst
        self.part, self.first, self.count, self.dep = part, first, count, dep
        self.shift = shift
        self.rank = rank
        self.after = []


def cut(first, count, size):
    return [(first + at, min(size, count - at)) for at in range(0, count, size)]


def plan(n_a, n_b):
    half = HALF_SET // 2
    quarter = (n_b - HALF_SET) // 4
    h1, h2 = cut(0, half // 2, CHUNK), cut(half // 2, half - half // 2, CHUNK)
    q1, q2 = cut(0, quarter // 2, CHUNK), cut(quarter // 2, quarter - quarter // 2, CHUNK)
    a1, a2 = cut(0, n_a // 2, A_CHUNK), cut(n_a // 2, n_a - n_a // 2, A_CHUNK)
    moves = []

    def add(link, kind, src, dst, part, piece, dep, rank, shift=0):
        move = Move(link, kind, src, dst, part, piece[0], piece[1], dep, shift, rank)
        move.index = len(moves)
        moves.append(move)
        if dep is not None:
            dep.after.append(move)
        if link != "d":
            row = {"+y": -1, "-y": 1}.get(link, 0) + shift
            add("d", kind, dst, dst, part, piece, move, 0, row)
        return move

    def spread(move, piece, far):
        if move.part == "h":
            add("+y" if piece in h1 else "-y", "b", move.dst, move.dst, "h", piece, move, far + 1)
            return
        up = add("+y", "b", move.dst, move.dst, "q", piece, move, far)
        down = add("-y", "b", move.dst, move.dst, "q", piece, move, far)
        if piece in q1:
            add("+y", "b", move.dst, move.dst, "q", piece, up, far + 2, -1)
        else:
            add("-y", "b", move.dst, move.dst, "q", piece, down, far + 2, 1)

    for kind, count in (("b", n_b), ("a", n_a)):
        add("d", kind, 0, 0, "all", (0, count), None, 9)
    for link, slot in (("+x", 3), ("-x", 1)):
        first = link == "+x"
        for part, one, two in (("q", q1, q2), ("h", h1, h2)):
            keep = one if first else two
            for piece in (one + two) if first else (two + one):
                move = add(link, "b", 0, slot, part, piece, None, 0)
                spread(move, piece, 0)
                if piece in keep:
                    spread(add(link, "b", slot, 2, part, piece, move, 1), piece, 3)
        keep = a1 if first else a2
        for piece in (a1 + a2) if first else (a2 + a1):
            move = add(link, "a", 0, slot, "all", piece, None, 2)
            if piece in keep:
                add(link, "a", slot, 2, "all", piece, move, 3)
    return moves


LINKS = ("+x", "-x", "+y", "-y")


def order(moves):
    waiting = {link: [m for m in moves if m.link == link and m.dep is None] for link in LINKS}
    flying = {link: 0 for link in LINKS}
    free = {link: 0.0 for link in LINKS}
    events, steps, now = [], [], 0.0

    def send():
        for link in LINKS:
            waiting[link].sort(key=lambda m: (m.rank, m.index))
        busy = True
        while busy:
            busy = False
            for link in LINKS:
                if waiting[link] and flying[link] < WINDOW:
                    move = waiting[link].pop(0)
                    flying[link] += 1
                    free[link] = max(now, free[link]) + move.count
                    events.append((free[link] + LAG, move.index, move))
                    steps.append((now, "send", move))
                    busy = True

    send()
    while events:
        events.sort(key=lambda e: e[:2])
        now, _, move = events.pop(0)
        flying[move.link] -= 1
        steps.append((now, "take", move))
        for nxt in move.after:
            if nxt.link == "d":
                steps.append((now, "send", nxt))
            else:
                waiting[nxt.link].append(nxt)
        send()
    assert not any(waiting.values())
    return steps


def kernel(sizes, a_hbm, b_hbm, pairs_hbm, plist_hbm, own_hbm, out_hbm, *scratch):
    n_x, n_y, n_a, n_b, n_own = sizes
    a_slot, b_slot = scratch[0:8], scratch[8:16]
    (acc, pairs_own, plist_own, own, pairs_in, plist_in, table_v, table,
     send_sem, recv_sem, list_send, list_recv, load_sem, out_sem) = scratch[16:]
    y = lax.axis_index("rows")
    p = lax.axis_index("ksplit")
    x, core = p // 2, p % 2
    moves = plan(n_a, n_b)
    steps = order(moves)

    def at(dx, other):
        return 2 * ((x + dx) % n_x) + (core + other) % 2

    target = {
        "+x": {"ksplit": at(1, 0)},
        "-x": {"ksplit": at(n_x - 1, 0)},
        "+y": {"rows": (y + 1) % n_y},
        "-y": {"rows": (y + n_y - 1) % n_y},
        "d": {"ksplit": at(0, 1)},
    }

    loads = [
        pltpu.make_async_copy(b_hbm, b_slot[0], load_sem.at[0]),
        pltpu.make_async_copy(a_hbm, a_slot[0], load_sem.at[1]),
        pltpu.make_async_copy(pairs_hbm, pairs_own, load_sem.at[2]),
        pltpu.make_async_copy(plist_hbm, plist_own, load_sem.at[3]),
        pltpu.make_async_copy(own_hbm, own, load_sem.at[4]),
    ]
    for load in loads:
        load.start()

    peers = [(dx, other) for dx in range(n_x) for other in range(2) if (dx, other) != (0, 0)]
    barrier = pltpu.get_barrier_semaphore()
    for dx, other in peers:
        pl.semaphore_signal(barrier, inc=1, device_id={"ksplit": at(dx, other)}, device_id_type=MESH)
    for link in ("+y", "-y"):
        pl.semaphore_signal(barrier, inc=1, device_id=target[link], device_id_type=MESH)
    pl.semaphore_wait(barrier, len(peers) + 2)

    def copy(move, row):
        holder = (row + move.shift + 2 * n_y) % n_y
        half = HALF_SET // 2
        quarter = (n_b - HALF_SET) // 4
        base = {"all": 0, "h": (holder % 2) * half, "q": HALF_SET + holder * quarter}[move.part]
        where = pl.ds(base + move.first, move.count)
        slots = a_slot if move.kind == "a" else b_slot
        src = slots[2 * move.src]
        dst = slots[2 * move.dst + (1 if move.link == "d" else 0)]
        return pltpu.make_async_remote_copy(
            src_ref=src.at[where],
            dst_ref=dst.at[where],
            send_sem=send_sem.at[move.index],
            recv_sem=recv_sem.at[move.index],
            device_id=target[move.link],
            device_id_type=MESH,
        )

    def start(move):
        copy(move, y).start()

    def receive(move):
        row = {"+y": y + n_y - 1, "-y": y + 1}.get(move.link, y)
        copy(move, row).wait_recv()

    def lists(number, dx, other):
        mine, theirs = 2 * dx + other, 2 * ((n_x - dx) % n_x) + other
        where = pl.ds(pl.multiple_of(((x + dx) % n_x) * 128, 128), 128)
        pair = []
        for which, (src, dst) in enumerate(((pairs_own, pairs_in), (plist_own, plist_in))):
            pair.append(pltpu.make_async_remote_copy(
                src_ref=src.at[:, where],
                dst_ref=dst.at[theirs],
                send_sem=list_send.at[2 * number + which],
                recv_sem=list_recv.at[2 * number + which],
                device_id={"ksplit": at(dx, other)},
                device_id_type=MESH,
            ))
        return pair

    def lists_in(number, dx, other):
        mine = 2 * dx + other
        pair = []
        back = peers.index(((n_x - dx) % n_x, other))
        for which, (src, dst) in enumerate(((pairs_own, pairs_in), (plist_own, plist_in))):
            pair.append(pltpu.make_async_remote_copy(
                src_ref=src.at[:, pl.ds(0, 128)],
                dst_ref=dst.at[mine],
                send_sem=list_send.at[2 * back + which],
                recv_sem=list_recv.at[2 * back + which],
                device_id={"ksplit": at(dx, other)},
                device_id_type=MESH,
            ))
        return pair

    def run(step):
        _, what, move = step
        if what == "send":
            start(move)
        else:
            receive(move)

    for load in loads:
        load.wait()
    while steps[0][1] == "send":
        run(steps.pop(0))
    for number, (dx, other) in enumerate(peers):
        for one in lists(number, dx, other):
            one.start()
    for move in moves:
        if move.dep is None and move.link == "d":
            start(move)

    def make_table():
        mine = pl.ds(pl.multiple_of(x * 128, 128), 128)
        pairs_in[0] = pairs_own[:, mine]
        plist_in[0] = plist_own[:, mine]
        for number, (dx, other) in enumerate(peers):
            for one in lists_in(number, dx, other):
                one.wait_recv()
        key = plist_in[:, 0, :] * 65536 + plist_in[:, 1, :]
        code = pairs_in[:, 0, :] * 65536 + pairs_in[:, 1, :]
        wanted = own[0:1, :] * 65536 + own[1:2, :]
        wanted = jnp.concatenate([wanted] * (128 // n_own), axis=1)
        wanted = jnp.broadcast_to(wanted, key.shape)

        def turn(_, state):
            key, code, found = state
            found = jnp.where(key == wanted, code, found)
            return pltpu.roll(key, 1, 1), pltpu.roll(code, 1, 1), found

        _, _, found = lax.fori_loop(0, 128, turn, (key, code, jnp.zeros_like(code)), unroll=8)
        table_v[0] = found // 65536
        table_v[1] = found % 65536

    def use_table():
        to_smem = pltpu.make_async_copy(table_v, table, load_sem.at[5])
        to_smem.start()
        to_smem.wait()

    def product(slot, c):
        left = a_slot[slot][table[0, slot, c]]
        right = b_slot[slot][table[1, slot, c]]
        part = jnp.dot(left, right, preferred_element_type=jnp.float32)
        return part.astype(jnp.bfloat16).astype(jnp.float32)

    def compute(slots, part=(0, 1), first=False, last=False):
        def step(i, _):
            for u in range(UNROLL):
                c = i * UNROLL + u
                total = product(slots[0], c)
                for slot in slots[1:]:
                    total = total + product(slot, c)
                acc[c] = total if first else acc[c] + total
            if last:
                out_copy(i).start()
            return 0

        count = n_own // UNROLL // part[1]
        lax.fori_loop(part[0] * count, (part[0] + 1) * count, step, 0)

    def out_copy(i):
        where = pl.ds(i * UNROLL, UNROLL)
        return pltpu.make_async_copy(acc.at[where], out_hbm.at[where], out_sem.at[i])

    def from_partner(dx):
        for move in moves:
            if move.link == "d" and move.dst == dx:
                receive(move)

    jobs = []
    queued = set()
    stage = 0

    def ready(dx):
        return not [s for s in steps if s[1] == "take" and s[2].dst == dx]

    while steps:
        now = steps[0][0]
        if stage == 0 and now > TABLE_AT:
            make_table()
            stage = 1
        elif stage == 1 and now > TABLE_AT + 3.0:
            use_table()
            from_partner(0)
            jobs += [functools.partial(compute, (0, 1), (i, 2), first=True) for i in range(2)]
            stage = 2
        run(steps.pop(0))
        while steps and steps[0][1] == "send":
            run(steps.pop(0))
        for dx in (1, 3):
            if dx not in queued and ready(dx):
                queued.add(dx)
                jobs.append(functools.partial(from_partner, dx))
                jobs += [functools.partial(compute, (2 * dx, 2 * dx + 1), (i, 2)) for i in range(2)]
        if jobs:
            jobs.pop(0)()
    for job in jobs:
        job()
    compute((4,))
    from_partner(2)
    compute((5,), last=True)

    for number, (dx, other) in enumerate(peers):
        for one in lists(number, dx, other):
            one.wait_send()
    for move in moves:
        copy(move, y).wait_send()
    for i in range(n_own // UNROLL):
        out_copy(i).wait()


def solution(mesh):
    n_y = mesh.shape["rows"]
    n_x = mesh.shape["ksplit"] // 2
    row_spec = P(("batch", "rows"), "ksplit")
    col_spec = P(("batch", "ksplit"))

    def device_step(a_loc, b_loc, pair_loc, plist_loc, cidx_loc):
        a, b = a_loc[0, 0], b_loc[0]
        n_a, size, _ = a.shape
        n_b = b.shape[0]
        n_own = cidx_loc.shape[2]
        n_part = plist_loc.shape[2]
        assert n_x == 4 and n_y == 4 and n_part == n_x * 128 and 128 % n_own == 0
        moves = plan(n_a, n_b)
        in_hbm = pl.BlockSpec(memory_space=pltpu.HBM)
        out = pl.pallas_call(
            functools.partial(kernel, (n_x, n_y, n_a, n_b, n_own)),
            out_shape=jax.ShapeDtypeStruct((n_own, size, size), jnp.float32),
            in_specs=[in_hbm] * 5,
            out_specs=in_hbm,
            scratch_shapes=[pltpu.VMEM((n_a, size, size), jnp.bfloat16)] * 8
            + [pltpu.VMEM((n_b, size, size), jnp.bfloat16)] * 8
            + [
                pltpu.VMEM((n_own, size, size), jnp.float32),
                pltpu.VMEM((2, n_part), jnp.int32),
                pltpu.VMEM((2, n_part), jnp.int32),
                pltpu.VMEM((2, n_own), jnp.int32),
                pltpu.VMEM((8, 2, 128), jnp.int32),
                pltpu.VMEM((8, 2, 128), jnp.int32),
                pltpu.VMEM((2, 8, 128), jnp.int32),
                pltpu.SMEM((2, 8, 128), jnp.int32),
                pltpu.SemaphoreType.DMA((len(moves),)),
                pltpu.SemaphoreType.DMA((len(moves),)),
                pltpu.SemaphoreType.DMA((14,)),
                pltpu.SemaphoreType.DMA((14,)),
                pltpu.SemaphoreType.DMA((6,)),
                pltpu.SemaphoreType.DMA((n_own // UNROLL,)),
            ],
            compiler_params=pltpu.CompilerParams(
                collective_id=0, has_side_effects=True, vmem_limit_bytes=VMEM
            ),
        )(a, b, pair_loc[0, 0, :, 0, :].T, plist_loc[0, 0].T, cidx_loc[0, 0].T)
        return out[None, None]

    return jax.shard_map(
        device_step, mesh=mesh, in_specs=(row_spec, col_spec, row_spec, row_spec, row_spec), out_specs=row_spec, check_vma=False
    )
```

```python
import functools

import jax
import jax.numpy as jnp
from jax import lax
from jax.experimental import pallas as pl
from jax.experimental.pallas import tpu as pltpu
from jax.sharding import PartitionSpec as P

MESH = pl.DeviceIdType.MESH
HALF_SET = 32
CHUNK = 8
A_CHUNK = 8
WINDOW = 2
TABLE_AT = 9.0
VMEM = 67_000_000
LAG = 3.0
UNROLL = 8


class Move:
    def __init__(self, link, kind, src, dst, part, first, count, dep, shift, rank):
        self.link, self.kind, self.src, self.dst = link, kind, src, dst
        self.part, self.first, self.count, self.dep = part, first, count, dep
        self.shift = shift
        self.rank = rank
        self.after = []


def cut(first, count, size):
    return [(first + at, min(size, count - at)) for at in range(0, count, size)]


def plan(n_a, n_b):
    half = HALF_SET // 2
    quarter = (n_b - HALF_SET) // 4
    h1, h2 = cut(0, half // 2, CHUNK), cut(half // 2, half - half // 2, CHUNK)
    q1, q2 = cut(0, quarter // 2, CHUNK), cut(quarter // 2, quarter - quarter // 2, CHUNK)
    a1, a2 = cut(0, n_a // 2, A_CHUNK), cut(n_a // 2, n_a - n_a // 2, A_CHUNK)
    moves = []

    def add(link, kind, src, dst, part, piece, dep, rank, shift=0):
        move = Move(link, kind, src, dst, part, piece[0], piece[1], dep, shift, rank)
        move.index = len(moves)
        moves.append(move)
        if dep is not None:
            dep.after.append(move)
        if link != "d":
            row = {"+y": -1, "-y": 1}.get(link, 0) + shift
            add("d", kind, dst, dst, part, piece, move, 0, row)
        return move

    def spread(move, piece, far):
        if move.part == "h":
            add("+y" if piece in h1 else "-y", "b", move.dst, move.dst, "h", piece, move, far + 1)
            return
        up = add("+y", "b", move.dst, move.dst, "q", piece, move, far)
        down = add("-y", "b", move.dst, move.dst, "q", piece, move, far)
        if piece in q1:
            add("+y", "b", move.dst, move.dst, "q", piece, up, far + 2, -1)
        else:
            add("-y", "b", move.dst, move.dst, "q", piece, down, far + 2, 1)

    for kind, count in (("b", n_b), ("a", n_a)):
        add("d", kind, 0, 0, "all", (0, count), None, 9)
    for link, slot in (("+x", 3), ("-x", 1)):
        first = link == "+x"
        for part, one, two in (("q", q1, q2), ("h", h1, h2)):
            keep = one if first else two
            for piece in (one + two) if first else (two + one):
                move = add(link, "b", 0, slot, part, piece, None, 0)
                spread(move, piece, 0)
                if piece in keep:
                    spread(add(link, "b", slot, 2, part, piece, move, 1), piece, 3)
        keep = a1 if first else a2
        for piece in (a1 + a2) if first else (a2 + a1):
            move = add(link, "a", 0, slot, "all", piece, None, 2)
            if piece in keep:
                add(link, "a", slot, 2, "all", piece, move, 3)
    return moves


LINKS = ("+x", "-x", "+y", "-y")


def order(moves):
    waiting = {link: [m for m in moves if m.link == link and m.dep is None] for link in LINKS}
    flying = {link: 0 for link in LINKS}
    free = {link: 0.0 for link in LINKS}
    events, steps, now = [], [], 0.0

    def send():
        for link in LINKS:
            waiting[link].sort(key=lambda m: (m.rank, m.index))
        busy = True
        while busy:
            busy = False
            for link in LINKS:
                if waiting[link] and flying[link] < WINDOW:
                    move = waiting[link].pop(0)
                    flying[link] += 1
                    free[link] = max(now, free[link]) + move.count
                    events.append((free[link] + LAG, move.index, move))
                    steps.append((now, "send", move))
                    busy = True

    send()
    while events:
        events.sort(key=lambda e: e[:2])
        now, _, move = events.pop(0)
        flying[move.link] -= 1
        steps.append((now, "take", move))
        for nxt in move.after:
            if nxt.link == "d":
                steps.append((now, "send", nxt))
            else:
                waiting[nxt.link].append(nxt)
        send()
    assert not any(waiting.values())
    return steps


def kernel(sizes, a_hbm, b_hbm, pairs_hbm, plist_hbm, own_hbm, out_hbm, *scratch):
    n_x, n_y, n_a, n_b, n_own = sizes
    a_slot, b_slot = scratch[0:8], scratch[8:16]
    (acc, pairs_own, plist_own, own, pairs_in, plist_in, table_v, table,
     send_sem, recv_sem, list_send, list_recv, load_sem, out_sem) = scratch[16:]
    y = lax.axis_index("rows")
    p = lax.axis_index("ksplit")
    x, core = p // 2, p % 2
    moves = plan(n_a, n_b)
    steps = order(moves)

    def at(dx, other):
        return 2 * ((x + dx) % n_x) + (core + other) % 2

    target = {
        "+x": {"ksplit": at(1, 0)},
        "-x": {"ksplit": at(n_x - 1, 0)},
        "+y": {"rows": (y + 1) % n_y},
        "-y": {"rows": (y + n_y - 1) % n_y},
        "d": {"ksplit": at(0, 1)},
    }

    loads = [
        pltpu.make_async_copy(b_hbm, b_slot[0], load_sem.at[0]),
        pltpu.make_async_copy(a_hbm, a_slot[0], load_sem.at[1]),
        pltpu.make_async_copy(pairs_hbm, pairs_own, load_sem.at[2]),
        pltpu.make_async_copy(plist_hbm, plist_own, load_sem.at[3]),
        pltpu.make_async_copy(own_hbm, own, load_sem.at[4]),
    ]
    for load in loads:
        load.start()

    peers = [(dx, other) for dx in range(n_x) for other in range(2) if (dx, other) != (0, 0)]
    barrier = pltpu.get_barrier_semaphore()
    for dx, other in peers:
        pl.semaphore_signal(barrier, inc=1, device_id={"ksplit": at(dx, other)}, device_id_type=MESH)
    for link in ("+y", "-y"):
        pl.semaphore_signal(barrier, inc=1, device_id=target[link], device_id_type=MESH)
    pl.semaphore_wait(barrier, len(peers) + 2)

    def copy(move, row):
        holder = (row + move.shift + 2 * n_y) % n_y
        half = HALF_SET // 2
        quarter = (n_b - HALF_SET) // 4
        base = {"all": 0, "h": (holder % 2) * half, "q": HALF_SET + holder * quarter}[move.part]
        where = pl.ds(base + move.first, move.count)
        slots = a_slot if move.kind == "a" else b_slot
        src = slots[2 * move.src]
        dst = slots[2 * move.dst + (1 if move.link == "d" else 0)]
        return pltpu.make_async_remote_copy(
            src_ref=src.at[where],
            dst_ref=dst.at[where],
            send_sem=send_sem.at[move.index],
            recv_sem=recv_sem.at[move.index],
            device_id=target[move.link],
            device_id_type=MESH,
        )

    def start(move):
        copy(move, y).start()

    def receive(move):
        row = {"+y": y + n_y - 1, "-y": y + 1}.get(move.link, y)
        copy(move, row).wait_recv()

    def lists(number, dx, other):
        mine, theirs = 2 * dx + other, 2 * ((n_x - dx) % n_x) + other
        where = pl.ds(pl.multiple_of(((x + dx) % n_x) * 128, 128), 128)
        pair = []
        for which, (src, dst) in enumerate(((pairs_own, pairs_in), (plist_own, plist_in))):
            pair.append(pltpu.make_async_remote_copy(
                src_ref=src.at[:, where],
                dst_ref=dst.at[theirs],
                send_sem=list_send.at[2 * number + which],
                recv_sem=list_recv.at[2 * number + which],
                device_id={"ksplit": at(dx, other)},
                device_id_type=MESH,
            ))
        return pair

    def lists_in(number, dx, other):
        mine = 2 * dx + other
        pair = []
        back = peers.index(((n_x - dx) % n_x, other))
        for which, (src, dst) in enumerate(((pairs_own, pairs_in), (plist_own, plist_in))):
            pair.append(pltpu.make_async_remote_copy(
                src_ref=src.at[:, pl.ds(0, 128)],
                dst_ref=dst.at[mine],
                send_sem=list_send.at[2 * back + which],
                recv_sem=list_recv.at[2 * back + which],
                device_id={"ksplit": at(dx, other)},
                device_id_type=MESH,
            ))
        return pair

    def run(step):
        _, what, move = step
        if what == "send":
            start(move)
        else:
            receive(move)

    for load in loads:
        load.wait()
    while steps[0][1] == "send":
        run(steps.pop(0))
    for number, (dx, other) in enumerate(peers):
        for one in lists(number, dx, other):
            one.start()
    for move in moves:
        if move.dep is None and move.link == "d":
            start(move)

    def make_table():
        mine = pl.ds(pl.multiple_of(x * 128, 128), 128)
        pairs_in[0] = pairs_own[:, mine]
        plist_in[0] = plist_own[:, mine]
        for number, (dx, other) in enumerate(peers):
            for one in lists_in(number, dx, other):
                one.wait_recv()
        key = plist_in[:, 0, :] * 65536 + plist_in[:, 1, :]
        code = pairs_in[:, 0, :] * 65536 + pairs_in[:, 1, :]
        wanted = own[0:1, :] * 65536 + own[1:2, :]
        wanted = jnp.concatenate([wanted] * (128 // n_own), axis=1)
        wanted = jnp.broadcast_to(wanted, key.shape)

        def turn(_, state):
            key, code, found = state
            found = jnp.where(key == wanted, code, found)
            return pltpu.roll(key, 1, 1), pltpu.roll(code, 1, 1), found

        _, _, found = lax.fori_loop(0, 128, turn, (key, code, jnp.zeros_like(code)), unroll=8)
        table_v[0] = found // 65536
        table_v[1] = found % 65536

    def use_table():
        to_smem = pltpu.make_async_copy(table_v, table, load_sem.at[5])
        to_smem.start()
        to_smem.wait()

    def product(slot, c):
        left = a_slot[slot][table[0, slot, c]]
        right = b_slot[slot][table[1, slot, c]]
        part = jnp.dot(left, right, preferred_element_type=jnp.float32)
        return part.astype(jnp.bfloat16).astype(jnp.float32)

    def compute(slots, part=(0, 1), first=False, last=False):
        def step(i, _):
            for u in range(UNROLL):
                c = i * UNROLL + u
                total = product(slots[0], c)
                for slot in slots[1:]:
                    total = total + product(slot, c)
                acc[c] = total if first else acc[c] + total
            if last:
                out_copy(i).start()
            return 0

        count = n_own // UNROLL // part[1]
        lax.fori_loop(part[0] * count, (part[0] + 1) * count, step, 0)

    def out_copy(i):
        where = pl.ds(i * UNROLL, UNROLL)
        return pltpu.make_async_copy(acc.at[where], out_hbm.at[where], out_sem.at[i])

    def from_partner(dx):
        for move in moves:
            if move.link == "d" and move.dst == dx:
                receive(move)

    jobs = []
    queued = set()
    stage = 0

    def ready(dx):
        return not [s for s in steps if s[1] == "take" and s[2].dst == dx]

    while steps:
        now = steps[0][0]
        if stage == 0 and now > TABLE_AT:
            make_table()
            stage = 1
        elif stage == 1 and now > TABLE_AT + 3.0:
            use_table()
            from_partner(0)
            jobs += [functools.partial(compute, (0, 1), (i, 2), first=True) for i in range(2)]
            stage = 2
        run(steps.pop(0))
        while steps and steps[0][1] == "send":
            run(steps.pop(0))
        for dx in (1, 3):
            if dx not in queued and ready(dx):
                queued.add(dx)
                jobs.append(functools.partial(from_partner, dx))
                jobs += [functools.partial(compute, (2 * dx, 2 * dx + 1), (i, 2)) for i in range(2)]
        if jobs:
            jobs.pop(0)()
    for job in jobs:
        job()
    compute((4,))
    from_partner(2)
    compute((5,), last=True)

    for number, (dx, other) in enumerate(peers):
        for one in lists(number, dx, other):
            one.wait_send()
    for move in moves:
        copy(move, y).wait_send()
    for i in range(n_own // UNROLL):
        out_copy(i).wait()


def solution(mesh):
    n_y = mesh.shape["rows"]
    n_x = mesh.shape["ksplit"] // 2
    row_spec = P(("batch", "rows"), "ksplit")
    col_spec = P(("batch", "ksplit"))

    def device_step(a_loc, b_loc, pair_loc, plist_loc, cidx_loc):
        a, b = a_loc[0, 0], b_loc[0]
        n_a, size, _ = a.shape
        n_b = b.shape[0]
        n_own = cidx_loc.shape[2]
        n_part = plist_loc.shape[2]
        assert n_x == 4 and n_y == 4 and n_part == n_x * 128 and 128 % n_own == 0
        moves = plan(n_a, n_b)
        in_hbm = pl.BlockSpec(memory_space=pltpu.HBM)
        out = pl.pallas_call(
            functools.partial(kernel, (n_x, n_y, n_a, n_b, n_own)),
            out_shape=jax.ShapeDtypeStruct((n_own, size, size), jnp.float32),
            in_specs=[in_hbm] * 5,
            out_specs=in_hbm,
            scratch_shapes=[pltpu.VMEM((n_a, size, size), jnp.bfloat16)] * 8
            + [pltpu.VMEM((n_b, size, size), jnp.bfloat16)] * 8
            + [
                pltpu.VMEM((n_own, size, size), jnp.float32),
                pltpu.VMEM((2, n_part), jnp.int32),
                pltpu.VMEM((2, n_part), jnp.int32),
                pltpu.VMEM((2, n_own), jnp.int32),
                pltpu.VMEM((8, 2, 128), jnp.int32),
                pltpu.VMEM((8, 2, 128), jnp.int32),
                pltpu.VMEM((2, 8, 128), jnp.int32),
                pltpu.SMEM((2, 8, 128), jnp.int32),
                pltpu.SemaphoreType.DMA((len(moves),)),
                pltpu.SemaphoreType.DMA((len(moves),)),
                pltpu.SemaphoreType.DMA((14,)),
                pltpu.SemaphoreType.DMA((14,)),
                pltpu.SemaphoreType.DMA((6,)),
                pltpu.SemaphoreType.DMA((n_own // UNROLL,)),
            ],
            compiler_params=pltpu.CompilerParams(
                collective_id=0, has_side_effects=True, vmem_limit_bytes=VMEM
            ),
        )(a, b, pair_loc[0, 0, :, 0, :].T, plist_loc[0, 0].T, cidx_loc[0, 0].T)
        return out[None, None]

    return jax.shard_map(
        device_step, mesh=mesh, in_specs=(row_spec, col_spec, row_spec, row_spec, row_spec), out_specs=row_spec, check_vma=False
    )
```

```python
import functools

import jax
import jax.numpy as jnp
from jax import lax
from jax.experimental import pallas as pl
from jax.experimental.pallas import tpu as pltpu
from jax.sharding import PartitionSpec as P

MESH = pl.DeviceIdType.MESH
HALF_SET = 40
CHUNK = 5
A_CHUNK = 4
WINDOW = 6
TABLE_AT = 6.0
VMEM = 67_000_000
LAG = 3.0
PIECES = 4
UNROLL = 8


class Move:
    def __init__(self, link, kind, src, dst, part, first, count, dep, shift, rank):
        self.link, self.kind, self.src, self.dst = link, kind, src, dst
        self.part, self.first, self.count, self.dep = part, first, count, dep
        self.shift = shift
        self.rank = rank
        self.after = []


def cut(first, count, size):
    return [(first + at, min(size, count - at)) for at in range(0, count, size)]


def plan(n_a, n_b):
    half = HALF_SET // 2
    quarter = (n_b - HALF_SET) // 4
    h1, h2 = cut(0, half // 2, CHUNK), cut(half // 2, half - half // 2, CHUNK)
    q1, q2 = cut(0, quarter // 2, CHUNK), cut(quarter // 2, quarter - quarter // 2, CHUNK)
    a1, a2 = cut(0, n_a // 2, A_CHUNK), cut(n_a // 2, n_a - n_a // 2, A_CHUNK)
    moves = []

    def add(link, kind, src, dst, part, piece, dep, rank, shift=0):
        move = Move(link, kind, src, dst, part, piece[0], piece[1], dep, shift, rank)
        move.index = len(moves)
        moves.append(move)
        if dep is not None:
            dep.after.append(move)
        if link != "d":
            row = {"+y": -1, "-y": 1}.get(link, 0) + shift
            add("d", kind, dst, dst, part, piece, move, 0, row)
        return move

    def spread(move, piece, far):
        if move.part == "h":
            add("+y" if piece in h1 else "-y", "b", move.dst, move.dst, "h", piece, move, far + 1)
            return
        up = add("+y", "b", move.dst, move.dst, "q", piece, move, far)
        down = add("-y", "b", move.dst, move.dst, "q", piece, move, far)
        if piece in q1:
            add("+y", "b", move.dst, move.dst, "q", piece, up, far + 2, -1)
        else:
            add("-y", "b", move.dst, move.dst, "q", piece, down, far + 2, 1)

    for kind, count in (("b", n_b), ("a", n_a)):
        add("d", kind, 0, 0, "all", (0, count), None, 9)
    for link, slot in (("+x", 3), ("-x", 1)):
        first = link == "+x"
        for part, one, two in (("q", q1, q2), ("h", h1, h2)):
            keep = one if first else two
            for piece in (one + two) if first else (two + one):
                move = add(link, "b", 0, slot, part, piece, None, 0)
                spread(move, piece, 0)
                if piece in keep:
                    spread(add(link, "b", slot, 2, part, piece, move, 1), piece, 3)
        keep = a1 if first else a2
        for piece in (a1 + a2) if first else (a2 + a1):
            move = add(link, "a", 0, slot, "all", piece, None, 2)
            if piece in keep:
                add(link, "a", slot, 2, "all", piece, move, 3)
    return moves


LINKS = ("+x", "-x", "+y", "-y")


def order(moves):
    waiting = {link: [m for m in moves if m.link == link and m.dep is None] for link in LINKS}
    flying = {link: 0 for link in LINKS}
    free = {link: 0.0 for link in LINKS}
    events, steps, now = [], [], 0.0

    def send():
        for link in LINKS:
            waiting[link].sort(key=lambda m: (m.rank, m.index))
        busy = True
        while busy:
            busy = False
            for link in LINKS:
                if waiting[link] and flying[link] < WINDOW:
                    move = waiting[link].pop(0)
                    flying[link] += 1
                    free[link] = max(now, free[link]) + move.count
                    events.append((free[link] + LAG, move.index, move))
                    steps.append((now, "send", move))
                    busy = True

    send()
    while events:
        events.sort(key=lambda e: e[:2])
        now, _, move = events.pop(0)
        flying[move.link] -= 1
        steps.append((now, "take", move))
        for nxt in move.after:
            if nxt.link == "d":
                steps.append((now, "send", nxt))
            else:
                waiting[nxt.link].append(nxt)
        send()
    assert not any(waiting.values())
    return steps


def kernel(sizes, a_hbm, b_hbm, pairs_hbm, plist_hbm, own_hbm, out_hbm, *scratch):
    n_x, n_y, n_a, n_b, n_own = sizes
    a_slot, b_slot = scratch[0:8], scratch[8:16]
    (acc, pairs_own, plist_own, own, pairs_in, plist_in, table_v, table,
     send_sem, recv_sem, list_send, list_recv, load_sem, out_sem) = scratch[16:]
    y = lax.axis_index("rows")
    p = lax.axis_index("ksplit")
    x, core = p // 2, p % 2
    moves = plan(n_a, n_b)
    steps = order(moves)

    def at(dx, other):
        return 2 * ((x + dx) % n_x) + (core + other) % 2

    target = {
        "+x": {"ksplit": at(1, 0)},
        "-x": {"ksplit": at(n_x - 1, 0)},
        "+y": {"rows": (y + 1) % n_y},
        "-y": {"rows": (y + n_y - 1) % n_y},
        "d": {"ksplit": at(0, 1)},
    }

    loads = [
        pltpu.make_async_copy(b_hbm, b_slot[0], load_sem.at[0]),
        pltpu.make_async_copy(a_hbm, a_slot[0], load_sem.at[1]),
        pltpu.make_async_copy(pairs_hbm, pairs_own, load_sem.at[2]),
        pltpu.make_async_copy(plist_hbm, plist_own, load_sem.at[3]),
        pltpu.make_async_copy(own_hbm, own, load_sem.at[4]),
    ]
    for load in loads:
        load.start()

    peers = [(dx, other) for dx in range(n_x) for other in range(2) if (dx, other) != (0, 0)]
    barrier = pltpu.get_barrier_semaphore()
    for dx, other in peers:
        pl.semaphore_signal(barrier, inc=1, device_id={"ksplit": at(dx, other)}, device_id_type=MESH)
    for link in ("+y", "-y"):
        pl.semaphore_signal(barrier, inc=1, device_id=target[link], device_id_type=MESH)
    pl.semaphore_wait(barrier, len(peers) + 2)

    def copy(move, row):
        holder = (row + move.shift + 2 * n_y) % n_y
        half = HALF_SET // 2
        quarter = (n_b - HALF_SET) // 4
        base = {"all": 0, "h": (holder % 2) * half, "q": HALF_SET + holder * quarter}[move.part]
        where = pl.ds(base + move.first, move.count)
        slots = a_slot if move.kind == "a" else b_slot
        src = slots[2 * move.src]
        dst = slots[2 * move.dst + (1 if move.link == "d" else 0)]
        return pltpu.make_async_remote_copy(
            src_ref=src.at[where],
            dst_ref=dst.at[where],
            send_sem=send_sem.at[move.index],
            recv_sem=recv_sem.at[move.index],
            device_id=target[move.link],
            device_id_type=MESH,
        )

    def start(move):
        copy(move, y).start()

    def receive(move):
        row = {"+y": y + n_y - 1, "-y": y + 1}.get(move.link, y)
        copy(move, row).wait_recv()

    def lists(number, dx, other):
        mine, theirs = 2 * dx + other, 2 * ((n_x - dx) % n_x) + other
        where = pl.ds(pl.multiple_of(((x + dx) % n_x) * 128, 128), 128)
        pair = []
        for which, (src, dst) in enumerate(((pairs_own, pairs_in), (plist_own, plist_in))):
            pair.append(pltpu.make_async_remote_copy(
                src_ref=src.at[:, where],
                dst_ref=dst.at[theirs],
                send_sem=list_send.at[2 * number + which],
                recv_sem=list_recv.at[2 * number + which],
                device_id={"ksplit": at(dx, other)},
                device_id_type=MESH,
            ))
        return pair

    def lists_in(number, dx, other):
        mine = 2 * dx + other
        pair = []
        back = peers.index(((n_x - dx) % n_x, other))
        for which, (src, dst) in enumerate(((pairs_own, pairs_in), (plist_own, plist_in))):
            pair.append(pltpu.make_async_remote_copy(
                src_ref=src.at[:, pl.ds(0, 128)],
                dst_ref=dst.at[mine],
                send_sem=list_send.at[2 * back + which],
                recv_sem=list_recv.at[2 * back + which],
                device_id={"ksplit": at(dx, other)},
                device_id_type=MESH,
            ))
        return pair

    def run(step):
        _, what, move = step
        if what == "send":
            start(move)
        else:
            receive(move)

    for load in loads[2:]:
        load.wait()
    for number, (dx, other) in enumerate(peers):
        for one in lists(number, dx, other):
            one.start()
    for load in loads[:2]:
        load.wait()
    while steps[0][1] == "send":
        run(steps.pop(0))
    for move in moves:
        if move.dep is None and move.link == "d":
            start(move)

    def make_table():
        mine = pl.ds(pl.multiple_of(x * 128, 128), 128)
        pairs_in[0] = pairs_own[:, mine]
        plist_in[0] = plist_own[:, mine]
        for number, (dx, other) in enumerate(peers):
            for one in lists_in(number, dx, other):
                one.wait_recv()
        key = plist_in[:, 0, :] * 65536 + plist_in[:, 1, :]
        code = pairs_in[:, 0, :] * 65536 + pairs_in[:, 1, :]
        wanted = own[0:1, :] * 65536 + own[1:2, :]
        wanted = jnp.concatenate([wanted] * (128 // n_own), axis=1)
        wanted = jnp.broadcast_to(wanted, key.shape)

        def turn(_, state):
            key, code, found = state
            found = jnp.where(key == wanted, code, found)
            return pltpu.roll(key, 1, 1), pltpu.roll(code, 1, 1), found

        _, _, found = lax.fori_loop(0, 128, turn, (key, code, jnp.zeros_like(code)), unroll=8)
        table_v[0] = found // 65536
        table_v[1] = found % 65536

    def use_table():
        to_smem = pltpu.make_async_copy(table_v, table, load_sem.at[5])
        to_smem.start()
        to_smem.wait()

    def product(slot, c):
        left = a_slot[slot][table[0, slot, c]]
        right = b_slot[slot][table[1, slot, c]]
        part = jnp.dot(left, right, preferred_element_type=jnp.float32)
        return part.astype(jnp.bfloat16).astype(jnp.float32)

    def compute(slots, part=(0, 1), first=False, last=False):
        def step(i, _):
            for u in range(UNROLL):
                c = i * UNROLL + u
                total = product(slots[0], c)
                for slot in slots[1:]:
                    total = total + product(slot, c)
                acc[c] = total if first else acc[c] + total
            if last:
                out_copy(i).start()
            return 0

        count = n_own // UNROLL // part[1]
        lax.fori_loop(part[0] * count, (part[0] + 1) * count, step, 0)

    def out_copy(i):
        where = pl.ds(i * UNROLL, UNROLL)
        return pltpu.make_async_copy(acc.at[where], out_hbm.at[where], out_sem.at[i])

    def from_partner(dx):
        for move in moves:
            if move.link == "d" and move.dst == dx:
                receive(move)

    jobs = []
    queued = set()
    stage = 0

    def ready(dx):
        return not [s for s in steps if s[1] == "take" and s[2].dst == dx]

    while steps:
        now = steps[0][0]
        if stage == 0 and now > TABLE_AT:
            make_table()
            stage = 1
        elif stage == 1 and now > TABLE_AT + 3.0:
            use_table()
            from_partner(0)
            jobs += [functools.partial(compute, (0, 1), (i, PIECES), first=True) for i in range(PIECES)]
            stage = 2
        run(steps.pop(0))
        while steps and steps[0][1] == "send":
            run(steps.pop(0))
        for dx in (1, 3):
            if dx not in queued and ready(dx):
                queued.add(dx)
                jobs.append(functools.partial(from_partner, dx))
                jobs += [functools.partial(compute, (2 * dx, 2 * dx + 1), (i, PIECES)) for i in range(PIECES)]
        if jobs:
            jobs.pop(0)()
    for job in jobs:
        job()
    compute((4,))
    from_partner(2)
    compute((5,), last=True)

    for number, (dx, other) in enumerate(peers):
        for one in lists(number, dx, other):
            one.wait_send()
    for move in moves:
        copy(move, y).wait_send()
    for i in range(n_own // UNROLL):
        out_copy(i).wait()


def solution(mesh):
    n_y = mesh.shape["rows"]
    n_x = mesh.shape["ksplit"] // 2
    row_spec = P(("batch", "rows"), "ksplit")
    col_spec = P(("batch", "ksplit"))

    def device_step(a_loc, b_loc, pair_loc, plist_loc, cidx_loc):
        a, b = a_loc[0, 0], b_loc[0]
        n_a, size, _ = a.shape
        n_b = b.shape[0]
        n_own = cidx_loc.shape[2]
        n_part = plist_loc.shape[2]
        assert n_x == 4 and n_y == 4 and n_part == n_x * 128 and 128 % n_own == 0
        moves = plan(n_a, n_b)
        in_hbm = pl.BlockSpec(memory_space=pltpu.HBM)
        out = pl.pallas_call(
            functools.partial(kernel, (n_x, n_y, n_a, n_b, n_own)),
            out_shape=jax.ShapeDtypeStruct((n_own, size, size), jnp.float32),
            in_specs=[in_hbm] * 5,
            out_specs=in_hbm,
            scratch_shapes=[pltpu.VMEM((n_a, size, size), jnp.bfloat16)] * 8
            + [pltpu.VMEM((n_b, size, size), jnp.bfloat16)] * 8
            + [
                pltpu.VMEM((n_own, size, size), jnp.float32),
                pltpu.VMEM((2, n_part), jnp.int32),
                pltpu.VMEM((2, n_part), jnp.int32),
                pltpu.VMEM((2, n_own), jnp.int32),
                pltpu.VMEM((8, 2, 128), jnp.int32),
                pltpu.VMEM((8, 2, 128), jnp.int32),
                pltpu.VMEM((2, 8, 128), jnp.int32),
                pltpu.SMEM((2, 8, 128), jnp.int32),
                pltpu.SemaphoreType.DMA((len(moves),)),
                pltpu.SemaphoreType.DMA((len(moves),)),
                pltpu.SemaphoreType.DMA((14,)),
                pltpu.SemaphoreType.DMA((14,)),
                pltpu.SemaphoreType.DMA((6,)),
                pltpu.SemaphoreType.DMA((n_own // UNROLL,)),
            ],
            compiler_params=pltpu.CompilerParams(
                collective_id=0, has_side_effects=True, vmem_limit_bytes=VMEM
            ),
        )(a, b, pair_loc[0, 0, :, 0, :].T, plist_loc[0, 0].T, cidx_loc[0, 0].T)
        return out[None, None]

    return jax.shard_map(
        device_step, mesh=mesh, in_specs=(row_spec, col_spec, row_spec, row_spec, row_spec), out_specs=row_spec, check_vma=False
    )
```

```python
import functools

import jax
import jax.numpy as jnp
from jax import lax
from jax.experimental import pallas as pl
from jax.experimental.pallas import tpu as pltpu
from jax.sharding import PartitionSpec as P

MESH = pl.DeviceIdType.MESH
HALF_SET = 40
CHUNK = 5
A_CHUNK = 4
WINDOW = 6
TABLE_AT = 6.0
VMEM = 67_000_000
LAG = 3.0
LATE = (4, 5)
JOB = 0.8
PIECES = 4
UNROLL = 8


class Move:
    def __init__(self, link, kind, src, dst, part, first, count, dep, shift, rank):
        self.link, self.kind, self.src, self.dst = link, kind, src, dst
        self.part, self.first, self.count, self.dep = part, first, count, dep
        self.shift = shift
        self.rank = rank
        self.after = []


def cut(first, count, size):
    return [(first + at, min(size, count - at)) for at in range(0, count, size)]


def plan(n_a, n_b):
    half = HALF_SET // 2
    quarter = (n_b - HALF_SET) // 4
    h1, h2 = cut(0, half // 2, CHUNK), cut(half // 2, half - half // 2, CHUNK)
    q1, q2 = cut(0, quarter // 2, CHUNK), cut(quarter // 2, quarter - quarter // 2, CHUNK)
    a1, a2 = cut(0, n_a // 2, A_CHUNK), cut(n_a // 2, n_a - n_a // 2, A_CHUNK)
    moves = []

    def add(link, kind, src, dst, part, piece, dep, rank, shift=0):
        move = Move(link, kind, src, dst, part, piece[0], piece[1], dep, shift, rank)
        move.index = len(moves)
        moves.append(move)
        if dep is not None:
            dep.after.append(move)
        if link != "d":
            row = {"+y": -1, "-y": 1}.get(link, 0) + shift
            add("d", kind, dst, dst, part, piece, move, 0, row)
        return move

    def spread(move, piece, far):
        if move.part == "h":
            add("+y" if piece in h1 else "-y", "b", move.dst, move.dst, "h", piece, move, far + 1)
            return
        up = add("+y", "b", move.dst, move.dst, "q", piece, move, far)
        down = add("-y", "b", move.dst, move.dst, "q", piece, move, far)
        if piece in q1:
            add("+y", "b", move.dst, move.dst, "q", piece, up, far + 2, -1)
        else:
            add("-y", "b", move.dst, move.dst, "q", piece, down, far + 2, 1)

    for kind, count in (("b", n_b), ("a", n_a)):
        add("d", kind, 0, 0, "all", (0, count), None, 9)
    for link, slot in (("+x", 3), ("-x", 1)):
        first = link == "+x"
        for part, one, two in (("q", q1, q2), ("h", h1, h2)):
            keep = one if first else two
            for piece in (one + two) if first else (two + one):
                move = add(link, "b", 0, slot, part, piece, None, 0)
                spread(move, piece, 0)
                if piece in keep:
                    spread(add(link, "b", slot, 2, part, piece, move, 1), piece, 3)
        keep = a1 if first else a2
        for piece in (a1 + a2) if first else (a2 + a1):
            move = add(link, "a", 0, slot, "all", piece, None, 2)
            if piece in keep:
                add(link, "a", slot, 2, "all", piece, move, 3)
    return moves


LINKS = ("+x", "-x", "+y", "-y")


def order(moves):
    waiting = {link: [m for m in moves if m.link == link and m.dep is None] for link in LINKS}
    flying = {link: 0 for link in LINKS}
    free = {link: 0.0 for link in LINKS}
    events, steps, now = [], [], 0.0

    def send():
        for link in LINKS:
            waiting[link].sort(key=lambda m: (m.rank, m.index))
        busy = True
        while busy:
            busy = False
            for link in LINKS:
                if waiting[link] and flying[link] < WINDOW:
                    move = waiting[link].pop(0)
                    flying[link] += 1
                    free[link] = max(now, free[link]) + move.count
                    events.append((free[link] + LAG, move.index, move))
                    steps.append((now, "send", move))
                    busy = True

    send()
    while events:
        events.sort(key=lambda e: e[:2])
        now, _, move = events.pop(0)
        flying[move.link] -= 1
        steps.append((now, "take", move))
        for nxt in move.after:
            if nxt.link == "d":
                steps.append((now, "send", nxt))
            else:
                waiting[nxt.link].append(nxt)
        send()
    assert not any(waiting.values())
    return steps


def gather_kernel(sizes, a_hbm, b_hbm, pairs_hbm, plist_hbm, own_hbm, acc, table_v, *refs):
    n_x, n_y, n_a, n_b, n_own = sizes
    a_slot, b_slot = list(refs[0:8]), list(refs[8:16])
    for place, slot in enumerate(LATE + tuple(s for s in range(8) if s not in LATE)):
        a_slot[slot], b_slot[slot] = refs[2 * place], refs[2 * place + 1]
    (pairs_own, plist_own, own, pairs_in, plist_in, table,
     send_sem, recv_sem, list_send, list_recv, load_sem) = refs[16:]
    y = lax.axis_index("rows")
    p = lax.axis_index("ksplit")
    x, core = p // 2, p % 2
    moves = plan(n_a, n_b)
    steps = order(moves)

    def at(dx, other):
        return 2 * ((x + dx) % n_x) + (core + other) % 2

    target = {
        "+x": {"ksplit": at(1, 0)},
        "-x": {"ksplit": at(n_x - 1, 0)},
        "+y": {"rows": (y + 1) % n_y},
        "-y": {"rows": (y + n_y - 1) % n_y},
        "d": {"ksplit": at(0, 1)},
    }

    loads = [
        pltpu.make_async_copy(b_hbm, b_slot[0], load_sem.at[0]),
        pltpu.make_async_copy(a_hbm, a_slot[0], load_sem.at[1]),
        pltpu.make_async_copy(pairs_hbm, pairs_own, load_sem.at[2]),
        pltpu.make_async_copy(plist_hbm, plist_own, load_sem.at[3]),
        pltpu.make_async_copy(own_hbm, own, load_sem.at[4]),
    ]
    for load in loads:
        load.start()

    peers = [(dx, other) for dx in range(n_x) for other in range(2) if (dx, other) != (0, 0)]
    barrier = pltpu.get_barrier_semaphore()
    for dx, other in peers:
        pl.semaphore_signal(barrier, inc=1, device_id={"ksplit": at(dx, other)}, device_id_type=MESH)
    for link in ("+y", "-y"):
        pl.semaphore_signal(barrier, inc=1, device_id=target[link], device_id_type=MESH)
    pl.semaphore_wait(barrier, len(peers) + 2)

    def copy(move, row):
        holder = (row + move.shift + 2 * n_y) % n_y
        half = HALF_SET // 2
        quarter = (n_b - HALF_SET) // 4
        base = {"all": 0, "h": (holder % 2) * half, "q": HALF_SET + holder * quarter}[move.part]
        where = pl.ds(base + move.first, move.count)
        slots = a_slot if move.kind == "a" else b_slot
        src = slots[2 * move.src]
        dst = slots[2 * move.dst + (1 if move.link == "d" else 0)]
        return pltpu.make_async_remote_copy(
            src_ref=src.at[where],
            dst_ref=dst.at[where],
            send_sem=send_sem.at[move.index],
            recv_sem=recv_sem.at[move.index],
            device_id=target[move.link],
            device_id_type=MESH,
        )

    def start(move):
        copy(move, y).start()

    def receive(move):
        row = {"+y": y + n_y - 1, "-y": y + 1}.get(move.link, y)
        copy(move, row).wait_recv()

    def lists(number, dx, other):
        mine, theirs = 2 * dx + other, 2 * ((n_x - dx) % n_x) + other
        where = pl.ds(pl.multiple_of(((x + dx) % n_x) * 128, 128), 128)
        pair = []
        for which, (src, dst) in enumerate(((pairs_own, pairs_in), (plist_own, plist_in))):
            pair.append(pltpu.make_async_remote_copy(
                src_ref=src.at[:, where],
                dst_ref=dst.at[theirs],
                send_sem=list_send.at[2 * number + which],
                recv_sem=list_recv.at[2 * number + which],
                device_id={"ksplit": at(dx, other)},
                device_id_type=MESH,
            ))
        return pair

    def lists_in(number, dx, other):
        mine = 2 * dx + other
        pair = []
        back = peers.index(((n_x - dx) % n_x, other))
        for which, (src, dst) in enumerate(((pairs_own, pairs_in), (plist_own, plist_in))):
            pair.append(pltpu.make_async_remote_copy(
                src_ref=src.at[:, pl.ds(0, 128)],
                dst_ref=dst.at[mine],
                send_sem=list_send.at[2 * back + which],
                recv_sem=list_recv.at[2 * back + which],
                device_id={"ksplit": at(dx, other)},
                device_id_type=MESH,
            ))
        return pair

    def run(step):
        _, what, move = step
        if what == "send":
            start(move)
        else:
            receive(move)

    for load in loads[2:]:
        load.wait()
    for number, (dx, other) in enumerate(peers):
        for one in lists(number, dx, other):
            one.start()
    for load in loads[:2]:
        load.wait()
    while steps[0][1] == "send":
        run(steps.pop(0))
    for move in moves:
        if move.dep is None and move.link == "d":
            start(move)

    def make_table():
        mine = pl.ds(pl.multiple_of(x * 128, 128), 128)
        pairs_in[0] = pairs_own[:, mine]
        plist_in[0] = plist_own[:, mine]
        for number, (dx, other) in enumerate(peers):
            for one in lists_in(number, dx, other):
                one.wait_recv()
        key = plist_in[:, 0, :] * 65536 + plist_in[:, 1, :]
        code = pairs_in[:, 0, :] * 65536 + pairs_in[:, 1, :]
        wanted = own[0:1, :] * 65536 + own[1:2, :]
        wanted = jnp.concatenate([wanted] * (128 // n_own), axis=1)
        wanted = jnp.broadcast_to(wanted, key.shape)

        def turn(_, state):
            key, code, found = state
            found = jnp.where(key == wanted, code, found)
            return pltpu.roll(key, 1, 1), pltpu.roll(code, 1, 1), found

        _, _, found = lax.fori_loop(0, 128, turn, (key, code, jnp.zeros_like(code)), unroll=8)
        table_v[0] = found // 65536
        table_v[1] = found % 65536

    def use_table():
        to_smem = pltpu.make_async_copy(table_v, table, load_sem.at[5])
        to_smem.start()
        to_smem.wait()

    def compute(slots, part, first=False):
        def step(i, _):
            for u in range(UNROLL):
                c = i * UNROLL + u
                total = product(a_slot, b_slot, table, slots[0], c)
                for slot in slots[1:]:
                    total = total + product(a_slot, b_slot, table, slot, c)
                acc[c] = total if first else acc[c] + total
            return 0

        count = n_own // UNROLL // part[1]
        lax.fori_loop(part[0] * count, (part[0] + 1) * count, step, 0)

    def from_partner(dx):
        for move in moves:
            if move.link == "d" and move.dst == dx:
                receive(move)

    def ready(dx):
        return not [s for s in steps if s[1] == "take" and s[2].dst == dx]

    early = [dx for dx in range(n_x) if 2 * dx not in LATE]
    jobs, queued = [], set()
    stage, clock = 0, 0.0
    while steps:
        now = steps[0][0]
        if stage == 0 and now > TABLE_AT:
            make_table()
            stage = 1
        elif stage == 1 and now > TABLE_AT + 3.0:
            use_table()
            stage = 2
        for dx in early:
            if stage == 2 and dx not in queued and ready(dx):
                jobs.append((0.0, functools.partial(from_partner, dx)))
                jobs += [(JOB, functools.partial(compute, (2 * dx, 2 * dx + 1), (i, PIECES), first=not queued)) for i in range(PIECES)]
                queued.add(dx)
        clock = max(clock, now)
        run(steps.pop(0))
        while steps and steps[0][0] == now:
            run(steps.pop(0))
        until = steps[0][0] if steps else clock + 100.0
        while jobs and clock + jobs[0][0] < until + 1.0:
            cost, job = jobs.pop(0)
            job()
            clock += cost
    for _, job in jobs:
        job()
    for dx in range(n_x):
        if dx not in early:
            from_partner(dx)

    for number, (dx, other) in enumerate(peers):
        for one in lists(number, dx, other):
            one.wait_send()
    for move in moves:
        copy(move, y).wait_send()


def product(a_slot, b_slot, table, slot, c):
    left = a_slot[slot][table[0, slot, c]]
    right = b_slot[slot][table[1, slot, c]]
    part = jnp.dot(left, right, preferred_element_type=jnp.float32)
    return part.astype(jnp.bfloat16).astype(jnp.float32)


def finish_kernel(acc, table_v, *refs):
    a_slot = {slot: refs[2 * place] for place, slot in enumerate(LATE)}
    b_slot = {slot: refs[2 * place + 1] for place, slot in enumerate(LATE)}
    out_hbm, total_v, table, sem, out_sem = refs[2 * len(LATE):]
    n_own = acc.shape[0]
    to_smem = pltpu.make_async_copy(table_v, table, sem)
    to_smem.start()
    to_smem.wait()

    def out_copy(i):
        where = pl.ds(i * UNROLL, UNROLL)
        return pltpu.make_async_copy(total_v.at[where], out_hbm.at[where], out_sem.at[i])

    def step(i, _):
        for u in range(UNROLL):
            c = i * UNROLL + u
            total = None if len(LATE) == 8 else acc[c]
            for slot in LATE:
                part = product(a_slot, b_slot, table, slot, c)
                total = part if total is None else total + part
            total_v[c] = total
        out_copy(i).start()
        return 0

    lax.fori_loop(0, n_own // UNROLL, step, 0)
    for i in range(n_own // UNROLL):
        out_copy(i).wait()


def solution(mesh):
    n_y = mesh.shape["rows"]
    n_x = mesh.shape["ksplit"] // 2
    row_spec = P(("batch", "rows"), "ksplit")
    col_spec = P(("batch", "ksplit"))

    def device_step(a_loc, b_loc, pair_loc, plist_loc, cidx_loc):
        a, b = a_loc[0, 0], b_loc[0]
        n_a, size, _ = a.shape
        n_b = b.shape[0]
        n_own = cidx_loc.shape[2]
        n_part = plist_loc.shape[2]
        assert n_x == 4 and n_y == 4 and n_part == n_x * 128 and 128 % n_own == 0
        moves = plan(n_a, n_b)
        in_hbm = pl.BlockSpec(memory_space=pltpu.HBM)
        in_vmem = pl.BlockSpec(memory_space=pltpu.VMEM)
        a_shape, b_shape = (n_a, size, size), (n_b, size, size)
        operands = [
            pltpu.with_memory_space_constraint(one, pltpu.HBM)
            for one in (a, b, pair_loc[0, 0, :, 0, :].T, plist_loc[0, 0].T, cidx_loc[0, 0].T)
        ]
        state = pl.pallas_call(
            functools.partial(gather_kernel, (n_x, n_y, n_a, n_b, n_own)),
            name="gather",
            out_shape=[pltpu.VMEM((n_own, size, size), jnp.float32), pltpu.VMEM((2, 8, 128), jnp.int32)]
            + [pltpu.VMEM(a_shape, jnp.bfloat16), pltpu.VMEM(b_shape, jnp.bfloat16)] * len(LATE),
            in_specs=[in_hbm] * 5,
            out_specs=[in_vmem] * (2 + 2 * len(LATE)),
            scratch_shapes=[pltpu.VMEM(a_shape, jnp.bfloat16), pltpu.VMEM(b_shape, jnp.bfloat16)] * (8 - len(LATE))
            + [
                pltpu.VMEM((2, n_part), jnp.int32),
                pltpu.VMEM((2, n_part), jnp.int32),
                pltpu.VMEM((2, n_own), jnp.int32),
                pltpu.VMEM((8, 2, 128), jnp.int32),
                pltpu.VMEM((8, 2, 128), jnp.int32),
                pltpu.SMEM((2, 8, 128), jnp.int32),
                pltpu.SemaphoreType.DMA((len(moves),)),
                pltpu.SemaphoreType.DMA((len(moves),)),
                pltpu.SemaphoreType.DMA((14,)),
                pltpu.SemaphoreType.DMA((14,)),
                pltpu.SemaphoreType.DMA((6,)),
            ],
            compiler_params=pltpu.CompilerParams(
                collective_id=0, has_side_effects=True, vmem_limit_bytes=28 * 1024 * 1024
            ),
        )(*operands)
        out = pl.pallas_call(
            finish_kernel,
            name="finish",
            out_shape=jax.ShapeDtypeStruct((n_own, size, size), jnp.float32),
            in_specs=[in_vmem] * len(state),
            out_specs=in_hbm,
            scratch_shapes=[
                pltpu.VMEM((n_own, size, size), jnp.float32),
                pltpu.SMEM((2, 8, 128), jnp.int32),
                pltpu.SemaphoreType.DMA,
                pltpu.SemaphoreType.DMA((n_own // UNROLL,)),
            ],
            compiler_params=pltpu.CompilerParams(vmem_limit_bytes=28 * 1024 * 1024),
        )(*state)
        return out[None, None]

    return jax.shard_map(
        device_step, mesh=mesh, in_specs=(row_spec, col_spec, row_spec, row_spec, row_spec), out_specs=row_spec, check_vma=False
    )
```

```python
import functools

import jax
import jax.numpy as jnp
from jax import lax
from jax.experimental import pallas as pl
from jax.experimental.pallas import tpu as pltpu
from jax.sharding import PartitionSpec as P

MESH = pl.DeviceIdType.MESH
HALF_SET = 48
CHUNK = 4
A_CHUNK = 4
A_GATE = 0
B_GATE = 0
SLACK = 2.0
FEED_SLACK = 1.0
VMEM = 67_000_000
LAG = 3.0
LATE = (4, 5)
JOB = 0.8
PIECES = 4
UNROLL = 8


class Move:
    def __init__(self, link, kind, src, dst, part, first, count, dep, shift, rank):
        self.link, self.kind, self.src, self.dst = link, kind, src, dst
        self.part, self.first, self.count, self.dep = part, first, count, dep
        self.shift = shift
        self.rank = rank
        self.after = []


def cut(first, count, size):
    return [(first + at, min(size, count - at)) for at in range(0, count, size)]


def plan(n_a, n_b):
    half = HALF_SET // 2
    quarter = (n_b - HALF_SET) // 4
    h1, h2 = cut(0, half // 2, CHUNK), cut(half // 2, half - half // 2, CHUNK)
    q1, q2 = cut(0, quarter // 2, CHUNK), cut(quarter // 2, quarter - quarter // 2, CHUNK)
    a1, a2 = cut(0, n_a // 2, A_CHUNK), cut(n_a // 2, n_a - n_a // 2, A_CHUNK)
    moves = []

    def add(link, kind, src, dst, part, piece, dep, rank, shift=0):
        move = Move(link, kind, src, dst, part, piece[0], piece[1], dep, shift, rank)
        move.index = len(moves)
        moves.append(move)
        if dep is not None:
            dep.after.append(move)
        if link != "d":
            row = {"+y": -1, "-y": 1}.get(link, 0) + shift
            add("d", kind, dst, dst, part, piece, move, 0, row)
        return move

    def spread(move, piece, far):
        if move.part == "h":
            add("+y" if piece in h1 else "-y", "b", move.dst, move.dst, "h", piece, move, far + 1)
            return
        up = add("+y", "b", move.dst, move.dst, "q", piece, move, far)
        down = add("-y", "b", move.dst, move.dst, "q", piece, move, far)
        if piece in q1:
            add("+y", "b", move.dst, move.dst, "q", piece, up, far + 2, -1)
        else:
            add("-y", "b", move.dst, move.dst, "q", piece, down, far + 2, 1)

    for kind, count in (("b", n_b), ("a", n_a), ("l", 1)):
        add("d", kind, 0, 0, "all", (0, count), None, 9)
    listed = set()
    for link, slot in (("+x", 3), ("-x", 1)):
        first = link == "+x"
        for part, one, two in (("q", q1, q2), ("h", h1, h2)):
            keep = one if first else two
            for piece in (one + two) if first else (two + one):
                move = add(link, "b", 0, slot, part, piece, None, 0)
                spread(move, piece, 0)
                if piece in keep:
                    spread(add(link, "b", slot, 2, part, piece, move, 1), piece, 3)
                if slot not in listed:
                    listed.add(slot)
                    lists = add(link, "l", 0, slot, "all", (0, 1), None, 0)
                    if first:
                        add(link, "l", slot, 2, "all", (0, 1), lists, 1)
        keep = a1 if first else a2
        mine = [m for m in moves if m.link == link and m.src == 0 and m.kind == "b"]
        gate = mine[-1 - (A_GATE if first else B_GATE)]
        for piece in (a1 + a2) if first else (a2 + a1):
            move = add(link, "a", 0, slot, "all", piece, gate, 2)
            if piece in keep:
                add(link, "a", slot, 2, "all", piece, move, 3)
    return moves


LINKS = ("+x", "-x", "+y", "-y")


def slack(move):
    feeds = [m for m in move.after if m.link != "d"]
    if move.link in ("+x", "-x"):
        return 0.0 if feeds else SLACK
    return FEED_SLACK if feeds else SLACK


def order(moves):
    free = {link: 0.0 for link in LINKS}
    events, steps, now = [], [], 0.0

    def send(move):
        steps.append((now, "send", move))
        if move.link != "d":
            free[move.link] = max(now, free[move.link]) + (0.3 if move.kind == "l" else move.count)
            events.append((free[move.link] + LAG + slack(move), move.index, move))

    for move in moves:
        if move.dep is None and move.link != "d":
            send(move)
    while events:
        events.sort(key=lambda e: e[:2])
        now, _, move = events.pop(0)
        steps.append((now, "take", move))
        for nxt in sorted(move.after, key=lambda m: (m.link == "d", m.rank)):
            send(nxt)
    return steps


def gather_kernel(sizes, a_hbm, b_hbm, pairs_hbm, plist_hbm, own_hbm, acc, table_v, *refs):
    n_x, n_y, n_a, n_b, n_own = sizes
    a_slot, b_slot = list(refs[0:8]), list(refs[8:16])
    for place, slot in enumerate(LATE + tuple(s for s in range(8) if s not in LATE)):
        a_slot[slot], b_slot[slot] = refs[2 * place], refs[2 * place + 1]
    l_slot = refs[16:24]
    own, table, send_sem, recv_sem, load_sem = refs[24:]
    y = lax.axis_index("rows")
    p = lax.axis_index("ksplit")
    x, core = p // 2, p % 2
    moves = plan(n_a, n_b)
    steps = order(moves)

    def at(dx, other):
        return 2 * ((x + dx) % n_x) + (core + other) % 2

    target = {
        "+x": {"ksplit": at(1, 0)},
        "-x": {"ksplit": at(n_x - 1, 0)},
        "+y": {"rows": (y + 1) % n_y},
        "-y": {"rows": (y + n_y - 1) % n_y},
        "d": {"ksplit": at(0, 1)},
    }

    loads = [
        pltpu.make_async_copy(b_hbm, b_slot[0], load_sem.at[0]),
        pltpu.make_async_copy(a_hbm, a_slot[0], load_sem.at[1]),
        pltpu.make_async_copy(pairs_hbm, l_slot[0].at[0], load_sem.at[2]),
        pltpu.make_async_copy(plist_hbm, l_slot[0].at[1], load_sem.at[3]),
        pltpu.make_async_copy(own_hbm, own, load_sem.at[4]),
    ]
    for load in loads:
        load.start()

    barrier = pltpu.get_barrier_semaphore()
    for device in target.values():
        pl.semaphore_signal(barrier, inc=1, device_id=device, device_id_type=MESH)
    pl.semaphore_wait(barrier, len(target))

    def copy(move, row):
        holder = (row + move.shift + 2 * n_y) % n_y
        half = HALF_SET // 2
        quarter = (n_b - HALF_SET) // 4
        base = {"all": 0, "h": (holder % 2) * half, "q": HALF_SET + holder * quarter}[move.part]
        where = pl.ds(base + move.first, move.count)
        slots = {"a": a_slot, "b": b_slot, "l": l_slot}[move.kind]
        src = slots[2 * move.src]
        dst = slots[2 * move.dst + (1 if move.link == "d" else 0)]
        if move.kind != "l":
            src, dst = src.at[where], dst.at[where]
        return pltpu.make_async_remote_copy(
            src_ref=src,
            dst_ref=dst,
            send_sem=send_sem.at[move.index],
            recv_sem=recv_sem.at[move.index],
            device_id=target[move.link],
            device_id_type=MESH,
        )

    def start(move):
        copy(move, y).start()

    def receive(move):
        row = {"+y": y + n_y - 1, "-y": y + 1}.get(move.link, y)
        copy(move, row).wait_recv()

    def run(step):
        _, what, move = step
        if what == "send":
            start(move)
        else:
            receive(move)

    for load in loads:
        load.wait()
    while steps[0][1] == "send":
        run(steps.pop(0))
    for move in moves:
        if move.dep is None and move.link == "d":
            start(move)

    def make_table():
        for move in moves:
            if move.kind == "l" and move.link == "d":
                receive(move)
        mine = pl.ds(pl.multiple_of(x * 128, 128), 128)
        rows = [[slot[what, which:which + 1, mine] for slot in l_slot] for what in range(2) for which in range(2)]
        pair_a, pair_q, at_i, at_j = [jnp.concatenate(row, axis=0) for row in rows]
        key = at_i * 65536 + at_j
        code = pair_a * 65536 + pair_q
        wanted = own[0:1, :] * 65536 + own[1:2, :]
        wanted = jnp.concatenate([wanted] * (128 // n_own), axis=1)
        wanted = jnp.broadcast_to(wanted, key.shape)

        def turn(_, state):
            key, code, found = state
            found = jnp.where(key == wanted, code, found)
            return pltpu.roll(key, 1, 1), pltpu.roll(code, 1, 1), found

        _, _, found = lax.fori_loop(0, 128, turn, (key, code, jnp.zeros_like(code)), unroll=8)
        table_v[0] = found // 65536
        table_v[1] = found % 65536

    def use_table():
        to_smem = pltpu.make_async_copy(table_v, table, load_sem.at[5])
        to_smem.start()
        to_smem.wait()

    def compute(slots, part, first=False):
        def step(i, _):
            for u in range(UNROLL):
                c = i * UNROLL + u
                total = product(a_slot, b_slot, table, slots[0], c)
                for slot in slots[1:]:
                    total = total + product(a_slot, b_slot, table, slot, c)
                acc[c] = total if first else acc[c] + total
            return 0

        count = n_own // UNROLL // part[1]
        lax.fori_loop(part[0] * count, (part[0] + 1) * count, step, 0)

    def from_partner(dx):
        for move in moves:
            if move.link == "d" and move.dst == dx and move.kind != "l":
                receive(move)

    def ready(dx):
        return not [s for s in steps if s[1] == "take" and s[2].dst == dx]

    early = [dx for dx in range(n_x) if 2 * dx not in LATE]
    jobs, queued = [], set()
    stage, clock = 0, 0.0
    listed = max(at for at, what, move in steps if what == "take" and move.kind == "l")
    while steps:
        now = steps[0][0]
        if stage == 0 and now > listed + 2.0:
            make_table()
            stage = 1
        elif stage == 1 and now > listed + 5.0:
            use_table()
            stage = 2
        for dx in early:
            if stage == 2 and dx not in queued and ready(dx):
                jobs.append((0.0, functools.partial(from_partner, dx)))
                jobs += [(JOB, functools.partial(compute, (2 * dx, 2 * dx + 1), (i, PIECES), first=not queued)) for i in range(PIECES)]
                queued.add(dx)
        clock = max(clock, now)
        run(steps.pop(0))
        while steps and steps[0][0] == now:
            run(steps.pop(0))
        until = steps[0][0] if steps else clock + 100.0
        while jobs and clock + jobs[0][0] < until + 1.0:
            cost, job = jobs.pop(0)
            job()
            clock += cost
    for _, job in jobs:
        job()
    for dx in range(n_x):
        if dx not in early:
            from_partner(dx)

    for move in moves:
        copy(move, y).wait_send()


def product(a_slot, b_slot, table, slot, c):
    left = a_slot[slot][table[0, slot, c]]
    right = b_slot[slot][table[1, slot, c]]
    part = jnp.dot(left, right, preferred_element_type=jnp.float32)
    return part.astype(jnp.bfloat16).astype(jnp.float32)


def finish_kernel(acc, table_v, *refs):
    a_slot = {slot: refs[2 * place] for place, slot in enumerate(LATE)}
    b_slot = {slot: refs[2 * place + 1] for place, slot in enumerate(LATE)}
    out_hbm, total_v, table, sem, out_sem = refs[2 * len(LATE):]
    n_own = acc.shape[0]
    to_smem = pltpu.make_async_copy(table_v, table, sem)
    to_smem.start()
    to_smem.wait()

    def out_copy(i):
        where = pl.ds(i * UNROLL, UNROLL)
        return pltpu.make_async_copy(total_v.at[where], out_hbm.at[where], out_sem.at[i])

    def step(i, _):
        for u in range(UNROLL):
            c = i * UNROLL + u
            total = None if len(LATE) == 8 else acc[c]
            for slot in LATE:
                part = product(a_slot, b_slot, table, slot, c)
                total = part if total is None else total + part
            total_v[c] = total
        out_copy(i).start()
        return 0

    lax.fori_loop(0, n_own // UNROLL, step, 0)
    for i in range(n_own // UNROLL):
        out_copy(i).wait()


def solution(mesh):
    n_y = mesh.shape["rows"]
    n_x = mesh.shape["ksplit"] // 2
    row_spec = P(("batch", "rows"), "ksplit")
    col_spec = P(("batch", "ksplit"))

    def device_step(a_loc, b_loc, pair_loc, plist_loc, cidx_loc):
        a, b = a_loc[0, 0], b_loc[0]
        n_a, size, _ = a.shape
        n_b = b.shape[0]
        n_own = cidx_loc.shape[2]
        n_part = plist_loc.shape[2]
        assert n_x == 4 and n_y == 4 and n_part == n_x * 128 and 128 % n_own == 0
        moves = plan(n_a, n_b)
        in_hbm = pl.BlockSpec(memory_space=pltpu.HBM)
        in_vmem = pl.BlockSpec(memory_space=pltpu.VMEM)
        a_shape, b_shape = (n_a, size, size), (n_b, size, size)
        operands = [
            pltpu.with_memory_space_constraint(one, pltpu.HBM)
            for one in (a, b, pair_loc[0, 0, :, 0, :].T, plist_loc[0, 0].T, cidx_loc[0, 0].T)
        ]
        state = pl.pallas_call(
            functools.partial(gather_kernel, (n_x, n_y, n_a, n_b, n_own)),
            name="gather",
            out_shape=[pltpu.VMEM((n_own, size, size), jnp.float32), pltpu.VMEM((2, 8, 128), jnp.int32)]
            + [pltpu.VMEM(a_shape, jnp.bfloat16), pltpu.VMEM(b_shape, jnp.bfloat16)] * len(LATE),
            in_specs=[in_hbm] * 5,
            out_specs=[in_vmem] * (2 + 2 * len(LATE)),
            scratch_shapes=[pltpu.VMEM(a_shape, jnp.bfloat16), pltpu.VMEM(b_shape, jnp.bfloat16)] * (8 - len(LATE))
            + [
                pltpu.VMEM((2, 2, n_part), jnp.int32) for _ in range(8)
            ]
            + [
                pltpu.VMEM((2, n_own), jnp.int32),
                pltpu.SMEM((2, 8, 128), jnp.int32),
                pltpu.SemaphoreType.DMA((len(moves),)),
                pltpu.SemaphoreType.DMA((len(moves),)),
                pltpu.SemaphoreType.DMA((6,)),
            ],
            compiler_params=pltpu.CompilerParams(
                collective_id=0, has_side_effects=True, vmem_limit_bytes=28 * 1024 * 1024
            ),
        )(*operands)
        out = pl.pallas_call(
            finish_kernel,
            name="finish",
            out_shape=jax.ShapeDtypeStruct((n_own, size, size), jnp.float32),
            in_specs=[in_vmem] * len(state),
            out_specs=in_hbm,
            scratch_shapes=[
                pltpu.VMEM((n_own, size, size), jnp.float32),
                pltpu.SMEM((2, 8, 128), jnp.int32),
                pltpu.SemaphoreType.DMA,
                pltpu.SemaphoreType.DMA((n_own // UNROLL,)),
            ],
            compiler_params=pltpu.CompilerParams(vmem_limit_bytes=28 * 1024 * 1024),
        )(*state)
        return out[None, None]

    return jax.shard_map(
        device_step, mesh=mesh, in_specs=(row_spec, col_spec, row_spec, row_spec, row_spec), out_specs=row_spec, check_vma=False
    )
```

```python
import functools

import jax
import jax.numpy as jnp
from jax import lax
from jax.experimental import pallas as pl
from jax.experimental.pallas import tpu as pltpu
from jax.sharding import PartitionSpec as P

MESH = pl.DeviceIdType.MESH
HALF_SET = 40
CHUNK = 5
A_CHUNK = 4
A_GATE = 0
B_GATE = 0
SLACK = 2.0
FEED_SLACK = 1.0
VMEM = 67_000_000
LAG = 3.0
LATE = (4, 5)
JOB = 0.8
PIECES = 4
UNROLL = 8


class Move:
    def __init__(self, link, kind, src, dst, part, first, count, dep, shift, rank):
        self.link, self.kind, self.src, self.dst = link, kind, src, dst
        self.part, self.first, self.count, self.dep = part, first, count, dep
        self.shift = shift
        self.rank = rank
        self.after = []


def cut(first, count, size):
    return [(first + at, min(size, count - at)) for at in range(0, count, size)]


def plan(n_a, n_b):
    half = HALF_SET // 2
    quarter = (n_b - HALF_SET) // 4
    h1, h2 = cut(0, half // 2, CHUNK), cut(half // 2, half - half // 2, CHUNK)
    q1, q2 = cut(0, quarter // 2, CHUNK), cut(quarter // 2, quarter - quarter // 2, CHUNK)
    a1, a2 = cut(0, n_a // 2, A_CHUNK), cut(n_a // 2, n_a - n_a // 2, A_CHUNK)
    moves = []

    def add(link, kind, src, dst, part, piece, dep, rank, shift=0):
        move = Move(link, kind, src, dst, part, piece[0], piece[1], dep, shift, rank)
        move.index = len(moves)
        moves.append(move)
        if dep is not None:
            dep.after.append(move)
        if link != "d":
            row = {"+y": -1, "-y": 1}.get(link, 0) + shift
            add("d", kind, dst, dst, part, piece, move, 0, row)
        return move

    def spread(move, piece, far):
        if move.part == "h":
            add("+y" if piece in h1 else "-y", "b", move.dst, move.dst, "h", piece, move, far + 1)
            return
        up = add("+y", "b", move.dst, move.dst, "q", piece, move, far)
        down = add("-y", "b", move.dst, move.dst, "q", piece, move, far)
        if piece in q1:
            add("+y", "b", move.dst, move.dst, "q", piece, up, far + 2, -1)
        else:
            add("-y", "b", move.dst, move.dst, "q", piece, down, far + 2, 1)

    for kind, count in (("b", n_b), ("a", n_a), ("l", 1)):
        add("d", kind, 0, 0, "all", (0, count), None, 9)
    listed = set()
    for link, slot in (("+x", 3), ("-x", 1)):
        first = link == "+x"
        for part, one, two in (("q", q1, q2), ("h", h1, h2)):
            keep = one if first else two
            for piece in (one + two) if first else (two + one):
                move = add(link, "b", 0, slot, part, piece, None, 0)
                spread(move, piece, 0)
                if piece in keep:
                    spread(add(link, "b", slot, 2, part, piece, move, 1), piece, 3)
                if slot not in listed:
                    listed.add(slot)
                    lists = add(link, "l", 0, slot, "all", (0, 1), None, 0)
                    if first:
                        add(link, "l", slot, 2, "all", (0, 1), lists, 1)
        keep = a1 if first else a2
        mine = [m for m in moves if m.link == link and m.src == 0 and m.kind == "b"]
        gate = mine[-1 - (A_GATE if first else B_GATE)]
        for piece in (a1 + a2) if first else (a2 + a1):
            move = add(link, "a", 0, slot, "all", piece, gate, 2)
            if piece in keep:
                add(link, "a", slot, 2, "all", piece, move, 3)
    return moves


LINKS = ("+x", "-x", "+y", "-y")


def slack(move):
    feeds = [m for m in move.after if m.link != "d"]
    if move.link in ("+x", "-x"):
        return 0.0 if feeds else SLACK
    return FEED_SLACK if feeds else SLACK


def order(moves):
    free = {link: 0.0 for link in LINKS}
    events, steps, now = [], [], 0.0

    def send(move):
        steps.append((now, "send", move))
        if move.link != "d":
            free[move.link] = max(now, free[move.link]) + (0.3 if move.kind == "l" else move.count)
            events.append((free[move.link] + LAG + slack(move), move.index, move))

    for move in moves:
        if move.dep is None and move.link != "d":
            send(move)
    while events:
        events.sort(key=lambda e: e[:2])
        now, _, move = events.pop(0)
        steps.append((now, "take", move))
        for nxt in sorted(move.after, key=lambda m: (m.link == "d", m.rank)):
            send(nxt)
    return steps


def gather_kernel(sizes, a_hbm, b_hbm, pairs_hbm, plist_hbm, own_hbm, acc, table_v, *refs):
    n_x, n_y, n_a, n_b, n_own = sizes
    a_slot, b_slot = list(refs[0:8]), list(refs[8:16])
    for place, slot in enumerate(LATE + tuple(s for s in range(8) if s not in LATE)):
        a_slot[slot], b_slot[slot] = refs[2 * place], refs[2 * place + 1]
    l_slot = refs[16:24]
    own, table, send_sem, recv_sem, load_sem = refs[24:]
    y = lax.axis_index("rows")
    p = lax.axis_index("ksplit")
    x, core = p // 2, p % 2
    moves = plan(n_a, n_b)
    steps = order(moves)

    def at(dx, other):
        return 2 * ((x + dx) % n_x) + (core + other) % 2

    target = {
        "+x": {"ksplit": at(1, 0)},
        "-x": {"ksplit": at(n_x - 1, 0)},
        "+y": {"rows": (y + 1) % n_y},
        "-y": {"rows": (y + n_y - 1) % n_y},
        "d": {"ksplit": at(0, 1)},
    }

    loads = [
        pltpu.make_async_copy(b_hbm, b_slot[0], load_sem.at[0]),
        pltpu.make_async_copy(a_hbm, a_slot[0], load_sem.at[1]),
        pltpu.make_async_copy(pairs_hbm, l_slot[0].at[0], load_sem.at[2]),
        pltpu.make_async_copy(plist_hbm, l_slot[0].at[1], load_sem.at[3]),
        pltpu.make_async_copy(own_hbm, own, load_sem.at[4]),
    ]
    for load in loads:
        load.start()

    barrier = pltpu.get_barrier_semaphore()
    for device in target.values():
        pl.semaphore_signal(barrier, inc=1, device_id=device, device_id_type=MESH)
    pl.semaphore_wait(barrier, len(target))

    def copy(move, row):
        holder = (row + move.shift + 2 * n_y) % n_y
        half = HALF_SET // 2
        quarter = (n_b - HALF_SET) // 4
        base = {"all": 0, "h": (holder % 2) * half, "q": HALF_SET + holder * quarter}[move.part]
        where = pl.ds(base + move.first, move.count)
        slots = {"a": a_slot, "b": b_slot, "l": l_slot}[move.kind]
        src = slots[2 * move.src]
        dst = slots[2 * move.dst + (1 if move.link == "d" else 0)]
        if move.kind != "l":
            src, dst = src.at[where], dst.at[where]
        return pltpu.make_async_remote_copy(
            src_ref=src,
            dst_ref=dst,
            send_sem=send_sem.at[move.index],
            recv_sem=recv_sem.at[move.index],
            device_id=target[move.link],
            device_id_type=MESH,
        )

    def start(move):
        copy(move, y).start()

    def receive(move):
        row = {"+y": y + n_y - 1, "-y": y + 1}.get(move.link, y)
        copy(move, row).wait_recv()

    def run(step):
        _, what, move = step
        if what == "send":
            start(move)
        else:
            receive(move)

    for load in loads:
        load.wait()
    while steps[0][1] == "send":
        run(steps.pop(0))
    for move in moves:
        if move.dep is None and move.link == "d":
            start(move)

    def make_table():
        for move in moves:
            if move.kind == "l" and move.link == "d":
                receive(move)
        mine = pl.ds(pl.multiple_of(x * 128, 128), 128)
        rows = [[slot[what, which:which + 1, mine] for slot in l_slot] for what in range(2) for which in range(2)]
        pair_a, pair_q, at_i, at_j = [jnp.concatenate(row, axis=0) for row in rows]
        key = at_i * 65536 + at_j
        code = pair_a * 65536 + pair_q
        wanted = own[0:1, :] * 65536 + own[1:2, :]
        wanted = jnp.concatenate([wanted] * (128 // n_own), axis=1)
        wanted = jnp.broadcast_to(wanted, key.shape)

        def turn(_, state):
            key, code, found = state
            found = jnp.where(key == wanted, code, found)
            return pltpu.roll(key, 1, 1), pltpu.roll(code, 1, 1), found

        _, _, found = lax.fori_loop(0, 128, turn, (key, code, jnp.zeros_like(code)), unroll=8)
        table_v[0] = found // 65536
        table_v[1] = found % 65536

    def use_table():
        to_smem = pltpu.make_async_copy(table_v, table, load_sem.at[5])
        to_smem.start()
        to_smem.wait()

    def compute(slots, part, first=False):
        def step(i, _):
            for u in range(UNROLL):
                c = i * UNROLL + u
                total = product(a_slot, b_slot, table, slots[0], c)
                for slot in slots[1:]:
                    total = total + product(a_slot, b_slot, table, slot, c)
                acc[c] = total if first else acc[c] + total
            return 0

        count = n_own // UNROLL // part[1]
        lax.fori_loop(part[0] * count, (part[0] + 1) * count, step, 0)

    def from_partner(dx):
        for move in moves:
            if move.link == "d" and move.dst == dx and move.kind != "l":
                receive(move)

    def ready(dx):
        return not [s for s in steps if s[1] == "take" and s[2].dst == dx]

    early = [dx for dx in range(n_x) if 2 * dx not in LATE]
    jobs, queued = [], set()
    stage, clock = 0, 0.0
    listed = max(at for at, what, move in steps if what == "take" and move.kind == "l")
    while steps:
        now = steps[0][0]
        if stage == 0 and now > listed + 2.0:
            make_table()
            stage = 1
        elif stage == 1 and now > listed + 5.0:
            use_table()
            stage = 2
        for dx in early:
            if stage == 2 and dx not in queued and ready(dx):
                jobs.append((0.0, functools.partial(from_partner, dx)))
                jobs += [(JOB, functools.partial(compute, (2 * dx, 2 * dx + 1), (i, PIECES), first=not queued)) for i in range(PIECES)]
                queued.add(dx)
        clock = max(clock, now)
        run(steps.pop(0))
        while steps and steps[0][0] == now:
            run(steps.pop(0))
        until = steps[0][0] if steps else clock + 100.0
        while jobs and clock + jobs[0][0] < until + 1.0:
            cost, job = jobs.pop(0)
            job()
            clock += cost
    for _, job in jobs:
        job()
    for dx in range(n_x):
        if dx not in early:
            from_partner(dx)

    for move in moves:
        copy(move, y).wait_send()


def product(a_slot, b_slot, table, slot, c):
    left = a_slot[slot][table[0, slot, c]]
    right = b_slot[slot][table[1, slot, c]]
    part = jnp.dot(left, right, preferred_element_type=jnp.float32)
    return part.astype(jnp.bfloat16).astype(jnp.float32)


def finish_kernel(acc, table_v, *refs):
    a_slot = {slot: refs[2 * place] for place, slot in enumerate(LATE)}
    b_slot = {slot: refs[2 * place + 1] for place, slot in enumerate(LATE)}
    out_hbm, total_v, table, sem, out_sem = refs[2 * len(LATE):]
    n_own = acc.shape[0]
    to_smem = pltpu.make_async_copy(table_v, table, sem)
    to_smem.start()
    to_smem.wait()

    def out_copy(i):
        where = pl.ds(i * UNROLL, UNROLL)
        return pltpu.make_async_copy(total_v.at[where], out_hbm.at[where], out_sem.at[i])

    def step(i, _):
        for u in range(UNROLL):
            c = i * UNROLL + u
            total = None if len(LATE) == 8 else acc[c]
            for slot in LATE:
                part = product(a_slot, b_slot, table, slot, c)
                total = part if total is None else total + part
            total_v[c] = total
        out_copy(i).start()
        return 0

    lax.fori_loop(0, n_own // UNROLL, step, 0)
    for i in range(n_own // UNROLL):
        out_copy(i).wait()


def solution(mesh):
    n_y = mesh.shape["rows"]
    n_x = mesh.shape["ksplit"] // 2
    row_spec = P(("batch", "rows"), "ksplit")
    col_spec = P(("batch", "ksplit"))

    def device_step(a_loc, b_loc, pair_loc, plist_loc, cidx_loc):
        a, b = a_loc[0, 0], b_loc[0]
        n_a, size, _ = a.shape
        n_b = b.shape[0]
        n_own = cidx_loc.shape[2]
        n_part = plist_loc.shape[2]
        assert n_x == 4 and n_y == 4 and n_part == n_x * 128 and 128 % n_own == 0
        moves = plan(n_a, n_b)
        in_hbm = pl.BlockSpec(memory_space=pltpu.HBM)
        in_vmem = pl.BlockSpec(memory_space=pltpu.VMEM)
        a_shape, b_shape = (n_a, size, size), (n_b, size, size)
        operands = [
            pltpu.with_memory_space_constraint(one, pltpu.HBM)
            for one in (a, b, pair_loc[0, 0, :, 0, :].T, plist_loc[0, 0].T, cidx_loc[0, 0].T)
        ]
        state = pl.pallas_call(
            functools.partial(gather_kernel, (n_x, n_y, n_a, n_b, n_own)),
            name="gather",
            out_shape=[pltpu.VMEM((n_own, size, size), jnp.float32), pltpu.VMEM((2, 8, 128), jnp.int32)]
            + [pltpu.VMEM(a_shape, jnp.bfloat16), pltpu.VMEM(b_shape, jnp.bfloat16)] * len(LATE),
            in_specs=[in_hbm] * 5,
            out_specs=[in_vmem] * (2 + 2 * len(LATE)),
            scratch_shapes=[pltpu.VMEM(a_shape, jnp.bfloat16), pltpu.VMEM(b_shape, jnp.bfloat16)] * (8 - len(LATE))
            + [
                pltpu.VMEM((2, 2, n_part), jnp.int32) for _ in range(8)
            ]
            + [
                pltpu.VMEM((2, n_own), jnp.int32),
                pltpu.SMEM((2, 8, 128), jnp.int32),
                pltpu.SemaphoreType.DMA((len(moves),)),
                pltpu.SemaphoreType.DMA((len(moves),)),
                pltpu.SemaphoreType.DMA((6,)),
            ],
            compiler_params=pltpu.CompilerParams(
                collective_id=0, has_side_effects=True, vmem_limit_bytes=28 * 1024 * 1024
            ),
        )(*operands)
        out = pl.pallas_call(
            finish_kernel,
            name="finish",
            out_shape=jax.ShapeDtypeStruct((n_own, size, size), jnp.float32),
            in_specs=[in_vmem] * len(state),
            out_specs=in_hbm,
            scratch_shapes=[
                pltpu.VMEM((n_own, size, size), jnp.float32),
                pltpu.SMEM((2, 8, 128), jnp.int32),
                pltpu.SemaphoreType.DMA,
                pltpu.SemaphoreType.DMA((n_own // UNROLL,)),
            ],
            compiler_params=pltpu.CompilerParams(vmem_limit_bytes=28 * 1024 * 1024),
        )(*state)
        return out[None, None]

    return jax.shard_map(
        device_step, mesh=mesh, in_specs=(row_spec, col_spec, row_spec, row_spec, row_spec), out_specs=row_spec, check_vma=False
    )
```

```python
import functools

import jax
import jax.numpy as jnp
from jax import lax
from jax.experimental import pallas as pl
from jax.experimental.pallas import tpu as pltpu
from jax.sharding import PartitionSpec as P

MESH = pl.DeviceIdType.MESH
HALF_SET = 36
CHUNK = 5
A_CHUNK = 4
A_GATE = 0
B_GATE = 0
SLACK = 2.0
FEED_SLACK = 1.0
VMEM = 67_000_000
LAG = 3.0
LATE = (4, 5)
JOB = 0.8
PIECES = 4
UNROLL = 8


class Move:
    def __init__(self, link, kind, src, dst, part, first, count, dep, shift, rank):
        self.link, self.kind, self.src, self.dst = link, kind, src, dst
        self.part, self.first, self.count, self.dep = part, first, count, dep
        self.shift = shift
        self.rank = rank
        self.after = []


def cut(first, count, size):
    return [(first + at, min(size, count - at)) for at in range(0, count, size)]


def plan(n_a, n_b):
    half = HALF_SET // 2
    quarter = (n_b - HALF_SET) // 4
    h1, h2 = cut(0, half // 2, CHUNK), cut(half // 2, half - half // 2, CHUNK)
    q1, q2 = cut(0, quarter // 2, CHUNK), cut(quarter // 2, quarter - quarter // 2, CHUNK)
    a1, a2 = cut(0, n_a // 2, A_CHUNK), cut(n_a // 2, n_a - n_a // 2, A_CHUNK)
    moves = []

    def add(link, kind, src, dst, part, piece, dep, rank, shift=0):
        move = Move(link, kind, src, dst, part, piece[0], piece[1], dep, shift, rank)
        move.index = len(moves)
        moves.append(move)
        if dep is not None:
            dep.after.append(move)
        if link != "d":
            row = {"+y": -1, "-y": 1}.get(link, 0) + shift
            add("d", kind, dst, dst, part, piece, move, 0, row)
        return move

    def spread(move, piece, far):
        if move.part == "h":
            add("+y" if piece in h1 else "-y", "b", move.dst, move.dst, "h", piece, move, far + 1)
            return
        up = add("+y", "b", move.dst, move.dst, "q", piece, move, far)
        down = add("-y", "b", move.dst, move.dst, "q", piece, move, far)
        if piece in q1:
            add("+y", "b", move.dst, move.dst, "q", piece, up, far + 2, -1)
        else:
            add("-y", "b", move.dst, move.dst, "q", piece, down, far + 2, 1)

    for kind, count in (("b", n_b), ("a", n_a), ("l", 1)):
        add("d", kind, 0, 0, "all", (0, count), None, 9)
    listed = set()
    for link, slot in (("+x", 3), ("-x", 1)):
        first = link == "+x"
        for part, one, two in (("q", q1, q2), ("h", h1, h2)):
            keep = one if first else two
            for piece in (one + two) if first else (two + one):
                move = add(link, "b", 0, slot, part, piece, None, 0)
                spread(move, piece, 0)
                if piece in keep:
                    spread(add(link, "b", slot, 2, part, piece, move, 1), piece, 3)
                if slot not in listed:
                    listed.add(slot)
                    lists = add(link, "l", 0, slot, "all", (0, 1), None, 0)
                    if first:
                        add(link, "l", slot, 2, "all", (0, 1), lists, 1)
        keep = a1 if first else a2
        mine = [m for m in moves if m.link == link and m.src == 0 and m.kind == "b"]
        gate = mine[-1 - (A_GATE if first else B_GATE)]
        for piece in (a1 + a2) if first else (a2 + a1):
            move = add(link, "a", 0, slot, "all", piece, gate, 2)
            if piece in keep:
                add(link, "a", slot, 2, "all", piece, move, 3)
    return moves


LINKS = ("+x", "-x", "+y", "-y")


def slack(move):
    feeds = [m for m in move.after if m.link != "d"]
    if move.link in ("+x", "-x"):
        return 0.0 if feeds else SLACK
    return FEED_SLACK if feeds else SLACK


def order(moves):
    free = {link: 0.0 for link in LINKS}
    events, steps, now = [], [], 0.0

    def send(move):
        steps.append((now, "send", move))
        if move.link != "d":
            free[move.link] = max(now, free[move.link]) + (0.3 if move.kind == "l" else move.count)
            events.append((free[move.link] + LAG + slack(move), move.index, move))

    for move in moves:
        if move.dep is None and move.link != "d":
            send(move)
    while events:
        events.sort(key=lambda e: e[:2])
        now, _, move = events.pop(0)
        steps.append((now, "take", move))
        for nxt in sorted(move.after, key=lambda m: (m.link == "d", m.rank)):
            send(nxt)
    return steps


def gather_kernel(sizes, a_hbm, b_hbm, pairs_hbm, plist_hbm, own_hbm, acc, table_v, *refs):
    n_x, n_y, n_a, n_b, n_own = sizes
    a_slot, b_slot = list(refs[0:8]), list(refs[8:16])
    for place, slot in enumerate(LATE + tuple(s for s in range(8) if s not in LATE)):
        a_slot[slot], b_slot[slot] = refs[2 * place], refs[2 * place + 1]
    l_slot = refs[16:24]
    own, table, send_sem, recv_sem, load_sem = refs[24:]
    y = lax.axis_index("rows")
    p = lax.axis_index("ksplit")
    x, core = p // 2, p % 2
    moves = plan(n_a, n_b)
    steps = order(moves)

    def at(dx, other):
        return 2 * ((x + dx) % n_x) + (core + other) % 2

    target = {
        "+x": {"ksplit": at(1, 0)},
        "-x": {"ksplit": at(n_x - 1, 0)},
        "+y": {"rows": (y + 1) % n_y},
        "-y": {"rows": (y + n_y - 1) % n_y},
        "d": {"ksplit": at(0, 1)},
    }

    loads = [
        pltpu.make_async_copy(b_hbm, b_slot[0], load_sem.at[0]),
        pltpu.make_async_copy(a_hbm, a_slot[0], load_sem.at[1]),
        pltpu.make_async_copy(pairs_hbm, l_slot[0].at[0], load_sem.at[2]),
        pltpu.make_async_copy(plist_hbm, l_slot[0].at[1], load_sem.at[3]),
        pltpu.make_async_copy(own_hbm, own, load_sem.at[4]),
    ]
    for load in loads:
        load.start()

    barrier = pltpu.get_barrier_semaphore()
    for device in target.values():
        pl.semaphore_signal(barrier, inc=1, device_id=device, device_id_type=MESH)
    pl.semaphore_wait(barrier, len(target))

    def copy(move, row):
        holder = (row + move.shift + 2 * n_y) % n_y
        half = HALF_SET // 2
        quarter = (n_b - HALF_SET) // 4
        base = {"all": 0, "h": (holder % 2) * half, "q": HALF_SET + holder * quarter}[move.part]
        where = pl.ds(base + move.first, move.count)
        slots = {"a": a_slot, "b": b_slot, "l": l_slot}[move.kind]
        src = slots[2 * move.src]
        dst = slots[2 * move.dst + (1 if move.link == "d" else 0)]
        if move.kind != "l":
            src, dst = src.at[where], dst.at[where]
        return pltpu.make_async_remote_copy(
            src_ref=src,
            dst_ref=dst,
            send_sem=send_sem.at[move.index],
            recv_sem=recv_sem.at[move.index],
            device_id=target[move.link],
            device_id_type=MESH,
        )

    def start(move):
        copy(move, y).start()

    def receive(move):
        row = {"+y": y + n_y - 1, "-y": y + 1}.get(move.link, y)
        copy(move, row).wait_recv()

    def run(step):
        _, what, move = step
        if what == "send":
            start(move)
        else:
            receive(move)

    for load in loads:
        load.wait()
    while steps[0][1] == "send":
        run(steps.pop(0))
    for move in moves:
        if move.dep is None and move.link == "d":
            start(move)

    def make_table():
        for move in moves:
            if move.kind == "l" and move.link == "d":
                receive(move)
        mine = pl.ds(pl.multiple_of(x * 128, 128), 128)
        rows = [[slot[what, which:which + 1, mine] for slot in l_slot] for what in range(2) for which in range(2)]
        pair_a, pair_q, at_i, at_j = [jnp.concatenate(row, axis=0) for row in rows]
        key = at_i * 65536 + at_j
        code = pair_a * 65536 + pair_q
        wanted = own[0:1, :] * 65536 + own[1:2, :]
        wanted = jnp.concatenate([wanted] * (128 // n_own), axis=1)
        wanted = jnp.broadcast_to(wanted, key.shape)

        def turn(_, state):
            key, code, found = state
            found = jnp.where(key == wanted, code, found)
            return pltpu.roll(key, 1, 1), pltpu.roll(code, 1, 1), found

        _, _, found = lax.fori_loop(0, 128, turn, (key, code, jnp.zeros_like(code)), unroll=8)
        table_v[0] = found // 65536
        table_v[1] = found % 65536

    def use_table():
        to_smem = pltpu.make_async_copy(table_v, table, load_sem.at[5])
        to_smem.start()
        to_smem.wait()

    def compute(slots, part, first=False):
        def step(i, _):
            for u in range(UNROLL):
                c = i * UNROLL + u
                total = product(a_slot, b_slot, table, slots[0], c)
                for slot in slots[1:]:
                    total = total + product(a_slot, b_slot, table, slot, c)
                acc[c] = total if first else acc[c] + total
            return 0

        count = n_own // UNROLL // part[1]
        lax.fori_loop(part[0] * count, (part[0] + 1) * count, step, 0)

    def from_partner(dx):
        for move in moves:
            if move.link == "d" and move.dst == dx and move.kind != "l":
                receive(move)

    def ready(dx):
        return not [s for s in steps if s[1] == "take" and s[2].dst == dx]

    early = [dx for dx in range(n_x) if 2 * dx not in LATE]
    jobs, queued = [], set()
    stage, clock = 0, 0.0
    listed = max(at for at, what, move in steps if what == "take" and move.kind == "l")
    while steps:
        now = steps[0][0]
        if stage == 0 and now > listed + 2.0:
            make_table()
            stage = 1
        elif stage == 1 and now > listed + 5.0:
            use_table()
            stage = 2
        for dx in early:
            if stage == 2 and dx not in queued and ready(dx):
                jobs.append((0.0, functools.partial(from_partner, dx)))
                jobs += [(JOB, functools.partial(compute, (2 * dx, 2 * dx + 1), (i, PIECES), first=not queued)) for i in range(PIECES)]
                queued.add(dx)
        clock = max(clock, now)
        run(steps.pop(0))
        while steps and steps[0][0] == now:
            run(steps.pop(0))
        until = steps[0][0] if steps else clock + 100.0
        while jobs and clock + jobs[0][0] < until + 1.0:
            cost, job = jobs.pop(0)
            job()
            clock += cost
    for _, job in jobs:
        job()
    for dx in range(n_x):
        if dx not in early:
            from_partner(dx)

    for move in moves:
        copy(move, y).wait_send()


def product(a_slot, b_slot, table, slot, c):
    left = a_slot[slot][table[0, slot, c]]
    right = b_slot[slot][table[1, slot, c]]
    part = jnp.dot(left, right, preferred_element_type=jnp.float32)
    return part.astype(jnp.bfloat16).astype(jnp.float32)


def finish_kernel(acc, table_v, *refs):
    a_slot = {slot: refs[2 * place] for place, slot in enumerate(LATE)}
    b_slot = {slot: refs[2 * place + 1] for place, slot in enumerate(LATE)}
    out_hbm, total_v, table, sem, out_sem = refs[2 * len(LATE):]
    n_own = acc.shape[0]
    to_smem = pltpu.make_async_copy(table_v, table, sem)
    to_smem.start()
    to_smem.wait()

    def out_copy(i):
        where = pl.ds(i * UNROLL, UNROLL)
        return pltpu.make_async_copy(total_v.at[where], out_hbm.at[where], out_sem.at[i])

    def step(i, _):
        for u in range(UNROLL):
            c = i * UNROLL + u
            total = None if len(LATE) == 8 else acc[c]
            for slot in LATE:
                part = product(a_slot, b_slot, table, slot, c)
                total = part if total is None else total + part
            total_v[c] = total
        out_copy(i).start()
        return 0

    lax.fori_loop(0, n_own // UNROLL, step, 0)
    for i in range(n_own // UNROLL):
        out_copy(i).wait()


def solution(mesh):
    n_y = mesh.shape["rows"]
    n_x = mesh.shape["ksplit"] // 2
    row_spec = P(("batch", "rows"), "ksplit")
    col_spec = P(("batch", "ksplit"))

    def device_step(a_loc, b_loc, pair_loc, plist_loc, cidx_loc):
        a, b = a_loc[0, 0], b_loc[0]
        n_a, size, _ = a.shape
        n_b = b.shape[0]
        n_own = cidx_loc.shape[2]
        n_part = plist_loc.shape[2]
        assert n_x == 4 and n_y == 4 and n_part == n_x * 128 and 128 % n_own == 0
        moves = plan(n_a, n_b)
        in_hbm = pl.BlockSpec(memory_space=pltpu.HBM)
        in_vmem = pl.BlockSpec(memory_space=pltpu.VMEM)
        a_shape, b_shape = (n_a, size, size), (n_b, size, size)
        operands = [
            pltpu.with_memory_space_constraint(one, pltpu.HBM)
            for one in (a, b, pair_loc[0, 0, :, 0, :].T, plist_loc[0, 0].T, cidx_loc[0, 0].T)
        ]
        state = pl.pallas_call(
            functools.partial(gather_kernel, (n_x, n_y, n_a, n_b, n_own)),
            name="gather",
            out_shape=[pltpu.VMEM((n_own, size, size), jnp.float32), pltpu.VMEM((2, 8, 128), jnp.int32)]
            + [pltpu.VMEM(a_shape, jnp.bfloat16), pltpu.VMEM(b_shape, jnp.bfloat16)] * len(LATE),
            in_specs=[in_hbm] * 5,
            out_specs=[in_vmem] * (2 + 2 * len(LATE)),
            scratch_shapes=[pltpu.VMEM(a_shape, jnp.bfloat16), pltpu.VMEM(b_shape, jnp.bfloat16)] * (8 - len(LATE))
            + [
                pltpu.VMEM((2, 2, n_part), jnp.int32) for _ in range(8)
            ]
            + [
                pltpu.VMEM((2, n_own), jnp.int32),
                pltpu.SMEM((2, 8, 128), jnp.int32),
                pltpu.SemaphoreType.DMA((len(moves),)),
                pltpu.SemaphoreType.DMA((len(moves),)),
                pltpu.SemaphoreType.DMA((6,)),
            ],
            compiler_params=pltpu.CompilerParams(
                collective_id=0, has_side_effects=True, vmem_limit_bytes=28 * 1024 * 1024
            ),
        )(*operands)
        out = pl.pallas_call(
            finish_kernel,
            name="finish",
            out_shape=jax.ShapeDtypeStruct((n_own, size, size), jnp.float32),
            in_specs=[in_vmem] * len(state),
            out_specs=in_hbm,
            scratch_shapes=[
                pltpu.VMEM((n_own, size, size), jnp.float32),
                pltpu.SMEM((2, 8, 128), jnp.int32),
                pltpu.SemaphoreType.DMA,
                pltpu.SemaphoreType.DMA((n_own // UNROLL,)),
            ],
            compiler_params=pltpu.CompilerParams(vmem_limit_bytes=28 * 1024 * 1024),
        )(*state)
        return out[None, None]

    return jax.shard_map(
        device_step, mesh=mesh, in_specs=(row_spec, col_spec, row_spec, row_spec, row_spec), out_specs=row_spec, check_vma=False
    )
```

```python
import functools

import jax
import jax.numpy as jnp
from jax import lax
from jax.experimental import pallas as pl
from jax.experimental.pallas import tpu as pltpu
from jax.sharding import PartitionSpec as P

MESH = pl.DeviceIdType.MESH
HALF_SET = 36
CHUNK = 5
A_CHUNK = 4
A_GATE = 0
B_GATE = 0
SLACK = 2.0
FEED_SLACK = 1.0
VMEM = 67_000_000
LAG = 3.0
LATE = (2, 3, 4, 5, 6, 7)
JOB = 0.8
PIECES = 4
UNROLL = 8


class Move:
    def __init__(self, link, kind, src, dst, part, first, count, dep, shift, rank):
        self.link, self.kind, self.src, self.dst = link, kind, src, dst
        self.part, self.first, self.count, self.dep = part, first, count, dep
        self.shift = shift
        self.rank = rank
        self.after = []


def cut(first, count, size):
    return [(first + at, min(size, count - at)) for at in range(0, count, size)]


def plan(n_a, n_b):
    half = HALF_SET // 2
    quarter = (n_b - HALF_SET) // 4
    h1, h2 = cut(0, half // 2, CHUNK), cut(half // 2, half - half // 2, CHUNK)
    q1, q2 = cut(0, quarter // 2, CHUNK), cut(quarter // 2, quarter - quarter // 2, CHUNK)
    a1, a2 = cut(0, n_a // 2, A_CHUNK), cut(n_a // 2, n_a - n_a // 2, A_CHUNK)
    moves = []

    def add(link, kind, src, dst, part, piece, dep, rank, shift=0):
        move = Move(link, kind, src, dst, part, piece[0], piece[1], dep, shift, rank)
        move.index = len(moves)
        moves.append(move)
        if dep is not None:
            dep.after.append(move)
        if link != "d":
            row = {"+y": -1, "-y": 1}.get(link, 0) + shift
            add("d", kind, dst, dst, part, piece, move, 0, row)
        return move

    def spread(move, piece, far):
        if move.part == "h":
            add("+y" if piece in h1 else "-y", "b", move.dst, move.dst, "h", piece, move, far + 1)
            return
        up = add("+y", "b", move.dst, move.dst, "q", piece, move, far)
        down = add("-y", "b", move.dst, move.dst, "q", piece, move, far)
        if piece in q1:
            add("+y", "b", move.dst, move.dst, "q", piece, up, far + 2, -1)
        else:
            add("-y", "b", move.dst, move.dst, "q", piece, down, far + 2, 1)

    for kind, count in (("b", n_b), ("a", n_a), ("l", 1)):
        add("d", kind, 0, 0, "all", (0, count), None, 9)
    listed = set()
    for link, slot in (("+x", 3), ("-x", 1)):
        first = link == "+x"
        for part, one, two in (("q", q1, q2), ("h", h1, h2)):
            keep = one if first else two
            for piece in (one + two) if first else (two + one):
                move = add(link, "b", 0, slot, part, piece, None, 0)
                spread(move, piece, 0)
                if piece in keep:
                    spread(add(link, "b", slot, 2, part, piece, move, 1), piece, 3)
                if slot not in listed:
                    listed.add(slot)
                    lists = add(link, "l", 0, slot, "all", (0, 1), None, 0)
                    if first:
                        add(link, "l", slot, 2, "all", (0, 1), lists, 1)
        keep = a1 if first else a2
        mine = [m for m in moves if m.link == link and m.src == 0 and m.kind == "b"]
        gate = mine[-1 - (A_GATE if first else B_GATE)]
        for piece in (a1 + a2) if first else (a2 + a1):
            move = add(link, "a", 0, slot, "all", piece, gate, 2)
            if piece in keep:
                add(link, "a", slot, 2, "all", piece, move, 3)
    return moves


LINKS = ("+x", "-x", "+y", "-y")


def slack(move):
    feeds = [m for m in move.after if m.link != "d"]
    if move.link in ("+x", "-x"):
        return 0.0 if feeds else SLACK
    return FEED_SLACK if feeds else SLACK


def order(moves):
    free = {link: 0.0 for link in LINKS}
    events, steps, now = [], [], 0.0

    def send(move):
        steps.append((now, "send", move))
        if move.link != "d":
            free[move.link] = max(now, free[move.link]) + (0.3 if move.kind == "l" else move.count)
            events.append((free[move.link] + LAG + slack(move), move.index, move))

    for move in moves:
        if move.dep is None and move.link != "d":
            send(move)
    while events:
        events.sort(key=lambda e: e[:2])
        now, _, move = events.pop(0)
        steps.append((now, "take", move))
        for nxt in sorted(move.after, key=lambda m: (m.link == "d", m.rank)):
            send(nxt)
    return steps


def gather_kernel(sizes, a_hbm, b_hbm, pairs_hbm, plist_hbm, own_hbm, acc, table_v, *refs):
    n_x, n_y, n_a, n_b, n_own = sizes
    a_slot, b_slot = list(refs[0:8]), list(refs[8:16])
    for place, slot in enumerate(LATE + tuple(s for s in range(8) if s not in LATE)):
        a_slot[slot], b_slot[slot] = refs[2 * place], refs[2 * place + 1]
    l_slot = refs[16:24]
    own, table, send_sem, recv_sem, load_sem = refs[24:]
    y = lax.axis_index("rows")
    p = lax.axis_index("ksplit")
    x, core = p // 2, p % 2
    moves = plan(n_a, n_b)
    steps = order(moves)

    def at(dx, other):
        return 2 * ((x + dx) % n_x) + (core + other) % 2

    target = {
        "+x": {"ksplit": at(1, 0)},
        "-x": {"ksplit": at(n_x - 1, 0)},
        "+y": {"rows": (y + 1) % n_y},
        "-y": {"rows": (y + n_y - 1) % n_y},
        "d": {"ksplit": at(0, 1)},
    }

    loads = [
        pltpu.make_async_copy(b_hbm, b_slot[0], load_sem.at[0]),
        pltpu.make_async_copy(a_hbm, a_slot[0], load_sem.at[1]),
        pltpu.make_async_copy(pairs_hbm, l_slot[0].at[0], load_sem.at[2]),
        pltpu.make_async_copy(plist_hbm, l_slot[0].at[1], load_sem.at[3]),
        pltpu.make_async_copy(own_hbm, own, load_sem.at[4]),
    ]
    for load in loads:
        load.start()

    barrier = pltpu.get_barrier_semaphore()
    for device in target.values():
        pl.semaphore_signal(barrier, inc=1, device_id=device, device_id_type=MESH)
    pl.semaphore_wait(barrier, len(target))

    def copy(move, row):
        holder = (row + move.shift + 2 * n_y) % n_y
        half = HALF_SET // 2
        quarter = (n_b - HALF_SET) // 4
        base = {"all": 0, "h": (holder % 2) * half, "q": HALF_SET + holder * quarter}[move.part]
        where = pl.ds(base + move.first, move.count)
        slots = {"a": a_slot, "b": b_slot, "l": l_slot}[move.kind]
        src = slots[2 * move.src]
        dst = slots[2 * move.dst + (1 if move.link == "d" else 0)]
        if move.kind != "l":
            src, dst = src.at[where], dst.at[where]
        return pltpu.make_async_remote_copy(
            src_ref=src,
            dst_ref=dst,
            send_sem=send_sem.at[move.index],
            recv_sem=recv_sem.at[move.index],
            device_id=target[move.link],
            device_id_type=MESH,
        )

    def start(move):
        copy(move, y).start()

    def receive(move):
        row = {"+y": y + n_y - 1, "-y": y + 1}.get(move.link, y)
        copy(move, row).wait_recv()

    def run(step):
        _, what, move = step
        if what == "send":
            start(move)
        else:
            receive(move)

    for load in loads:
        load.wait()
    while steps[0][1] == "send":
        run(steps.pop(0))
    for move in moves:
        if move.dep is None and move.link == "d":
            start(move)

    def make_table():
        for move in moves:
            if move.kind == "l" and move.link == "d":
                receive(move)
        mine = pl.ds(pl.multiple_of(x * 128, 128), 128)
        rows = [[slot[what, which:which + 1, mine] for slot in l_slot] for what in range(2) for which in range(2)]
        pair_a, pair_q, at_i, at_j = [jnp.concatenate(row, axis=0) for row in rows]
        key = at_i * 65536 + at_j
        code = pair_a * 65536 + pair_q
        wanted = own[0:1, :] * 65536 + own[1:2, :]
        wanted = jnp.concatenate([wanted] * (128 // n_own), axis=1)
        wanted = jnp.broadcast_to(wanted, key.shape)

        def turn(_, state):
            key, code, found = state
            found = jnp.where(key == wanted, code, found)
            return pltpu.roll(key, 1, 1), pltpu.roll(code, 1, 1), found

        _, _, found = lax.fori_loop(0, 128, turn, (key, code, jnp.zeros_like(code)), unroll=8)
        table_v[0] = found // 65536
        table_v[1] = found % 65536

    def use_table():
        to_smem = pltpu.make_async_copy(table_v, table, load_sem.at[5])
        to_smem.start()
        to_smem.wait()

    def compute(slots, part, first=False):
        def step(i, _):
            for u in range(UNROLL):
                c = i * UNROLL + u
                total = product(a_slot, b_slot, table, slots[0], c)
                for slot in slots[1:]:
                    total = total + product(a_slot, b_slot, table, slot, c)
                acc[c] = total if first else acc[c] + total
            return 0

        count = n_own // UNROLL // part[1]
        lax.fori_loop(part[0] * count, (part[0] + 1) * count, step, 0)

    def from_partner(dx):
        for move in moves:
            if move.link == "d" and move.dst == dx and move.kind != "l":
                receive(move)

    def ready(dx):
        return not [s for s in steps if s[1] == "take" and s[2].dst == dx]

    early = [dx for dx in range(n_x) if 2 * dx not in LATE]
    jobs, queued = [], set()
    stage, clock = 0, 0.0
    listed = max(at for at, what, move in steps if what == "take" and move.kind == "l")
    while steps:
        now = steps[0][0]
        if stage == 0 and now > listed + 2.0:
            make_table()
            stage = 1
        elif stage == 1 and now > listed + 5.0:
            use_table()
            stage = 2
        for dx in early:
            if stage == 2 and dx not in queued and ready(dx):
                jobs.append((0.0, functools.partial(from_partner, dx)))
                jobs += [(JOB, functools.partial(compute, (2 * dx, 2 * dx + 1), (i, PIECES), first=not queued)) for i in range(PIECES)]
                queued.add(dx)
        clock = max(clock, now)
        run(steps.pop(0))
        while steps and steps[0][0] == now:
            run(steps.pop(0))
        until = steps[0][0] if steps else clock + 100.0
        while jobs and clock + jobs[0][0] < until + 1.0:
            cost, job = jobs.pop(0)
            job()
            clock += cost
    for _, job in jobs:
        job()
    for dx in range(n_x):
        if dx not in early:
            from_partner(dx)

    for move in moves:
        copy(move, y).wait_send()


def product(a_slot, b_slot, table, slot, c):
    left = a_slot[slot][table[0, slot, c]]
    right = b_slot[slot][table[1, slot, c]]
    part = jnp.dot(left, right, preferred_element_type=jnp.float32)
    return part.astype(jnp.bfloat16).astype(jnp.float32)


def finish_kernel(acc, table_v, *refs):
    a_slot = {slot: refs[2 * place] for place, slot in enumerate(LATE)}
    b_slot = {slot: refs[2 * place + 1] for place, slot in enumerate(LATE)}
    out_hbm, total_v, table, sem, out_sem = refs[2 * len(LATE):]
    n_own = acc.shape[0]
    to_smem = pltpu.make_async_copy(table_v, table, sem)
    to_smem.start()
    to_smem.wait()

    def out_copy(i):
        where = pl.ds(i * UNROLL, UNROLL)
        return pltpu.make_async_copy(total_v.at[where], out_hbm.at[where], out_sem.at[i])

    def step(i, _):
        for u in range(UNROLL):
            c = i * UNROLL + u
            total = None if len(LATE) == 8 else acc[c]
            for slot in LATE:
                part = product(a_slot, b_slot, table, slot, c)
                total = part if total is None else total + part
            total_v[c] = total
        out_copy(i).start()
        return 0

    lax.fori_loop(0, n_own // UNROLL, step, 0)
    for i in range(n_own // UNROLL):
        out_copy(i).wait()


def solution(mesh):
    n_y = mesh.shape["rows"]
    n_x = mesh.shape["ksplit"] // 2
    row_spec = P(("batch", "rows"), "ksplit")
    col_spec = P(("batch", "ksplit"))

    def device_step(a_loc, b_loc, pair_loc, plist_loc, cidx_loc):
        a, b = a_loc[0, 0], b_loc[0]
        n_a, size, _ = a.shape
        n_b = b.shape[0]
        n_own = cidx_loc.shape[2]
        n_part = plist_loc.shape[2]
        assert n_x == 4 and n_y == 4 and n_part == n_x * 128 and 128 % n_own == 0
        moves = plan(n_a, n_b)
        in_hbm = pl.BlockSpec(memory_space=pltpu.HBM)
        in_vmem = pl.BlockSpec(memory_space=pltpu.VMEM)
        a_shape, b_shape = (n_a, size, size), (n_b, size, size)
        operands = [
            pltpu.with_memory_space_constraint(one, pltpu.HBM)
            for one in (a, b, pair_loc[0, 0, :, 0, :].T, plist_loc[0, 0].T, cidx_loc[0, 0].T)
        ]
        state = pl.pallas_call(
            functools.partial(gather_kernel, (n_x, n_y, n_a, n_b, n_own)),
            name="gather",
            out_shape=[pltpu.VMEM((n_own, size, size), jnp.float32), pltpu.VMEM((2, 8, 128), jnp.int32)]
            + [pltpu.VMEM(a_shape, jnp.bfloat16), pltpu.VMEM(b_shape, jnp.bfloat16)] * len(LATE),
            in_specs=[in_hbm] * 5,
            out_specs=[in_vmem] * (2 + 2 * len(LATE)),
            scratch_shapes=[pltpu.VMEM(a_shape, jnp.bfloat16), pltpu.VMEM(b_shape, jnp.bfloat16)] * (8 - len(LATE))
            + [
                pltpu.VMEM((2, 2, n_part), jnp.int32) for _ in range(8)
            ]
            + [
                pltpu.VMEM((2, n_own), jnp.int32),
                pltpu.SMEM((2, 8, 128), jnp.int32),
                pltpu.SemaphoreType.DMA((len(moves),)),
                pltpu.SemaphoreType.DMA((len(moves),)),
                pltpu.SemaphoreType.DMA((6,)),
            ],
            compiler_params=pltpu.CompilerParams(
                collective_id=0, has_side_effects=True, vmem_limit_bytes=28 * 1024 * 1024
            ),
        )(*operands)
        out = pl.pallas_call(
            finish_kernel,
            name="finish",
            out_shape=jax.ShapeDtypeStruct((n_own, size, size), jnp.float32),
            in_specs=[in_vmem] * len(state),
            out_specs=in_hbm,
            scratch_shapes=[
                pltpu.VMEM((n_own, size, size), jnp.float32),
                pltpu.SMEM((2, 8, 128), jnp.int32),
                pltpu.SemaphoreType.DMA,
                pltpu.SemaphoreType.DMA((n_own // UNROLL,)),
            ],
            compiler_params=pltpu.CompilerParams(vmem_limit_bytes=28 * 1024 * 1024),
        )(*state)
        return out[None, None]

    return jax.shard_map(
        device_step, mesh=mesh, in_specs=(row_spec, col_spec, row_spec, row_spec, row_spec), out_specs=row_spec, check_vma=False
    )
```

```python
import functools

import jax
import jax.numpy as jnp
from jax import lax
from jax.experimental import pallas as pl
from jax.experimental.pallas import tpu as pltpu
from jax.sharding import PartitionSpec as P

MESH = pl.DeviceIdType.MESH
HALF_SET = 36
CHUNK = 5
A_CHUNK = 4
A_GATE = 0
B_GATE = 3
SLACK = 2.0
FEED_SLACK = 1.0
VMEM = 67_000_000
LAG = 3.0
LATE = (4, 5)
JOB = 0.8
PIECES = 4
UNROLL = 8


class Move:
    def __init__(self, link, kind, src, dst, part, first, count, dep, shift, rank):
        self.link, self.kind, self.src, self.dst = link, kind, src, dst
        self.part, self.first, self.count, self.dep = part, first, count, dep
        self.shift = shift
        self.rank = rank
        self.after = []


def cut(first, count, size):
    return [(first + at, min(size, count - at)) for at in range(0, count, size)]


def plan(n_a, n_b):
    half = HALF_SET // 2
    quarter = (n_b - HALF_SET) // 4
    h1, h2 = cut(0, half // 2, CHUNK), cut(half // 2, half - half // 2, CHUNK)
    q1, q2 = cut(0, quarter // 2, CHUNK), cut(quarter // 2, quarter - quarter // 2, CHUNK)
    a1, a2 = cut(0, n_a // 2, A_CHUNK), cut(n_a // 2, n_a - n_a // 2, A_CHUNK)
    moves = []

    def add(link, kind, src, dst, part, piece, dep, rank, shift=0):
        move = Move(link, kind, src, dst, part, piece[0], piece[1], dep, shift, rank)
        move.index = len(moves)
        moves.append(move)
        if dep is not None:
            dep.after.append(move)
        if link != "d":
            row = {"+y": -1, "-y": 1}.get(link, 0) + shift
            add("d", kind, dst, dst, part, piece, move, 0, row)
        return move

    def spread(move, piece, far):
        if move.part == "h":
            add("+y" if piece in h1 else "-y", "b", move.dst, move.dst, "h", piece, move, far + 1)
            return
        up = add("+y", "b", move.dst, move.dst, "q", piece, move, far)
        down = add("-y", "b", move.dst, move.dst, "q", piece, move, far)
        if piece in q1:
            add("+y", "b", move.dst, move.dst, "q", piece, up, far + 2, -1)
        else:
            add("-y", "b", move.dst, move.dst, "q", piece, down, far + 2, 1)

    for kind, count in (("b", n_b), ("a", n_a), ("l", 1)):
        add("d", kind, 0, 0, "all", (0, count), None, 9)
    listed = set()
    for link, slot in (("+x", 3), ("-x", 1)):
        first = link == "+x"
        for part, one, two in (("q", q1, q2), ("h", h1, h2)):
            keep = one if first else two
            for piece in (one + two) if first else (two + one):
                move = add(link, "b", 0, slot, part, piece, None, 0)
                spread(move, piece, 0)
                if piece in keep:
                    spread(add(link, "b", slot, 2, part, piece, move, 1), piece, 3)
                if slot not in listed:
                    listed.add(slot)
                    lists = add(link, "l", 0, slot, "all", (0, 1), None, 0)
                    if first:
                        add(link, "l", slot, 2, "all", (0, 1), lists, 1)
        keep = a1 if first else a2
        mine = [m for m in moves if m.link == link and m.src == 0 and m.kind == "b"]
        gate = mine[-1 - (A_GATE if first else B_GATE)]
        for piece in (a1 + a2) if first else (a2 + a1):
            move = add(link, "a", 0, slot, "all", piece, gate, 2)
            if piece in keep:
                add(link, "a", slot, 2, "all", piece, move, 3)
    return moves


LINKS = ("+x", "-x", "+y", "-y")


def slack(move):
    feeds = [m for m in move.after if m.link != "d"]
    if move.link in ("+x", "-x"):
        return 0.0 if feeds else SLACK
    return FEED_SLACK if feeds else SLACK


def order(moves):
    free = {link: 0.0 for link in LINKS}
    events, steps, now = [], [], 0.0

    def send(move):
        steps.append((now, "send", move))
        if move.link != "d":
            free[move.link] = max(now, free[move.link]) + (0.3 if move.kind == "l" else move.count)
            events.append((free[move.link] + LAG + slack(move), move.index, move))

    for move in moves:
        if move.dep is None and move.link != "d":
            send(move)
    while events:
        events.sort(key=lambda e: e[:2])
        now, _, move = events.pop(0)
        steps.append((now, "take", move))
        for nxt in sorted(move.after, key=lambda m: (m.link == "d", m.rank)):
            send(nxt)
    return steps


def gather_kernel(sizes, a_hbm, b_hbm, pairs_hbm, plist_hbm, own_hbm, acc, table_v, *refs):
    n_x, n_y, n_a, n_b, n_own = sizes
    a_slot, b_slot = list(refs[0:8]), list(refs[8:16])
    for place, slot in enumerate(LATE + tuple(s for s in range(8) if s not in LATE)):
        a_slot[slot], b_slot[slot] = refs[2 * place], refs[2 * place + 1]
    l_slot = refs[16:24]
    own, table, send_sem, recv_sem, load_sem = refs[24:]
    y = lax.axis_index("rows")
    p = lax.axis_index("ksplit")
    x, core = p // 2, p % 2
    moves = plan(n_a, n_b)
    steps = order(moves)

    def at(dx, other):
        return 2 * ((x + dx) % n_x) + (core + other) % 2

    target = {
        "+x": {"ksplit": at(1, 0)},
        "-x": {"ksplit": at(n_x - 1, 0)},
        "+y": {"rows": (y + 1) % n_y},
        "-y": {"rows": (y + n_y - 1) % n_y},
        "d": {"ksplit": at(0, 1)},
    }

    loads = [
        pltpu.make_async_copy(b_hbm, b_slot[0], load_sem.at[0]),
        pltpu.make_async_copy(a_hbm, a_slot[0], load_sem.at[1]),
        pltpu.make_async_copy(pairs_hbm, l_slot[0].at[0], load_sem.at[2]),
        pltpu.make_async_copy(plist_hbm, l_slot[0].at[1], load_sem.at[3]),
        pltpu.make_async_copy(own_hbm, own, load_sem.at[4]),
    ]
    for load in loads:
        load.start()

    barrier = pltpu.get_barrier_semaphore()
    for device in target.values():
        pl.semaphore_signal(barrier, inc=1, device_id=device, device_id_type=MESH)
    pl.semaphore_wait(barrier, len(target))

    def copy(move, row):
        holder = (row + move.shift + 2 * n_y) % n_y
        half = HALF_SET // 2
        quarter = (n_b - HALF_SET) // 4
        base = {"all": 0, "h": (holder % 2) * half, "q": HALF_SET + holder * quarter}[move.part]
        where = pl.ds(base + move.first, move.count)
        slots = {"a": a_slot, "b": b_slot, "l": l_slot}[move.kind]
        src = slots[2 * move.src]
        dst = slots[2 * move.dst + (1 if move.link == "d" else 0)]
        if move.kind != "l":
            src, dst = src.at[where], dst.at[where]
        return pltpu.make_async_remote_copy(
            src_ref=src,
            dst_ref=dst,
            send_sem=send_sem.at[move.index],
            recv_sem=recv_sem.at[move.index],
            device_id=target[move.link],
            device_id_type=MESH,
        )

    def start(move):
        copy(move, y).start()

    def receive(move):
        row = {"+y": y + n_y - 1, "-y": y + 1}.get(move.link, y)
        copy(move, row).wait_recv()

    def run(step):
        _, what, move = step
        if what == "send":
            start(move)
        else:
            receive(move)

    for load in loads:
        load.wait()
    while steps[0][1] == "send":
        run(steps.pop(0))
    for move in moves:
        if move.dep is None and move.link == "d":
            start(move)

    def make_table():
        for move in moves:
            if move.kind == "l" and move.link == "d":
                receive(move)
        mine = pl.ds(pl.multiple_of(x * 128, 128), 128)
        rows = [[slot[what, which:which + 1, mine] for slot in l_slot] for what in range(2) for which in range(2)]
        pair_a, pair_q, at_i, at_j = [jnp.concatenate(row, axis=0) for row in rows]
        key = at_i * 65536 + at_j
        code = pair_a * 65536 + pair_q
        wanted = own[0:1, :] * 65536 + own[1:2, :]
        wanted = jnp.concatenate([wanted] * (128 // n_own), axis=1)
        wanted = jnp.broadcast_to(wanted, key.shape)

        def turn(_, state):
            key, code, found = state
            found = jnp.where(key == wanted, code, found)
            return pltpu.roll(key, 1, 1), pltpu.roll(code, 1, 1), found

        _, _, found = lax.fori_loop(0, 128, turn, (key, code, jnp.zeros_like(code)), unroll=8)
        table_v[0] = found // 65536
        table_v[1] = found % 65536

    def use_table():
        to_smem = pltpu.make_async_copy(table_v, table, load_sem.at[5])
        to_smem.start()
        to_smem.wait()

    def compute(slots, part, first=False):
        def step(i, _):
            for u in range(UNROLL):
                c = i * UNROLL + u
                total = product(a_slot, b_slot, table, slots[0], c)
                for slot in slots[1:]:
                    total = total + product(a_slot, b_slot, table, slot, c)
                acc[c] = total if first else acc[c] + total
            return 0

        count = n_own // UNROLL // part[1]
        lax.fori_loop(part[0] * count, (part[0] + 1) * count, step, 0)

    def from_partner(dx):
        for move in moves:
            if move.link == "d" and move.dst == dx and move.kind != "l":
                receive(move)

    def ready(dx):
        return not [s for s in steps if s[1] == "take" and s[2].dst == dx]

    early = [dx for dx in range(n_x) if 2 * dx not in LATE]
    jobs, queued = [], set()
    stage, clock = 0, 0.0
    listed = max(at for at, what, move in steps if what == "take" and move.kind == "l")
    while steps:
        now = steps[0][0]
        if stage == 0 and now > listed + 2.0:
            make_table()
            stage = 1
        elif stage == 1 and now > listed + 5.0:
            use_table()
            stage = 2
        for dx in early:
            if stage == 2 and dx not in queued and ready(dx):
                jobs.append((0.0, functools.partial(from_partner, dx)))
                jobs += [(JOB, functools.partial(compute, (2 * dx, 2 * dx + 1), (i, PIECES), first=not queued)) for i in range(PIECES)]
                queued.add(dx)
        clock = max(clock, now)
        run(steps.pop(0))
        while steps and steps[0][0] == now:
            run(steps.pop(0))
        until = steps[0][0] if steps else clock + 100.0
        while jobs and clock + jobs[0][0] < until + 1.0:
            cost, job = jobs.pop(0)
            job()
            clock += cost
    for _, job in jobs:
        job()
    for dx in range(n_x):
        if dx not in early:
            from_partner(dx)

    for move in moves:
        copy(move, y).wait_send()


def product(a_slot, b_slot, table, slot, c):
    left = a_slot[slot][table[0, slot, c]]
    right = b_slot[slot][table[1, slot, c]]
    part = jnp.dot(left, right, preferred_element_type=jnp.float32)
    return part.astype(jnp.bfloat16).astype(jnp.float32)


def finish_kernel(acc, table_v, *refs):
    a_slot = {slot: refs[2 * place] for place, slot in enumerate(LATE)}
    b_slot = {slot: refs[2 * place + 1] for place, slot in enumerate(LATE)}
    out_hbm, total_v, table, sem, out_sem = refs[2 * len(LATE):]
    n_own = acc.shape[0]
    to_smem = pltpu.make_async_copy(table_v, table, sem)
    to_smem.start()
    to_smem.wait()

    def out_copy(i):
        where = pl.ds(i * UNROLL, UNROLL)
        return pltpu.make_async_copy(total_v.at[where], out_hbm.at[where], out_sem.at[i])

    def step(i, _):
        for u in range(UNROLL):
            c = i * UNROLL + u
            total = None if len(LATE) == 8 else acc[c]
            for slot in LATE:
                part = product(a_slot, b_slot, table, slot, c)
                total = part if total is None else total + part
            total_v[c] = total
        out_copy(i).start()
        return 0

    lax.fori_loop(0, n_own // UNROLL, step, 0)
    for i in range(n_own // UNROLL):
        out_copy(i).wait()


def solution(mesh):
    n_y = mesh.shape["rows"]
    n_x = mesh.shape["ksplit"] // 2
    row_spec = P(("batch", "rows"), "ksplit")
    col_spec = P(("batch", "ksplit"))

    def device_step(a_loc, b_loc, pair_loc, plist_loc, cidx_loc):
        a, b = a_loc[0, 0], b_loc[0]
        n_a, size, _ = a.shape
        n_b = b.shape[0]
        n_own = cidx_loc.shape[2]
        n_part = plist_loc.shape[2]
        assert n_x == 4 and n_y == 4 and n_part == n_x * 128 and 128 % n_own == 0
        moves = plan(n_a, n_b)
        in_hbm = pl.BlockSpec(memory_space=pltpu.HBM)
        in_vmem = pl.BlockSpec(memory_space=pltpu.VMEM)
        a_shape, b_shape = (n_a, size, size), (n_b, size, size)
        operands = [
            pltpu.with_memory_space_constraint(one, pltpu.HBM)
            for one in (a, b, pair_loc[0, 0, :, 0, :].T, plist_loc[0, 0].T, cidx_loc[0, 0].T)
        ]
        state = pl.pallas_call(
            functools.partial(gather_kernel, (n_x, n_y, n_a, n_b, n_own)),
            name="gather",
            out_shape=[pltpu.VMEM((n_own, size, size), jnp.float32), pltpu.VMEM((2, 8, 128), jnp.int32)]
            + [pltpu.VMEM(a_shape, jnp.bfloat16), pltpu.VMEM(b_shape, jnp.bfloat16)] * len(LATE),
            in_specs=[in_hbm] * 5,
            out_specs=[in_vmem] * (2 + 2 * len(LATE)),
            scratch_shapes=[pltpu.VMEM(a_shape, jnp.bfloat16), pltpu.VMEM(b_shape, jnp.bfloat16)] * (8 - len(LATE))
            + [
                pltpu.VMEM((2, 2, n_part), jnp.int32) for _ in range(8)
            ]
            + [
                pltpu.VMEM((2, n_own), jnp.int32),
                pltpu.SMEM((2, 8, 128), jnp.int32),
                pltpu.SemaphoreType.DMA((len(moves),)),
                pltpu.SemaphoreType.DMA((len(moves),)),
                pltpu.SemaphoreType.DMA((6,)),
            ],
            compiler_params=pltpu.CompilerParams(
                collective_id=0, has_side_effects=True, vmem_limit_bytes=28 * 1024 * 1024
            ),
        )(*operands)
        out = pl.pallas_call(
            finish_kernel,
            name="finish",
            out_shape=jax.ShapeDtypeStruct((n_own, size, size), jnp.float32),
            in_specs=[in_vmem] * len(state),
            out_specs=in_hbm,
            scratch_shapes=[
                pltpu.VMEM((n_own, size, size), jnp.float32),
                pltpu.SMEM((2, 8, 128), jnp.int32),
                pltpu.SemaphoreType.DMA,
                pltpu.SemaphoreType.DMA((n_own // UNROLL,)),
            ],
            compiler_params=pltpu.CompilerParams(vmem_limit_bytes=28 * 1024 * 1024),
        )(*state)
        return out[None, None]

    return jax.shard_map(
        device_step, mesh=mesh, in_specs=(row_spec, col_spec, row_spec, row_spec, row_spec), out_specs=row_spec, check_vma=False
    )
```

```python
import functools

import jax
import jax.numpy as jnp
from jax import lax
from jax.experimental import pallas as pl
from jax.experimental.pallas import tpu as pltpu
from jax.sharding import PartitionSpec as P

MESH = pl.DeviceIdType.MESH
HALF_SET = 36
CHUNK = 5
A_CHUNK = 4
A_GATE = 0
B_GATE = 3
SLACK = 2.0
FEED_SLACK = 1.0
VMEM = 67_000_000
LAG = 3.0
SHARE_AT = 12.0
LATE = (4, 5)
JOB = 0.8
PIECES = 4
UNROLL = 8


class Move:
    def __init__(self, link, kind, src, dst, part, first, count, dep, shift, rank):
        self.link, self.kind, self.src, self.dst = link, kind, src, dst
        self.part, self.first, self.count, self.dep = part, first, count, dep
        self.shift = shift
        self.rank = rank
        self.after = []


def cut(first, count, size):
    return [(first + at, min(size, count - at)) for at in range(0, count, size)]


def plan(n_a, n_b):
    half = HALF_SET // 2
    quarter = (n_b - HALF_SET) // 4
    h1, h2 = cut(0, half // 2, CHUNK), cut(half // 2, half - half // 2, CHUNK)
    q1, q2 = cut(0, quarter // 2, CHUNK), cut(quarter // 2, quarter - quarter // 2, CHUNK)
    a1, a2 = cut(0, n_a // 2, A_CHUNK), cut(n_a // 2, n_a - n_a // 2, A_CHUNK)
    moves = []

    def add(link, kind, src, dst, part, piece, dep, rank, shift=0):
        move = Move(link, kind, src, dst, part, piece[0], piece[1], dep, shift, rank)
        move.index = len(moves)
        moves.append(move)
        if dep is not None:
            dep.after.append(move)
        if link != "d":
            row = {"+y": -1, "-y": 1}.get(link, 0) + shift
            add("d", kind, dst, dst, part, piece, move, 0, row)
        return move

    def spread(move, piece, far):
        if move.part == "h":
            add("+y" if piece in h1 else "-y", "b", move.dst, move.dst, "h", piece, move, far + 1)
            return
        up = add("+y", "b", move.dst, move.dst, "q", piece, move, far)
        down = add("-y", "b", move.dst, move.dst, "q", piece, move, far)
        if piece in q1:
            add("+y", "b", move.dst, move.dst, "q", piece, up, far + 2, -1)
        else:
            add("-y", "b", move.dst, move.dst, "q", piece, down, far + 2, 1)

    for kind, count in (("b", n_b), ("a", n_a), ("l", 1)):
        add("d", kind, 0, 0, "all", (0, count), None, 9)
    listed = set()
    for link, slot in (("+x", 3), ("-x", 1)):
        first = link == "+x"
        for part, one, two in (("q", q1, q2), ("h", h1, h2)):
            keep = one if first else two
            for piece in (one + two) if first else (two + one):
                move = add(link, "b", 0, slot, part, piece, None, 0)
                spread(move, piece, 0)
                if piece in keep:
                    spread(add(link, "b", slot, 2, part, piece, move, 1), piece, 3)
                if slot not in listed:
                    listed.add(slot)
                    lists = add(link, "l", 0, slot, "all", (0, 1), None, 0)
                    if first:
                        add(link, "l", slot, 2, "all", (0, 1), lists, 1)
        keep = a1 if first else a2
        mine = [m for m in moves if m.link == link and m.src == 0 and m.kind == "b"]
        gate = mine[-1 - (A_GATE if first else B_GATE)]
        for piece in (a1 + a2) if first else (a2 + a1):
            move = add(link, "a", 0, slot, "all", piece, gate, 2)
            if piece in keep:
                add(link, "a", slot, 2, "all", piece, move, 3)
    return moves


LINKS = ("+x", "-x", "+y", "-y")


def slack(move):
    feeds = [m for m in move.after if m.link != "d"]
    if move.link in ("+x", "-x"):
        return 0.0 if feeds else SLACK
    return FEED_SLACK if feeds else SLACK


def order(moves):
    free = {link: 0.0 for link in LINKS}
    events, steps, now = [], [], 0.0

    def send(move):
        steps.append((now, "send", move))
        if move.link != "d":
            free[move.link] = max(now, free[move.link]) + (0.3 if move.kind == "l" else move.count)
            events.append((free[move.link] + LAG + slack(move), move.index, move))

    for move in moves:
        if move.dep is None and move.link != "d":
            send(move)
    while events:
        events.sort(key=lambda e: e[:2])
        now, _, move = events.pop(0)
        steps.append((now, "take", move))
        for nxt in sorted(move.after, key=lambda m: (m.link == "d", m.rank)):
            send(nxt)
    return steps


def gather_kernel(sizes, a_hbm, b_hbm, pairs_hbm, plist_hbm, own_hbm, acc, table_v, *refs):
    n_x, n_y, n_a, n_b, n_own = sizes
    a_slot, b_slot = list(refs[0:8]), list(refs[8:16])
    for place, slot in enumerate(LATE + tuple(s for s in range(8) if s not in LATE)):
        a_slot[slot], b_slot[slot] = refs[2 * place], refs[2 * place + 1]
    l_slot = refs[16:24]
    own, table, send_sem, recv_sem, load_sem = refs[24:]
    y = lax.axis_index("rows")
    p = lax.axis_index("ksplit")
    x, core = p // 2, p % 2
    moves = plan(n_a, n_b)
    steps = order(moves)

    def at(dx, other):
        return 2 * ((x + dx) % n_x) + (core + other) % 2

    target = {
        "+x": {"ksplit": at(1, 0)},
        "-x": {"ksplit": at(n_x - 1, 0)},
        "+y": {"rows": (y + 1) % n_y},
        "-y": {"rows": (y + n_y - 1) % n_y},
        "d": {"ksplit": at(0, 1)},
    }

    loads = [
        pltpu.make_async_copy(b_hbm, b_slot[0], load_sem.at[0]),
        pltpu.make_async_copy(a_hbm, a_slot[0], load_sem.at[1]),
        pltpu.make_async_copy(pairs_hbm, l_slot[0].at[0], load_sem.at[2]),
        pltpu.make_async_copy(plist_hbm, l_slot[0].at[1], load_sem.at[3]),
        pltpu.make_async_copy(own_hbm, own, load_sem.at[4]),
    ]
    for load in loads:
        load.start()

    barrier = pltpu.get_barrier_semaphore()
    for device in target.values():
        pl.semaphore_signal(barrier, inc=1, device_id=device, device_id_type=MESH)
    pl.semaphore_wait(barrier, len(target))

    def copy(move, row):
        holder = (row + move.shift + 2 * n_y) % n_y
        half = HALF_SET // 2
        quarter = (n_b - HALF_SET) // 4
        base = {"all": 0, "h": (holder % 2) * half, "q": HALF_SET + holder * quarter}[move.part]
        where = pl.ds(base + move.first, move.count)
        slots = {"a": a_slot, "b": b_slot, "l": l_slot}[move.kind]
        src = slots[2 * move.src]
        dst = slots[2 * move.dst + (1 if move.link == "d" else 0)]
        if move.kind != "l":
            src, dst = src.at[where], dst.at[where]
        return pltpu.make_async_remote_copy(
            src_ref=src,
            dst_ref=dst,
            send_sem=send_sem.at[move.index],
            recv_sem=recv_sem.at[move.index],
            device_id=target[move.link],
            device_id_type=MESH,
        )

    def start(move):
        copy(move, y).start()

    def receive(move):
        row = {"+y": y + n_y - 1, "-y": y + 1}.get(move.link, y)
        copy(move, row).wait_recv()

    def run(step):
        _, what, move = step
        if what == "send":
            start(move)
        else:
            receive(move)

    for load in loads:
        load.wait()
    while steps[0][1] == "send":
        run(steps.pop(0))

    def make_table():
        for move in moves:
            if move.kind == "l" and move.link == "d":
                receive(move)
        mine = pl.ds(pl.multiple_of(x * 128, 128), 128)
        rows = [[slot[what, which:which + 1, mine] for slot in l_slot] for what in range(2) for which in range(2)]
        pair_a, pair_q, at_i, at_j = [jnp.concatenate(row, axis=0) for row in rows]
        key = at_i * 65536 + at_j
        code = pair_a * 65536 + pair_q
        wanted = own[0:1, :] * 65536 + own[1:2, :]
        wanted = jnp.concatenate([wanted] * (128 // n_own), axis=1)
        wanted = jnp.broadcast_to(wanted, key.shape)

        def turn(_, state):
            key, code, found = state
            found = jnp.where(key == wanted, code, found)
            return pltpu.roll(key, 1, 1), pltpu.roll(code, 1, 1), found

        _, _, found = lax.fori_loop(0, 128, turn, (key, code, jnp.zeros_like(code)), unroll=8)
        table_v[0] = found // 65536
        table_v[1] = found % 65536

    def use_table():
        to_smem = pltpu.make_async_copy(table_v, table, load_sem.at[5])
        to_smem.start()
        to_smem.wait()

    def compute(slots, part, first=False):
        def step(i, _):
            for u in range(UNROLL):
                c = i * UNROLL + u
                total = product(a_slot, b_slot, table, slots[0], c)
                for slot in slots[1:]:
                    total = total + product(a_slot, b_slot, table, slot, c)
                acc[c] = total if first else acc[c] + total
            return 0

        count = n_own // UNROLL // part[1]
        lax.fori_loop(part[0] * count, (part[0] + 1) * count, step, 0)

    def from_partner(dx):
        for move in moves:
            if move.link == "d" and move.dst == dx and move.kind != "l":
                receive(move)

    def ready(dx):
        return not [s for s in steps if s[1] == "take" and s[2].dst == dx]

    early = [dx for dx in range(n_x) if 2 * dx not in LATE]
    jobs, queued = [], set()
    stage, clock, shared = 0, 0.0, False
    listed = max(at for at, what, move in steps if what == "take" and move.kind == "l")
    while steps:
        now = steps[0][0]
        if not shared and now > SHARE_AT:
            shared = True
            for move in moves:
                if move.dep is None and move.link == "d":
                    start(move)
        if stage == 0 and now > listed + 2.0:
            make_table()
            stage = 1
        elif stage == 1 and now > listed + 5.0:
            use_table()
            stage = 2
        for dx in early:
            if stage == 2 and dx not in queued and ready(dx):
                jobs.append((0.0, functools.partial(from_partner, dx)))
                jobs += [(JOB, functools.partial(compute, (2 * dx, 2 * dx + 1), (i, PIECES), first=not queued)) for i in range(PIECES)]
                queued.add(dx)
        clock = max(clock, now)
        run(steps.pop(0))
        while steps and steps[0][0] == now:
            run(steps.pop(0))
        until = steps[0][0] if steps else clock + 100.0
        while jobs and clock + jobs[0][0] < until + 1.0:
            cost, job = jobs.pop(0)
            job()
            clock += cost
    for _, job in jobs:
        job()
    for dx in range(n_x):
        if dx not in early:
            from_partner(dx)

    for move in moves:
        copy(move, y).wait_send()


def product(a_slot, b_slot, table, slot, c):
    left = a_slot[slot][table[0, slot, c]]
    right = b_slot[slot][table[1, slot, c]]
    part = jnp.dot(left, right, preferred_element_type=jnp.float32)
    return part.astype(jnp.bfloat16).astype(jnp.float32)


def finish_kernel(acc, table_v, *refs):
    a_slot = {slot: refs[2 * place] for place, slot in enumerate(LATE)}
    b_slot = {slot: refs[2 * place + 1] for place, slot in enumerate(LATE)}
    out_hbm, total_v, table, sem, out_sem = refs[2 * len(LATE):]
    n_own = acc.shape[0]
    to_smem = pltpu.make_async_copy(table_v, table, sem)
    to_smem.start()
    to_smem.wait()

    def out_copy(i):
        where = pl.ds(i * UNROLL, UNROLL)
        return pltpu.make_async_copy(total_v.at[where], out_hbm.at[where], out_sem.at[i])

    def step(i, _):
        for u in range(UNROLL):
            c = i * UNROLL + u
            total = None if len(LATE) == 8 else acc[c]
            for slot in LATE:
                part = product(a_slot, b_slot, table, slot, c)
                total = part if total is None else total + part
            total_v[c] = total
        out_copy(i).start()
        return 0

    lax.fori_loop(0, n_own // UNROLL, step, 0)
    for i in range(n_own // UNROLL):
        out_copy(i).wait()


def solution(mesh):
    n_y = mesh.shape["rows"]
    n_x = mesh.shape["ksplit"] // 2
    row_spec = P(("batch", "rows"), "ksplit")
    col_spec = P(("batch", "ksplit"))

    def device_step(a_loc, b_loc, pair_loc, plist_loc, cidx_loc):
        a, b = a_loc[0, 0], b_loc[0]
        n_a, size, _ = a.shape
        n_b = b.shape[0]
        n_own = cidx_loc.shape[2]
        n_part = plist_loc.shape[2]
        assert n_x == 4 and n_y == 4 and n_part == n_x * 128 and 128 % n_own == 0
        moves = plan(n_a, n_b)
        in_hbm = pl.BlockSpec(memory_space=pltpu.HBM)
        in_vmem = pl.BlockSpec(memory_space=pltpu.VMEM)
        a_shape, b_shape = (n_a, size, size), (n_b, size, size)
        operands = [
            pltpu.with_memory_space_constraint(one, pltpu.HBM)
            for one in (a, b, pair_loc[0, 0, :, 0, :].T, plist_loc[0, 0].T, cidx_loc[0, 0].T)
        ]
        state = pl.pallas_call(
            functools.partial(gather_kernel, (n_x, n_y, n_a, n_b, n_own)),
            name="gather",
            out_shape=[pltpu.VMEM((n_own, size, size), jnp.float32), pltpu.VMEM((2, 8, 128), jnp.int32)]
            + [pltpu.VMEM(a_shape, jnp.bfloat16), pltpu.VMEM(b_shape, jnp.bfloat16)] * len(LATE),
            in_specs=[in_hbm] * 5,
            out_specs=[in_vmem] * (2 + 2 * len(LATE)),
            scratch_shapes=[pltpu.VMEM(a_shape, jnp.bfloat16), pltpu.VMEM(b_shape, jnp.bfloat16)] * (8 - len(LATE))
            + [
                pltpu.VMEM((2, 2, n_part), jnp.int32) for _ in range(8)
            ]
            + [
                pltpu.VMEM((2, n_own), jnp.int32),
                pltpu.SMEM((2, 8, 128), jnp.int32),
                pltpu.SemaphoreType.DMA((len(moves),)),
                pltpu.SemaphoreType.DMA((len(moves),)),
                pltpu.SemaphoreType.DMA((6,)),
            ],
            compiler_params=pltpu.CompilerParams(
                collective_id=0, has_side_effects=True, vmem_limit_bytes=28 * 1024 * 1024
            ),
        )(*operands)
        out = pl.pallas_call(
            finish_kernel,
            name="finish",
            out_shape=jax.ShapeDtypeStruct((n_own, size, size), jnp.float32),
            in_specs=[in_vmem] * len(state),
            out_specs=in_hbm,
            scratch_shapes=[
                pltpu.VMEM((n_own, size, size), jnp.float32),
                pltpu.SMEM((2, 8, 128), jnp.int32),
                pltpu.SemaphoreType.DMA,
                pltpu.SemaphoreType.DMA((n_own // UNROLL,)),
            ],
            compiler_params=pltpu.CompilerParams(vmem_limit_bytes=28 * 1024 * 1024),
        )(*state)
        return out[None, None]

    return jax.shard_map(
        device_step, mesh=mesh, in_specs=(row_spec, col_spec, row_spec, row_spec, row_spec), out_specs=row_spec, check_vma=False
    )
```
